256 devices in a mesh: radial: 64 (over x, z, core), phi: 4 (over y).
Axes of the slice: x: 4, y: 4, z: 8, core: 2. Of those that a mesh axis runs over, the one named last changes fastest.
Arguments:
- conserved: float32 [8, 512, 64, 128], P(None, 'radial', 'phi'), may hold values from -2.5 to 7, as said below
- core_mass: float32 [1], replicated, may hold values from 0.2 to 1
Outputs:
- advanced: float32 [8, 512, 64, 128], P(None, 'radial', 'phi')
- enclosed_mass: float32 [512], P('radial')
The draws below stay inside these ranges and needn't reach their ends.
Inputs may be any that keep to these rules, and one draw needn't show every extreme that they name: conserved[0] (density) lies between 0.4 and 2.5; conserved[4] exceeds (conserved[1]^2 + conserved[2]^2 + conserved[3]^2)/(2 conserved[0]) by at least 0.6; the speeds |conserved[m]/conserved[0]| stay below 1; conserved[5..7] lie between 0 and conserved[0].
All inputs are finite; a program needn't handle non-finite values.
Results may differ from the reference program's by a relative error of at most 0.0003.
Values sent between devices are 32-bit elements; how exact they have to be, the bound alone decides.
A program may use at most 64 MiB of HBM per device.

```python
import math
import jax
import jax.numpy as jnp
from jax import lax

RD = 8
NT = 128
NR = 512
NP = 64


def draw_conserved(key, part):
    subkeys = jax.random.split(key, 12)
    shape = (NR, NP, NT)
    depth = (jnp.arange(NR, dtype=jnp.float32) + 0.5) / NR
    azimuth = (jnp.arange(NP, dtype=jnp.float32) + 0.5) * (2.0 * math.pi / NP)
    centres = jax.random.uniform(subkeys[6], (3,), jnp.float32, 0.0, 1.0)
    heights = jax.random.uniform(subkeys[7], (3,), jnp.float32, -0.13, 0.13)
    bumps = jnp.exp(-jnp.square((depth[:, None] - centres[None, :]) / 0.15))
    profile = jnp.exp(jnp.sum(bumps * heights[None, :], axis=1))
    turn = jax.random.uniform(subkeys[8], (), jnp.float32, 0.0, 2.0 * math.pi)
    twist = jax.random.uniform(subkeys[9], (), jnp.float32, -0.5 * math.pi, 0.5 * math.pi)
    phase = turn + twist * depth
    angular = 1.0 + 0.35 * jnp.cos(azimuth[None, :] - phase[:, None])
    smooth = (profile[:, None] * angular)[:, :, None]
    rough = jnp.exp(jax.random.uniform(subkeys[0], shape, jnp.float32, jnp.log(0.75), jnp.log(1.33)))
    density = jnp.clip(smooth * rough, 0.4, 2.5)
    speeds = [jnp.clip(0.3 * jax.random.normal(subkeys[1 + which], shape, jnp.float32), -0.99, 0.99) for which in range(3)]
    pressure = jax.random.uniform(subkeys[4], shape, jnp.float32, 0.3, 0.9)
    kinetic = 0.5 * density * (speeds[0] * speeds[0] + speeds[1] * speeds[1] + speeds[2] * speeds[2])
    energy = pressure / (4.0 / 3.0 - 1.0) + kinetic
    tracers = jax.random.uniform(subkeys[5], (3,) + shape, jnp.float32, 0.0, 1.0) * density[None]
    momenta = jnp.stack([density * speeds[0], density * speeds[1], density * speeds[2]])
    return jnp.concatenate([density[None], momenta, energy[None], tracers], axis=0)


def setup_inputs(seed: int = 0) -> dict:
    streams_of = jax.random.split(jax.random.key(seed), 3)
    conserved = draw_conserved(jax.random.fold_in(streams_of[2], 71), 0)
    core_mass = jnp.clip(jnp.exp(jax.random.uniform(streams_of[1], (1,), jnp.float32, math.log(0.2), math.log(1.0))), 0.2, 1.0)
    return {"conserved": conserved, "core_mass": core_mass}


ADIABATIC = 4.0 / 3.0
INNER_RADIUS = 1.0
OUTER_RADIUS = 2.0
COURANT = 0.4
GRAVITY_KICK = 0.004
MINIMUM_DENSITY = 0.05
PRESSURE_FLOOR = 0.01

def step_sizes(radial_total, phi_total, theta_total):
    theta_step = math.pi / theta_total
    phi_step = 2.0 * math.pi / phi_total
    polar_width = INNER_RADIUS * math.sin(0.5 * theta_step) * phi_step
    radial_step = min(2.0 * polar_width, (OUTER_RADIUS - INNER_RADIUS) / radial_total)
    timestep = COURANT * min(radial_step, polar_width)
    return (radial_step, theta_step, phi_step, timestep)

def thermo(values):
    density = jnp.maximum(values[0], MINIMUM_DENSITY)
    kinetic = 0.5 * (values[1] * values[1] + values[2] * values[2] + values[3] * values[3]) / density
    pressure = jnp.maximum((ADIABATIC - 1.0) * (values[4] - kinetic), PRESSURE_FLOOR * density)
    return (density, pressure)

def physical(values, component):
    density, pressure = thermo(values)
    normal = values[component] / density
    sound = jnp.sqrt(ADIABATIC * pressure / density)
    pieces = [values[which] * normal for which in range(values.shape[0])]
    pieces[component] = pieces[component] + pressure
    pieces[4] = pieces[4] + pressure * normal
    return (jnp.stack(pieces), jnp.abs(normal) + sound)

def face_flux(values, along_dim, component):
    interior = values.shape[along_dim] - 4
    neighbour_differences = lax.slice_in_dim(values, 1, interior + 4, axis=along_dim) - lax.slice_in_dim(values, 0, interior + 3, axis=along_dim)
    below_diff = lax.slice_in_dim(neighbour_differences, 0, interior + 2, axis=along_dim)
    above_diff = lax.slice_in_dim(neighbour_differences, 1, interior + 3, axis=along_dim)
    limited = 0.5 * (jnp.sign(below_diff) + jnp.sign(above_diff)) * jnp.minimum(jnp.abs(below_diff), jnp.abs(above_diff))
    left_state = lax.slice_in_dim(values, 1, interior + 2, axis=along_dim) + 0.5 * lax.slice_in_dim(limited, 0, interior + 1, axis=along_dim)
    right_state = lax.slice_in_dim(values, 2, interior + 3, axis=along_dim) - 0.5 * lax.slice_in_dim(limited, 1, interior + 2, axis=along_dim)
    left_flux, left_signal = physical(left_state, component)
    right_flux, right_signal = physical(right_state, component)
    signal = jnp.maximum(left_signal, right_signal)
    return 0.5 * (left_flux + right_flux) - 0.5 * signal * (right_state - left_state)

def hydro_rate(extended, cell_centers, enclosed, radial_step, theta_step, phi_step, strength):
    theta_cells = extended.shape[3]
    centre_cells = extended[:, 2:-2, 2:-2, :]
    polar_padded = jnp.pad(centre_cells, ((0, 0), (0, 0), (0, 0), (2, 2)), mode='edge')
    radial_flux = face_flux(extended[:, :, 2:-2, :], 1, 1)
    polar_flux = face_flux(polar_padded, 3, 2)
    azimuth_flux = face_flux(extended[:, 2:-2, :, :], 2, 3)
    angles = (jnp.arange(theta_cells, dtype=jnp.float32) + 0.5) * theta_step
    sine_center = jnp.sin(angles)
    cosine = jnp.cos(angles)
    face_sine = jnp.sin(jnp.arange(theta_cells + 1, dtype=jnp.float32) * theta_step)
    radius = cell_centers[:, None, None]
    face_radius = jnp.concatenate([cell_centers - 0.5 * radial_step, cell_centers[-1:] + 0.5 * radial_step])[:, None, None]
    radial_area = face_radius * face_radius * radial_flux
    divergence = (radial_area[:, 1:] - radial_area[:, :-1]) / (radius * radius * radial_step)
    polar_area = face_sine * polar_flux
    divergence = divergence + (polar_area[..., 1:] - polar_area[..., :-1]) / (radius * sine_center * theta_step)
    divergence = divergence + (azimuth_flux[:, :, 1:] - azimuth_flux[:, :, :-1]) / (radius * sine_center * phi_step)
    density, pressure = thermo(centre_cells)
    radial_speed = centre_cells[1] / density
    polar_speed = centre_cells[2] / density
    azimuth_speed = centre_cells[3] / density
    cotangent = cosine / sine_center
    gravity_pull = strength * enclosed[:, None, None] / (radius * radius)
    source_radial = (2.0 * pressure + density * (polar_speed * polar_speed + azimuth_speed * azimuth_speed)) / radius - density * gravity_pull
    source_polar = (pressure * cotangent + density * azimuth_speed * azimuth_speed * cotangent - density * radial_speed * polar_speed) / radius
    source_azimuth = -density * azimuth_speed * (radial_speed + polar_speed * cotangent) / radius
    source_energy = -centre_cells[1] * gravity_pull
    nothing = jnp.zeros_like(pressure)
    source = jnp.stack([nothing, source_radial, source_polar, source_azimuth, source_energy, nothing, nothing, nothing])
    return source - divergence

def reference(conserved, core_mass):
    radial_total = conserved.shape[1]
    phi_total = conserved.shape[2]
    theta_total = conserved.shape[3]
    radial_step, theta_step, phi_step, timestep = step_sizes(radial_total, phi_total, theta_total)
    strength = GRAVITY_KICK / timestep
    cell_centers = INNER_RADIUS + (jnp.arange(radial_total, dtype=jnp.float32) + 0.5) * radial_step
    sine_center = jnp.sin((jnp.arange(theta_total, dtype=jnp.float32) + 0.5) * theta_step)
    shells = jnp.dot(lax.optimization_barrier(jnp.sum(conserved[0], axis=1)), sine_center, precision=lax.Precision.HIGHEST)
    shells = shells * cell_centers * cell_centers * (radial_step * theta_step * phi_step)
    enclosed = core_mass[0] + jnp.cumsum(shells) - 0.5 * shells
    blocks = radial_total // RD

    def full_rate(values):
        padded = jnp.pad(values, ((0, 0), (2, 2), (0, 0), (0, 0)), mode='edge')
        padded = jnp.pad(padded, ((0, 0), (0, 0), (2, 2), (0, 0)), mode='wrap')

        def one_block(block_index):
            first_row = (block_index * RD).astype(jnp.int32)
            radial_segment = lax.dynamic_slice_in_dim(padded, first_row, RD + 4, 1)
            radius_part = lax.dynamic_slice_in_dim(cell_centers, first_row, RD, 0)
            mass_part = lax.dynamic_slice_in_dim(enclosed, first_row, RD, 0)
            return hydro_rate(radial_segment, radius_part, mass_part, radial_step, theta_step, phi_step, strength)
        stacked = lax.map(one_block, jnp.arange(blocks, dtype=jnp.int32))
        return jnp.transpose(stacked, (1, 0, 2, 3, 4)).reshape(values.shape)
    section_one = conserved + timestep * full_rate(conserved)
    section_two = section_one + timestep * full_rate(section_one)
    advanced = 0.5 * conserved + 0.5 * section_two
    return (advanced, enclosed)
```

```python
import functools
import math

import jax
import jax.numpy as jnp
import numpy as np
from jax import lax
from jax.experimental import pallas as pl
from jax.experimental.pallas import tpu as pltpu
from jax.sharding import PartitionSpec as P

ADIABATIC = 4.0 / 3.0
INNER_RADIUS = 1.0
OUTER_RADIUS = 2.0
COURANT = 0.4
GRAVITY_KICK = 0.004
MINIMUM_DENSITY = 0.05
PRESSURE_FLOOR = 0.01

NV = 8
MESH = pl.DeviceIdType.MESH


def step_sizes(radial_total, phi_total, theta_total):
    theta_step = math.pi / theta_total
    phi_step = 2.0 * math.pi / phi_total
    polar_width = INNER_RADIUS * math.sin(0.5 * theta_step) * phi_step
    radial_step = min(2.0 * polar_width, (OUTER_RADIUS - INNER_RADIUS) / radial_total)
    timestep = COURANT * min(radial_step, polar_width)
    return (radial_step, theta_step, phi_step, timestep)


def half_slope(low, high):
    return jnp.maximum(jnp.minimum(low, high), jnp.minimum(jnp.maximum(low, high), 0.0))


def face_side(state, component):
    density = jnp.maximum(state[0], MINIMUM_DENSITY)
    inverse = 1.0 / density
    squares = state[1] * state[1] + state[2] * state[2] + state[3] * state[3]
    pressure = jnp.maximum(
        (ADIABATIC - 1.0) * (state[4] - 0.5 * squares * inverse), PRESSURE_FLOOR * density
    )
    normal = state[component] * inverse
    square = ADIABATIC * pressure * inverse
    sound = square * lax.rsqrt(square)
    return pressure, normal, jnp.abs(normal) + sound


def twice_flux(left, right, component):
    left_p, left_v, left_s = face_side(left, component)
    right_p, right_v, right_s = face_side(right, component)
    signal = jnp.maximum(left_s, right_s)
    left_w, right_w = left_v + signal, right_v - signal
    flux = [left[k] * left_w + right[k] * right_w for k in range(NV)]
    flux[component] = flux[component] + (left_p + right_p)
    flux[4] = flux[4] + (left_p * left_v + right_p * right_v)
    return flux


def edge_pair(cells, component):
    lefts, rights = [], []
    for k in range(NV):
        halves = [0.5 * (cells[i + 1][k] - cells[i][k]) for i in range(4)]
        slopes = [half_slope(halves[i], halves[i + 1]) for i in range(3)]
        lefts.append((cells[1][k] + slopes[0], cells[2][k] + slopes[1]))
        rights.append((cells[2][k] - slopes[1], cells[3][k] - slopes[2]))
    return [
        twice_flux([a[i] for a in lefts], [b[i] for b in rights], component) for i in range(2)
    ]


def kernel(
    sizes, state_hbm, mass_smem, angles_hbm,
    out_hbm, enclosed_ref,
    u0, u1, hr0, hr1, hp0, hp1, pk0, pk1, sr, acc, fp, fr, sl, outv,
    m1, m2, tab, grav, ct,
    in_sem, out_sem, halo_send, halo_recv, m1_send, m1_recv, m2_send, m2_recv,
):
    rows, width, slabs, wedges, groups, radial_step, theta_step, phi_step, timestep = sizes
    strength = GRAVITY_KICK / timestep
    place = lax.axis_index("radial")
    wedge = lax.axis_index("phi")
    inner = slabs // groups
    group, member = place // inner, lax.rem(place, inner)
    span = width + 8

    def at(radial, phi):
        return {"radial": radial, "phi": phi}

    up, down = lax.rem(place + 1, slabs), lax.rem(place + slabs - 1, slabs)
    east, west = lax.rem(wedge + 1, wedges), lax.rem(wedge + wedges - 1, wedges)
    plane = [
        at(lax.rem(place + inner * (j // wedges), slabs), lax.rem(wedge + j % wedges, wedges))
        for j in range(groups * wedges)
    ]
    column = [at(group * inner + lax.rem(member + j, inner), wedge) for j in range(inner)]

    fetch = pltpu.make_async_copy(state_hbm, u0.at[:, pl.ds(8, rows * width), :], in_sem.at[0])
    fetch.start()
    fetch_angles = pltpu.make_async_copy(angles_hbm, ct, in_sem.at[1])
    fetch_angles.start()

    barrier = pltpu.get_barrier_semaphore()
    greeted = plane[1:] + column[1:] + [at(up, wedge), at(down, wedge)]
    for peer in greeted:
        pl.semaphore_signal(barrier, inc=1, device_id=peer, device_id_type=MESH)

    row = lax.broadcasted_iota(jnp.int32, (8, 128), 0)
    lane = lax.broadcasted_iota(jnp.int32, (8, 128), 1)
    first = place * rows

    def radius_of(index):
        return INNER_RADIUS + (index.astype(jnp.float32) + 0.5) * radial_step

    radius = radius_of(first + row)
    inverse_radius = 1.0 / radius
    low_face, high_face = radius - 0.5 * radial_step, radius + 0.5 * radial_step
    area = inverse_radius * inverse_radius * (0.5 * timestep / radial_step)
    tab[0] = timestep * inverse_radius
    tab[1] = low_face * low_face * area
    tab[2] = high_face * high_face * area

    fetch_angles.wait()
    fetch.wait()

    total = u0[0, pl.ds(8, 8, stride=width), :]
    for f in range(1, width):
        total = total + u0[0, pl.ds(8 + f, 8, stride=width), :]
    shells = jnp.sum(total * ct[3:4, :], axis=1, keepdims=True) * (
        radius * radius * (radial_step * theta_step * phi_step)
    )
    m1[0] = jnp.sum(jnp.where(lane == member * rows + row, shells, 0.0), axis=0, keepdims=True)

    def pack(source, packed):
        for side, zones in enumerate(((width - 2, width - 1), (0, 1))):
            for k in range(NV):
                for i, zone in enumerate(zones):
                    packed[side, k, i] = source[k, pl.ds(8 + zone, 8, stride=width), :]

    pack(u0, pk0)
    pl.semaphore_wait(barrier, len(greeted))

    m1_copies = [
        pltpu.make_async_remote_copy(
            src_ref=m1.at[0], dst_ref=m1.at[j], send_sem=m1_send.at[j], recv_sem=m1_recv.at[j],
            device_id=plane[j], device_id_type=MESH,
        )
        for j in range(1, groups * wedges)
    ]
    for copy in m1_copies:
        copy.start()

    def halo_copies(number, high_rows, low_rows, packed, radial_halo, phi_halo):
        def copy(which, source, target, peer):
            return pltpu.make_async_remote_copy(
                src_ref=source, dst_ref=target, send_sem=halo_send.at[4 * number + which],
                recv_sem=halo_recv.at[4 * number + which], device_id=peer, device_id_type=MESH,
            )

        return (
            copy(0, high_rows, radial_halo.at[0], at(up, wedge)),
            copy(1, low_rows, radial_halo.at[1], at(down, wedge)),
            copy(2, packed.at[0], phi_halo.at[0], at(place, east)),
            copy(3, packed.at[1], phi_halo.at[1], at(place, west)),
        )

    def start_halos(copies, radial_halo, low_row, high_row):
        pl.when(place < slabs - 1)(lambda: copies[0].start())
        pl.when(place > 0)(lambda: copies[1].start())
        copies[2].start()
        copies[3].start()

        @pl.when(place == 0)
        def _():
            for k in range(NV):
                for i in range(2):
                    radial_halo[0, k, pl.ds(width * i, width), :] = low_row(k)

        @pl.when(place == slabs - 1)
        def _():
            for k in range(NV):
                for i in range(2):
                    radial_halo[1, k, pl.ds(width * i, width), :] = high_row(k)

    def wait_radial(copies):
        pl.when(place > 0)(lambda: copies[0].wait_recv())
        pl.when(place < slabs - 1)(lambda: copies[1].wait_recv())

    def wait_sent(copies):
        pl.when(place < slabs - 1)(lambda: copies[0].wait_send())
        pl.when(place > 0)(lambda: copies[1].wait_send())
        copies[2].wait_send()
        copies[3].wait_send()

    first_halos = halo_copies(
        0, u0.at[:, pl.ds(8 + (rows - 2) * width, 2 * width), :], u0.at[:, pl.ds(8, 2 * width), :],
        pk0, hr0, hp0,
    )
    start_halos(
        first_halos, hr0,
        lambda k: u0[k, pl.ds(8, width), :],
        lambda k: u0[k, pl.ds(8 + (rows - 1) * width, width), :],
    )

    wide_lane = lax.broadcasted_iota(jnp.int32, (width, 128), 1)

    def polar_and_azimuth(u):
        def one_row(r, carry):
            base = pl.multiple_of(8 + r * width, 8)
            here = pl.ds(base, width)
            cells = [u[k, here, :] for k in range(NV)]
            scale = tab[0, pl.ds(r, 1), :]
            density = jnp.maximum(cells[0], MINIMUM_DENSITY)
            inverse = 1.0 / density
            speed = [None] + [cells[m] * inverse for m in (1, 2, 3)]
            squares = cells[1] * speed[1] + cells[2] * speed[2] + cells[3] * speed[3]
            pressure = jnp.maximum(
                (ADIABATIC - 1.0) * (cells[4] - 0.5 * squares), PRESSURE_FLOOR * density
            )
            cotangent = ct[2:3, :]
            spin = cells[3] * speed[3]
            source = [None] * NV
            source[1] = 2.0 * pressure + (cells[2] * speed[2] + spin)
            source[2] = (pressure + spin) * cotangent - cells[1] * speed[2]
            source[3] = -speed[3] * (cells[1] + cells[2] * cotangent)
            mask = ct[4:5, :]
            left, right = [], []
            for k in range(NV):
                high = (pltpu.roll(cells[k], 127, 1) - cells[k]) * mask
                slope = half_slope(pltpu.roll(high, 1, 1), high)
                left.append(cells[k] + slope)
                right.append(
                    jnp.where(wide_lane == 127, cells[k], pltpu.roll(cells[k] - slope, 127, 1))
                )
            flux = twice_flux(left, right, 2)
            sine, inverse_sine = ct[0:1, :], ct[1:2, :]
            for k in range(NV):
                through = flux[k] * sine
                change = (pltpu.roll(through, 1, 1) - through) * inverse_sine
                if source[k] is not None:
                    change = change + source[k]
                acc[k, pl.ds(pl.multiple_of(r * width, 8), width), :] = cells[k] + scale * change
            left, right = [], []
            for k in range(NV):
                low = 0.5 * (cells[k] - u[k, pl.ds(base - 1, width), :])
                high = 0.5 * (u[k, pl.ds(base + 1, width), :] - cells[k])
                slope = half_slope(low, high)
                left.append(pltpu.roll(cells[k] + slope, 1, 0))
                right.append(cells[k] - slope)
            flux = twice_flux(left, right, 3)
            for k in range(NV):
                fp[k, pl.ds(pl.multiple_of(r * span, 8), width), :] = flux[k]
            return carry

        lax.fori_loop(0, rows, one_row, 0)

    def inner_radial(u):
        def one_row(r, carry):
            base = pl.multiple_of(8 + r * width, 8)
            store = pl.multiple_of(r * width, 8)
            right = []
            left = []
            for k in range(NV):
                cell = u[k, pl.ds(base, width), :]
                low = 0.5 * (cell - u[k, pl.ds(base - width, width), :])
                high = 0.5 * (u[k, pl.ds(base + width, width), :] - cell)
                slope = half_slope(low, high)
                right.append(cell - slope)
                left.append(sl[k, pl.ds(store - width, width), :])
                sl[k, pl.ds(store, width), :] = cell + slope
            flux = twice_flux(left, right, 1)
            for k in range(NV):
                fr[k, pl.ds(store, width), :] = flux[k]
            return carry

        lax.fori_loop(1, rows - 1, one_row, 0)

    def edge_azimuth(u, halo):
        for side in range(2):
            own = (0, 1, 2) if side == 0 else (width - 3, width - 2, width - 1)
            inside = [
                [u[k, pl.ds(8 + f, 8, stride=width), :] for k in range(NV)] for f in own
            ]
            outside = [[halo[side, k, i] for k in range(NV)] for i in range(2)]
            cells = outside + inside if side == 0 else inside + outside
            fluxes = edge_pair(cells, 3)
            faces = (0, 1) if side == 0 else (width - 1, width)
            for face, flux in zip(faces, fluxes):
                for k in range(NV):
                    fp[k, pl.ds(face, 8, stride=span), :] = flux[k]

    def edge_radial(u, halo):
        for side in range(2):
            own = (0, 1, 2) if side == 0 else (rows - 3, rows - 2, rows - 1)
            inside = [[u[k, pl.ds(8 + r * width, width), :] for k in range(NV)] for r in own]
            outside = [
                [halo[side, k, pl.ds(width * i, width), :] for k in range(NV)] for i in range(2)
            ]
            cells = outside + inside if side == 0 else inside + outside
            fluxes = edge_pair(cells, 1)
            faces = (0, 1) if side == 0 else (rows - 1, rows)
            for face, flux in zip(faces, fluxes):
                for k in range(NV):
                    fr[k, pl.ds(face * width, width), :] = flux[k]

    azimuth_scale = 0.5 / phi_step

    def advanced_row(r):
        store = pl.multiple_of(r * width, 8)
        low_area, high_area = tab[1, pl.ds(r, 1), :], tab[2, pl.ds(r, 1), :]
        across = tab[0, pl.ds(r, 1), :] * ct[1:2, :] * azimuth_scale
        below = pl.multiple_of(r * span, 8)
        values = []
        for k in range(NV):
            values.append(
                acc[k, pl.ds(store, width), :]
                + across * (fp[k, pl.ds(below, width), :] - fp[k, pl.ds(below + 1, width), :])
                + low_area * fr[k, pl.ds(store, width), :]
                - high_area * fr[k, pl.ds(pl.multiple_of(store + width, 8), width), :]
            )
        return values

    polar_and_azimuth(u0)
    inner_radial(u0)

    for copy in m1_copies:
        copy.wait_recv()
    for i in range(groups):
        shell = m1[i * wedges]
        for j in range(1, wedges):
            shell = shell + m1[i * wedges + j]
        m2[0, i : i + 1, :] = shell
    m2_copies = [
        pltpu.make_async_remote_copy(
            src_ref=m2.at[0], dst_ref=m2.at[j], send_sem=m2_send.at[j], recv_sem=m2_recv.at[j],
            device_id=column[j], device_id_type=MESH,
        )
        for j in range(1, inner)
    ]
    for copy in m2_copies:
        copy.start()

    first_halos[2].wait_recv()
    first_halos[3].wait_recv()
    edge_azimuth(u0, hp0)
    wait_radial(first_halos)
    edge_radial(u0, hr0)

    def section_one_row(r, carry):
        values = advanced_row(r)
        for k in range(NV):
            u1[k, pl.ds(pl.multiple_of(8 + r * width, 8), width), :] = values[k]
        return carry

    lax.fori_loop(0, rows, section_one_row, 0)
    pack(u1, pk1)
    for k in range(NV):
        sr[0, k] = u1[k, pl.ds(8 + (rows - 2) * width, 2 * width), :]
        sr[1, k] = u1[k, pl.ds(8, 2 * width), :]
    second_halos = halo_copies(1, sr.at[0], sr.at[1], pk1, hr1, hp1)
    start_halos(
        second_halos, hr1,
        lambda k: sr[1, k, pl.ds(0, width), :],
        lambda k: sr[0, k, pl.ds(width, width), :],
    )

    for copy in m2_copies:
        copy.wait_recv()
    table = m2[0]
    for j in range(1, inner):
        table = table + m2[j]
    last = slabs * rows - 1
    beyond = jnp.clip(first + jnp.where(row < 2, row - 2, rows - 2 + row), 0, last)
    enclosed = []
    for target in (first + row, beyond):
        inside = jnp.zeros((8, 128), jnp.float32)
        for i in range(groups):
            index = lax.rem(group + groups - i, groups) * (inner * rows) + lane
            share = jnp.where(index < target, 1.0, jnp.where(index == target, 0.5, 0.0))
            inside = inside + share * table[i : i + 1, :]
        enclosed.append(jnp.sum(inside, axis=1, keepdims=True) + mass_smem[0])
    for i, target in enumerate((first + row, beyond)):
        inverse = 1.0 / radius_of(target)
        grav[8 * i : 8 * i + 8, :] = (timestep * strength) * enclosed[i] * inverse * inverse
    enclosed_ref[...] = jnp.sum(
        jnp.where(lane == row, enclosed[0], 0.0), axis=0, keepdims=True
    )[:, :rows]

    def gravity_row(r, carry):
        base = pl.ds(pl.multiple_of(8 + r * width, 8), width)
        pull = grav[pl.ds(r, 1), :]
        u1[1, base, :] = u1[1, base, :] - pull * jnp.maximum(u0[0, base, :], MINIMUM_DENSITY)
        u1[4, base, :] = u1[4, base, :] - pull * u0[1, base, :]
        return carry

    lax.fori_loop(0, rows, gravity_row, 0)

    polar_and_azimuth(u1)
    inner_radial(u1)
    second_halos[2].wait_recv()
    second_halos[3].wait_recv()
    pull = grav[0:8, :]
    for side in range(2):
        for i in range(2):
            hp1[side, 1, i] = hp1[side, 1, i] - pull * jnp.maximum(
                hp0[side, 0, i], MINIMUM_DENSITY
            )
            hp1[side, 4, i] = hp1[side, 4, i] - pull * hp0[side, 1, i]
    edge_azimuth(u1, hp1)
    wait_radial(second_halos)
    for side in range(2):
        for i in range(2):
            which = pl.ds(width * i, width)
            pull = grav[8 + 2 * side + i : 9 + 2 * side + i, :]
            hr1[side, 1, which, :] = hr1[side, 1, which, :] - pull * jnp.maximum(
                hr0[side, 0, which, :], MINIMUM_DENSITY
            )
            hr1[side, 4, which, :] = hr1[side, 4, which, :] - pull * hr0[side, 1, which, :]
    edge_radial(u1, hr1)

    def section_two_row(r, carry):
        values = advanced_row(r)
        base = pl.ds(pl.multiple_of(8 + r * width, 8), width)
        pull = grav[pl.ds(r, 1), :]
        values[1] = values[1] - pull * jnp.maximum(u1[0, base, :], MINIMUM_DENSITY)
        values[4] = values[4] - pull * u1[1, base, :]
        for k in range(NV):
            outv[k, pl.ds(pl.multiple_of(r * width, 8), width), :] = 0.5 * (
                u0[k, base, :] + values[k]
            )
        return carry

    lax.fori_loop(0, rows, section_two_row, 0)
    give = pltpu.make_async_copy(outv, out_hbm, out_sem.at[0])
    give.start()
    for copy in m1_copies + m2_copies:
        copy.wait_send()
    wait_sent(first_halos)
    wait_sent(second_halos)
    give.wait()


def body(groups, conserved, core_mass):
    _, rows, width, lanes = conserved.shape
    slabs, wedges = lax.axis_size("radial"), lax.axis_size("phi")
    inner = slabs // groups
    radial_step, theta_step, phi_step, timestep = step_sizes(rows * slabs, width * wedges, lanes)
    centers = (np.arange(lanes) + 0.5) * theta_step
    faces = (np.arange(lanes) + 1.0) * theta_step
    angles = np.zeros((8, lanes))
    angles[0] = np.sin(faces) * (0.5 / theta_step)
    angles[1] = 1.0 / np.sin(centers)
    angles[2] = np.cos(centers) / np.sin(centers)
    angles[3] = np.sin(centers)
    angles[4] = np.where(np.arange(lanes) == lanes - 1, 0.0, 0.5)
    angles = jnp.asarray(angles.astype(np.float32))
    sizes = (rows, width, slabs, wedges, groups, radial_step, theta_step, phi_step, timestep)
    f32 = jnp.float32
    vmem = lambda *shape: pltpu.VMEM(shape, f32)
    dma = lambda count: pltpu.SemaphoreType.DMA((count,))
    cells = rows * width
    advanced, enclosed = pl.pallas_call(
        functools.partial(kernel, sizes),
        out_shape=(
            jax.ShapeDtypeStruct((NV, cells, lanes), f32),
            jax.ShapeDtypeStruct((1, rows), f32),
        ),
        in_specs=[
            pl.BlockSpec(memory_space=pl.ANY),
            pl.BlockSpec(memory_space=pltpu.SMEM),
            pl.BlockSpec(memory_space=pl.ANY),
        ],
        out_specs=(
            pl.BlockSpec(memory_space=pl.ANY),
            pl.BlockSpec(memory_space=pltpu.VMEM),
        ),
        scratch_shapes=[
            vmem(NV, cells + 16, lanes), vmem(NV, cells + 16, lanes),
            vmem(2, NV, 2 * width, lanes), vmem(2, NV, 2 * width, lanes),
            vmem(2, NV, 2, 8, lanes), vmem(2, NV, 2, 8, lanes),
            vmem(2, NV, 2, 8, lanes), vmem(2, NV, 2, 8, lanes),
            vmem(2, NV, 2 * width, lanes),
            vmem(NV, cells, lanes),
            vmem(NV, rows * (width + 8), lanes),
            vmem(NV, cells + width, lanes),
            vmem(NV, cells, lanes),
            vmem(NV, cells, lanes),
            vmem(groups * wedges, 1, lanes), vmem(inner, groups, lanes),
            vmem(3, 8, lanes), vmem(16, lanes), vmem(8, lanes),
            dma(2), dma(1), dma(8), dma(8),
            dma(groups * wedges), dma(groups * wedges), dma(inner), dma(inner),
        ],
        compiler_params=pltpu.CompilerParams(collective_id=0, has_side_effects=True),
    )(conserved.reshape(NV, cells, lanes), core_mass, angles)
    return advanced.reshape(conserved.shape), enclosed.reshape(rows)


def solution(mesh):
    in_specs = (P(None, "radial", "phi", None), P())
    out_specs = (P(None, "radial", "phi", None), P("radial"))
    return jax.shard_map(
        functools.partial(body, 4), mesh=mesh, in_specs=in_specs, out_specs=out_specs,
        check_vma=False,
    )
```

```python
import functools
import math

import jax
import jax.numpy as jnp
import numpy as np
from jax import lax
from jax.experimental import pallas as pl
from jax.experimental.pallas import tpu as pltpu
from jax.sharding import PartitionSpec as P

ADIABATIC = 4.0 / 3.0
INNER_RADIUS = 1.0
OUTER_RADIUS = 2.0
COURANT = 0.4
GRAVITY_KICK = 0.004
MINIMUM_DENSITY = 0.05
PRESSURE_FLOOR = 0.01

NV = 8
MESH = pl.DeviceIdType.MESH


def step_sizes(radial_total, phi_total, theta_total):
    theta_step = math.pi / theta_total
    phi_step = 2.0 * math.pi / phi_total
    polar_width = INNER_RADIUS * math.sin(0.5 * theta_step) * phi_step
    radial_step = min(2.0 * polar_width, (OUTER_RADIUS - INNER_RADIUS) / radial_total)
    timestep = COURANT * min(radial_step, polar_width)
    return (radial_step, theta_step, phi_step, timestep)


def half_slope(low, high):
    return jnp.maximum(jnp.minimum(low, high), jnp.minimum(jnp.maximum(low, high), 0.0))


def face_side(state, component):
    density = jnp.maximum(state[0], MINIMUM_DENSITY)
    inverse = 1.0 / density
    squares = state[1] * state[1] + state[2] * state[2] + state[3] * state[3]
    pressure = jnp.maximum(
        (ADIABATIC - 1.0) * (state[4] - 0.5 * squares * inverse), PRESSURE_FLOOR * density
    )
    normal = state[component] * inverse
    square = ADIABATIC * pressure * inverse
    sound = square * lax.rsqrt(square)
    return pressure, normal, jnp.abs(normal) + sound


def twice_flux(left, right, component):
    left_p, left_v, left_s = face_side(left, component)
    right_p, right_v, right_s = face_side(right, component)
    signal = jnp.maximum(left_s, right_s)
    left_w, right_w = left_v + signal, right_v - signal
    flux = [left[k] * left_w + right[k] * right_w for k in range(NV)]
    flux[component] = flux[component] + (left_p + right_p)
    flux[4] = flux[4] + (left_p * left_v + right_p * right_v)
    return flux


def edge_pair(cells, component):
    lefts, rights = [], []
    for k in range(NV):
        halves = [0.5 * (cells[i + 1][k] - cells[i][k]) for i in range(4)]
        slopes = [half_slope(halves[i], halves[i + 1]) for i in range(3)]
        lefts.append((cells[1][k] + slopes[0], cells[2][k] + slopes[1]))
        rights.append((cells[2][k] - slopes[1], cells[3][k] - slopes[2]))
    return [
        twice_flux([a[i] for a in lefts], [b[i] for b in rights], component) for i in range(2)
    ]


def sources(cells, cotangent):
    density = jnp.maximum(cells[0], MINIMUM_DENSITY)
    inverse = 1.0 / density
    speed = [None] + [cells[m] * inverse for m in (1, 2, 3)]
    squares = cells[1] * speed[1] + cells[2] * speed[2] + cells[3] * speed[3]
    pressure = jnp.maximum(
        (ADIABATIC - 1.0) * (cells[4] - 0.5 * squares), PRESSURE_FLOOR * density
    )
    spin = cells[3] * speed[3]
    source = [None] * NV
    source[1] = 2.0 * pressure + (cells[2] * speed[2] + spin)
    source[2] = (pressure + spin) * cotangent - cells[1] * speed[2]
    source[3] = -speed[3] * (cells[1] + cells[2] * cotangent)
    return source


def kernel(
    sizes, state_hbm, mass_hbm, angles_hbm,
    outv, enclosed_ref,
    u0, u1, hr0, hr1, hp0, hp1, pk0, pk1, sr, acc, fp, fr, sl, lt, rt, th,
    shared, below_above, wedge_rows, tab, grav, ct, core,
    in_sem, halo_send, halo_recv, shared_send, shared_recv, side_send, side_recv,
    wedge_send, wedge_recv, from_higher, from_opposite,
):
    rows, width, slabs, wedges, groups, radial_step, theta_step, phi_step, timestep = sizes
    strength = GRAVITY_KICK / timestep
    place = lax.axis_index("radial")
    wedge = lax.axis_index("phi")
    inner = slabs // groups
    levels = inner // 2
    group, member = place // inner, lax.rem(place, inner)
    level, core_index = member // 2, lax.rem(member, 2)
    span = width + 8
    last = slabs - 1

    def at(radial, phi):
        return {"radial": radial, "phi": phi}

    def signal(semaphore, radial, phi):
        pl.semaphore_signal(semaphore, inc=1, device_id=at(radial, phi), device_id_type=MESH)

    east, west = lax.rem(wedge + 1, wedges), lax.rem(wedge + wedges - 1, wedges)
    opposite = lax.rem(wedge + wedges // 2, wedges)

    fetch_mass = pltpu.make_async_copy(mass_hbm, core, in_sem.at[3])
    fetch_density = pltpu.make_async_copy(
        state_hbm.at[pl.ds(0, 1)], u0.at[pl.ds(0, 1), pl.ds(8, rows * width), :], in_sem.at[0]
    )
    fetch = pltpu.make_async_copy(
        state_hbm.at[pl.ds(1, NV - 1)], u0.at[pl.ds(1, NV - 1), pl.ds(8, rows * width), :],
        in_sem.at[1],
    )
    fetch_angles = pltpu.make_async_copy(angles_hbm, ct, in_sem.at[2])
    for copy in (fetch_density, fetch_angles, fetch, fetch_mass):
        copy.start()

    barrier = pltpu.get_barrier_semaphore()
    signal(barrier, place, east)
    signal(barrier, place, west)
    pl.when(wedge < wedges // 2)(lambda: signal(barrier, place, opposite))
    pl.when(place < last)(lambda: signal(barrier, place + 1, wedge))
    pl.when(place > 0)(lambda: signal(barrier, place - 1, wedge))

    def greet(x_start, x_stop, z_start, z_stop, semaphore):
        def one_level(z, carry):
            def one_group(x, inner_carry):
                for c in range(2):
                    signal(semaphore, x * inner + z * 2 + c, wedge)
                return inner_carry

            return lax.fori_loop(x_start, x_stop, one_group, carry)

        lax.fori_loop(z_start, z_stop, one_level, 0)

    greet(group + 1, groups, level, level + 1, barrier)
    greet(0, groups, level + 1, levels, barrier)
    greetings = (
        2 + 2 * groups * level + 2 * group + jnp.where(wedge < wedges // 2, 0, 1)
        + jnp.where(place > 0, 1, 0) + jnp.where(place < last, 1, 0)
    )

    row = lax.broadcasted_iota(jnp.int32, (8, 128), 0)
    lane = lax.broadcasted_iota(jnp.int32, (8, 128), 1)
    first = place * rows

    def radius_of(index):
        return INNER_RADIUS + (index.astype(jnp.float32) + 0.5) * radial_step

    radius = radius_of(first + row)
    inverse_radius = 1.0 / radius
    low_face, high_face = radius - 0.5 * radial_step, radius + 0.5 * radial_step
    area = inverse_radius * inverse_radius * (0.5 * timestep / radial_step)
    tab[0] = timestep * inverse_radius
    tab[1] = low_face * low_face * area
    tab[2] = high_face * high_face * area

    with jax.named_scope("fetch_wait"):
        fetch_angles.wait()
        fetch_density.wait()
    total = u0[0, pl.ds(8, 8, stride=width), :]
    for f in range(1, width):
        total = total + u0[0, pl.ds(8 + f, 8, stride=width), :]
    shells = jnp.sum(total * ct[3:4, :], axis=1, keepdims=True) * (
        radius * radius * (radial_step * theta_step * phi_step)
    )
    wedge_rows[0] = jnp.sum(jnp.where(lane == row, shells, 0.0), axis=0, keepdims=True)
    fetch.wait()

    def pack(source, packed):
        for side, zones in enumerate(((width - 2, width - 1), (0, 1))):
            for k in range(NV):
                for i, zone in enumerate(zones):
                    packed[side, k, i] = source[k, pl.ds(8 + zone, 8, stride=width), :]

    pack(u0, pk0)
    with jax.named_scope("barrier_wait"):
        pl.semaphore_wait(barrier, greetings)

    def copy_of(source, target, send, recv, radial, phi):
        return pltpu.make_async_remote_copy(
            src_ref=source, dst_ref=target, send_sem=send, recv_sem=recv,
            device_id=at(radial, phi), device_id_type=MESH,
        )

    def mass_copy(source, x, z, c):
        return copy_of(
            source, shared.at[level * 2 * groups + group * 2 + core_index],
            shared_send.at[z], shared_recv.at[level], x * inner + z * 2 + c, wedge,
        )

    def send_masses(source, x_start, z_start, z_stop):
        def one_group(x, carry):
            def one_level(z, inner_carry):
                for c in range(2):
                    mass_copy(source, x, z, c).start()
                return inner_carry

            return lax.fori_loop(z_start, z_stop, one_level, carry)

        lax.fori_loop(x_start, groups, one_group, 0)

    def many(count, z):
        rows_of = shared.at[pl.ds(z * 2 * groups, count)]
        return copy_of(rows_of, rows_of, shared_send.at[z], shared_recv.at[z], place, wedge)

    def await_masses(counts, z_start, z_stop, act):
        for x in range(groups):
            if counts[x]:

                @pl.when(group == x)
                def _(count=counts[x]):
                    def one_level(z, carry):
                        act(many(count, z))
                        return carry

                    lax.fori_loop(z_start, z_stop, one_level, 0)

    def wedge_copy(step):
        return copy_of(
            wedge_rows.at[0], wedge_rows.at[step], wedge_send, wedge_recv, place,
            lax.rem(wedge + step, wedges),
        )

    def wedge_all():
        others = wedge_rows.at[pl.ds(1, wedges - 1)]
        return copy_of(others, others, wedge_send, wedge_recv, place, east)

    def side_copy(side):
        target = jnp.minimum(place + 1, last) if side == 0 else jnp.maximum(place - 1, 0)
        return copy_of(
            below_above.at[2], below_above.at[side], side_send.at[side], side_recv.at[side],
            target, wedge,
        )

    for step in range(1, wedges):
        if step != wedges // 2:
            wedge_copy(step).start()

    def halo_copies(number, high_rows, low_rows, packed, radial_halo, phi_halo):
        def copy(which, source, target, peer):
            return pltpu.make_async_remote_copy(
                src_ref=source, dst_ref=target, send_sem=halo_send.at[4 * number + which],
                recv_sem=halo_recv.at[4 * number + which], device_id=peer, device_id_type=MESH,
            )

        return (
            copy(0, high_rows, radial_halo.at[0], at(jnp.minimum(place + 1, last), wedge)),
            copy(1, low_rows, radial_halo.at[1], at(jnp.maximum(place - 1, 0), wedge)),
            copy(2, packed.at[0], phi_halo.at[0], at(place, east)),
            copy(3, packed.at[1], phi_halo.at[1], at(place, west)),
        )

    def start_halos(copies, radial_halo, low_row, high_row):
        pl.when(place < last)(lambda: copies[0].start())
        pl.when(place > 0)(lambda: copies[1].start())
        copies[2].start()
        copies[3].start()

        @pl.when(place == 0)
        def _():
            for k in range(NV):
                for i in range(2):
                    radial_halo[0, k, pl.ds(width * i, width), :] = low_row(k)

        @pl.when(place == last)
        def _():
            for k in range(NV):
                for i in range(2):
                    radial_halo[1, k, pl.ds(width * i, width), :] = high_row(k)

    def wait_radial(copies):
        pl.when(place > 0)(lambda: copies[0].wait_recv())
        pl.when(place < last)(lambda: copies[1].wait_recv())

    def wait_sent(copies):
        pl.when(place < last)(lambda: copies[0].wait_send())
        pl.when(place > 0)(lambda: copies[1].wait_send())
        copies[2].wait_send()
        copies[3].wait_send()

    first_halos = halo_copies(
        0, u0.at[:, pl.ds(8 + (rows - 2) * width, 2 * width), :], u0.at[:, pl.ds(8, 2 * width), :],
        pk0, hr0, hp0,
    )
    start_halos(
        first_halos, hr0,
        lambda k: u0[k, pl.ds(8, width), :],
        lambda k: u0[k, pl.ds(8 + (rows - 1) * width, width), :],
    )

    greet(0, group, level, level + 1, from_higher)
    greet(0, groups, 0, level, from_higher)
    pl.when(wedge >= wedges // 2)(lambda: signal(from_opposite, place, opposite))

    wide_lane = lax.broadcasted_iota(jnp.int32, (width, 128), 1)

    def polar_and_azimuth(u):
        def one_step(i, carry):
            sine, inverse_sine, cotangent, mask = ct[0:1, :], ct[1:2, :], ct[2:3, :], ct[4:5, :]
            r = jnp.maximum(i - 2, 0)
            store = pl.ds(pl.multiple_of(r * width, 8), width)
            scale = tab[0, pl.ds(r, 1), :]
            cells = [u[k, pl.ds(pl.multiple_of(8 + r * width, 8), width), :] for k in range(NV)]
            source = sources(cells, cotangent)
            for k in range(NV):
                through = th[k, store, :]
                change = (pltpu.roll(through, 1, 1) - through) * inverse_sine
                if source[k] is not None:
                    change = change + source[k]
                acc[k, store, :] = cells[k] + scale * change
            r = jnp.clip(i - 1, 0, rows - 1)
            store = pl.ds(pl.multiple_of(r * width, 8), width)
            left = [lt[k, store, :] for k in range(NV)]
            right = []
            for k in range(NV):
                value = rt[k, store, :]
                cell = u[k, pl.ds(pl.multiple_of(8 + r * width, 8), width), :]
                right.append(jnp.where(wide_lane == 127, cell, pltpu.roll(value, 127, 1)))
            flux = twice_flux(left, right, 2)
            for k in range(NV):
                th[k, store, :] = flux[k] * sine
            r = jnp.minimum(i, rows - 1)
            base = pl.multiple_of(8 + r * width, 8)
            store = pl.ds(pl.multiple_of(r * width, 8), width)
            cells = [u[k, pl.ds(base, width), :] for k in range(NV)]
            for k in range(NV):
                high = (pltpu.roll(cells[k], 127, 1) - cells[k]) * mask
                low = (cells[k] - pltpu.roll(cells[k], 1, 1)) * ct[5:6, :]
                slope = half_slope(low, high)
                lt[k, store, :] = cells[k] + slope
                rt[k, store, :] = cells[k] - slope
            left, right = [], []
            for k in range(NV):
                low = 0.5 * (cells[k] - u[k, pl.ds(base - 1, width), :])
                high = 0.5 * (u[k, pl.ds(base + 1, width), :] - cells[k])
                slope = half_slope(low, high)
                left.append(pltpu.roll(cells[k] + slope, 1, 0))
                right.append(cells[k] - slope)
            flux = twice_flux(left, right, 3)
            for k in range(NV):
                fp[k, pl.ds(pl.multiple_of(r * span, 8), width), :] = flux[k]
            return carry

        lax.fori_loop(0, rows + 2, one_step, 0)

    def inner_radial(u):
        def one_row(r, carry):
            base = pl.multiple_of(8 + r * width, 8)
            store = pl.multiple_of(r * width, 8)
            right = []
            left = []
            for k in range(NV):
                cell = u[k, pl.ds(base, width), :]
                low = 0.5 * (cell - u[k, pl.ds(base - width, width), :])
                high = 0.5 * (u[k, pl.ds(base + width, width), :] - cell)
                slope = half_slope(low, high)
                right.append(cell - slope)
                left.append(sl[k, pl.ds(store - width, width), :])
                sl[k, pl.ds(store, width), :] = cell + slope
            flux = twice_flux(left, right, 1)
            for k in range(NV):
                fr[k, pl.ds(store, width), :] = flux[k]
            return carry

        lax.fori_loop(1, rows - 1, one_row, 0)

    def edge_azimuth(u, halo):
        for side in range(2):
            own = (0, 1, 2) if side == 0 else (width - 3, width - 2, width - 1)
            inside = [
                [u[k, pl.ds(8 + f, 8, stride=width), :] for k in range(NV)] for f in own
            ]
            outside = [[halo[side, k, i] for k in range(NV)] for i in range(2)]
            cells = outside + inside if side == 0 else inside + outside
            fluxes = edge_pair(cells, 3)
            faces = (0, 1) if side == 0 else (width - 1, width)
            for face, flux in zip(faces, fluxes):
                for k in range(NV):
                    fp[k, pl.ds(face, 8, stride=span), :] = flux[k]

    def edge_radial(u, halo):
        for side in range(2):
            own = (0, 1, 2) if side == 0 else (rows - 3, rows - 2, rows - 1)
            inside = [[u[k, pl.ds(8 + r * width, width), :] for k in range(NV)] for r in own]
            outside = [
                [halo[side, k, pl.ds(width * i, width), :] for k in range(NV)] for i in range(2)
            ]
            cells = outside + inside if side == 0 else inside + outside
            fluxes = edge_pair(cells, 1)
            faces = (0, 1) if side == 0 else (rows - 1, rows)
            for face, flux in zip(faces, fluxes):
                for k in range(NV):
                    fr[k, pl.ds(face * width, width), :] = flux[k]

    azimuth_scale = 0.5 / phi_step

    def advanced_row(r):
        store = pl.multiple_of(r * width, 8)
        low_area, high_area = tab[1, pl.ds(r, 1), :], tab[2, pl.ds(r, 1), :]
        across = tab[0, pl.ds(r, 1), :] * ct[1:2, :] * azimuth_scale
        below = pl.multiple_of(r * span, 8)
        values = []
        for k in range(NV):
            values.append(
                acc[k, pl.ds(store, width), :]
                + across * (fp[k, pl.ds(below, width), :] - fp[k, pl.ds(below + 1, width), :])
                + low_area * fr[k, pl.ds(store, width), :]
                - high_area * fr[k, pl.ds(pl.multiple_of(store + width, 8), width), :]
            )
        return values

    with jax.named_scope("pre1"):
        polar_and_azimuth(u0)
    pl.when(wedge < wedges // 2)(lambda: pl.semaphore_wait(from_opposite, 1))
    wedge_copy(wedges // 2).start()
    with jax.named_scope("rad1"):
        inner_radial(u0)

    with jax.named_scope("wedge_wait"):
        wedge_all().wait_recv()
    shell_row = wedge_rows[0]
    for j in range(1, wedges):
        shell_row = shell_row + wedge_rows[j]
    below_above[2] = shell_row
    pl.when(place < last)(lambda: side_copy(0).start())
    pl.when(place > 0)(lambda: side_copy(1).start())
    send_masses(below_above.at[2], group + 1, 0, level)

    with jax.named_scope("h1_phi_wait"):
        first_halos[2].wait_recv()
        first_halos[3].wait_recv()
    with jax.named_scope("edge_phi1"):
        edge_azimuth(u0, hp0)
    with jax.named_scope("h1_rad_wait"):
        wait_radial(first_halos)
    with jax.named_scope("edge_rad1"):
        edge_radial(u0, hr0)

    def section_one_row(r, carry):
        values = advanced_row(r)
        for k in range(NV):
            u1[k, pl.ds(pl.multiple_of(8 + r * width, 8), width), :] = values[k]
        return carry

    with jax.named_scope("final1"):
        lax.fori_loop(0, rows, section_one_row, 0)
    pack(u1, pk1)
    for k in range(NV):
        sr[0, k] = u1[k, pl.ds(8 + (rows - 2) * width, 2 * width), :]
        sr[1, k] = u1[k, pl.ds(8, 2 * width), :]
    second_halos = halo_copies(1, sr.at[0], sr.at[1], pk1, hr1, hp1)
    start_halos(
        second_halos, hr1,
        lambda k: sr[1, k, pl.ds(0, width), :],
        lambda k: sr[0, k, pl.ds(width, width), :],
    )

    with jax.named_scope("asc_wait"):
        answers = 2 * groups * (levels - 1 - level) + 2 * (groups - 1 - group)
        pl.when(answers > 0)(lambda: pl.semaphore_wait(from_higher, answers))
    send_masses(below_above.at[2], group + 1, level, level + 1)
    send_masses(below_above.at[2], group, level + 1, levels)

    from_all = [2 * x for x in range(groups)]
    from_lower = [2 * x + 2 for x in range(groups)]

    def mass_between(z_start, z_stop, count):
        def one_level(z, value):
            part = shared[pl.ds(z * 2 * groups, 2 * groups)]
            return value + jnp.sum(jnp.where(slot < count, part, 0.0), axis=0)

        return lax.fori_loop(z_start, z_stop, one_level, jnp.zeros((1, 128), jnp.float32))

    slot = lax.broadcasted_iota(jnp.int32, (2 * groups, 1, 128), 0)
    with jax.named_scope("m1_wait"):
        await_masses(from_all, level, levels, lambda copy: copy.wait_recv())
        await_masses(from_lower, 0, level, lambda copy: copy.wait_recv())
        pl.when(place > 0)(lambda: side_copy(0).wait_recv())
        pl.when(place < last)(lambda: side_copy(1).wait_recv())
    below, above, own = below_above[0], below_above[1], below_above[2]
    half_of = lambda index: jnp.where(lane < index, 1.0, jnp.where(lane == index, 0.5, 0.0))
    none = jnp.zeros((8, 128), jnp.float32)
    lower = jnp.where(row < 2, jnp.where(place == 0, half_of(0), none), 0.0)
    upper = jnp.where(row < 2, none, jnp.where(place == last, half_of(rows - 1), 1.0))
    minus = jnp.where(lane >= rows, 0.0, half_of(rows - 2 + row) - 1.0)
    minus = jnp.where(row < 2, minus, none)
    plus = jnp.where(row < 2, none, half_of(row - 2))
    inside = (
        mass_between(level, levels, 2 * group)
        + mass_between(0, level, 2 * group + 2)
        + jnp.where(core_index == 1, below, 0.0)
    )
    table = (
        inside + half_of(row) * own,
        inside
        + (lower + upper) * own
        + jnp.where(place > 0, minus * below, none)
        + jnp.where(place < last, plus * above, none),
    )
    beyond = jnp.clip(first + jnp.where(row < 2, row - 2, rows - 2 + row), 0, slabs * rows - 1)
    fetch_mass.wait()
    for i, target in enumerate((first + row, beyond)):
        enclosed = jnp.sum(table[i], axis=1, keepdims=True) + core[0]
        inverse = 1.0 / radius_of(target)
        grav[8 * i : 8 * i + 8, :] = (timestep * strength) * enclosed * inverse * inverse
        if i == 0:
            enclosed_ref[...] = jnp.sum(
                jnp.where(lane == row, enclosed, 0.0), axis=0, keepdims=True
            )[:, :rows]

    def gravity_row(r, carry):
        base = pl.ds(pl.multiple_of(8 + r * width, 8), width)
        pull = grav[pl.ds(r, 1), :]
        u1[1, base, :] = u1[1, base, :] - pull * jnp.maximum(u0[0, base, :], MINIMUM_DENSITY)
        u1[4, base, :] = u1[4, base, :] - pull * u0[1, base, :]
        return carry

    with jax.named_scope("grav"):
        lax.fori_loop(0, rows, gravity_row, 0)

    with jax.named_scope("pre2"):
        polar_and_azimuth(u1)
    with jax.named_scope("rad2"):
        inner_radial(u1)
    with jax.named_scope("h2_phi_wait"):
        second_halos[2].wait_recv()
        second_halos[3].wait_recv()
    pull = grav[0:8, :]
    for side in range(2):
        for i in range(2):
            hp1[side, 1, i] = hp1[side, 1, i] - pull * jnp.maximum(
                hp0[side, 0, i], MINIMUM_DENSITY
            )
            hp1[side, 4, i] = hp1[side, 4, i] - pull * hp0[side, 1, i]
    with jax.named_scope("edge_phi2"):
        edge_azimuth(u1, hp1)
    with jax.named_scope("h2_rad_wait"):
        wait_radial(second_halos)
    for side in range(2):
        for i in range(2):
            which = pl.ds(width * i, width)
            pull = grav[8 + 2 * side + i : 9 + 2 * side + i, :]
            hr1[side, 1, which, :] = hr1[side, 1, which, :] - pull * jnp.maximum(
                hr0[side, 0, which, :], MINIMUM_DENSITY
            )
            hr1[side, 4, which, :] = hr1[side, 4, which, :] - pull * hr0[side, 1, which, :]
    with jax.named_scope("edge_rad2"):
        edge_radial(u1, hr1)

    def section_two_row(r, carry):
        values = advanced_row(r)
        base = pl.ds(pl.multiple_of(8 + r * width, 8), width)
        pull = grav[pl.ds(r, 1), :]
        values[1] = values[1] - pull * jnp.maximum(u1[0, base, :], MINIMUM_DENSITY)
        values[4] = values[4] - pull * u1[1, base, :]
        for k in range(NV):
            outv[k, pl.ds(pl.multiple_of(r * width, 8), width), :] = 0.5 * (
                u0[k, base, :] + values[k]
            )
        return carry

    with jax.named_scope("final2"):
        lax.fori_loop(0, rows, section_two_row, 0)
    with jax.named_scope("drain"):
        to_larger = [2 * (groups - 1 - x) for x in range(groups)]
        to_same = [2 * (groups - x) for x in range(groups)]
        await_masses(to_larger, 0, level + 1, lambda copy: copy.wait_send())
        await_masses(to_same, level + 1, levels, lambda copy: copy.wait_send())
        wedge_all().wait_send()
        pl.when(place < last)(lambda: side_copy(0).wait_send())
        pl.when(place > 0)(lambda: side_copy(1).wait_send())
        wait_sent(first_halos)
        wait_sent(second_halos)


def put_out(advanced, enclosed, advanced_hbm, enclosed_hbm, sem):
    copies = [
        pltpu.make_async_copy(advanced, advanced_hbm, sem.at[0]),
        pltpu.make_async_copy(enclosed, enclosed_hbm, sem.at[1]),
    ]
    for copy in copies:
        copy.start()
    for copy in copies:
        copy.wait()


def body(groups, conserved, core_mass):
    _, rows, width, lanes = conserved.shape
    slabs, wedges = lax.axis_size("radial"), lax.axis_size("phi")
    inner = slabs // groups
    radial_step, theta_step, phi_step, timestep = step_sizes(rows * slabs, width * wedges, lanes)
    centers = (np.arange(lanes) + 0.5) * theta_step
    faces = (np.arange(lanes) + 1.0) * theta_step
    angles = np.zeros((8, lanes))
    angles[0] = np.sin(faces) * (0.5 / theta_step)
    angles[1] = 1.0 / np.sin(centers)
    angles[2] = np.cos(centers) / np.sin(centers)
    angles[3] = np.sin(centers)
    angles[4] = np.where(np.arange(lanes) == lanes - 1, 0.0, 0.5)
    angles[5] = np.where(np.arange(lanes) == 0, 0.0, 0.5)
    angles = jnp.asarray(angles.astype(np.float32))
    sizes = (rows, width, slabs, wedges, groups, radial_step, theta_step, phi_step, timestep)
    f32 = jnp.float32
    vmem = lambda *shape: pltpu.VMEM(shape, f32)
    dma = lambda count: pltpu.SemaphoreType.DMA((count,))
    in_hbm = lambda value: pltpu.with_memory_space_constraint(value, pltpu.HBM)
    cells = rows * width
    advanced, enclosed = pl.pallas_call(
        functools.partial(kernel, sizes),
        out_shape=(
            jax.ShapeDtypeStruct((NV, cells, lanes), f32),
            jax.ShapeDtypeStruct((1, rows), f32),
        ),
        in_specs=[
            pl.BlockSpec(memory_space=pltpu.HBM),
            pl.BlockSpec(memory_space=pltpu.HBM),
            pl.BlockSpec(memory_space=pltpu.HBM),
        ],
        out_specs=(
            pl.BlockSpec(memory_space=pltpu.VMEM),
            pl.BlockSpec(memory_space=pltpu.VMEM),
        ),
        scratch_shapes=[
            vmem(NV, cells + 16, lanes), vmem(NV, cells + 16, lanes),
            vmem(2, NV, 2 * width, lanes), vmem(2, NV, 2 * width, lanes),
            vmem(2, NV, 2, 8, lanes), vmem(2, NV, 2, 8, lanes),
            vmem(2, NV, 2, 8, lanes), vmem(2, NV, 2, 8, lanes),
            vmem(2, NV, 2 * width, lanes),
            vmem(NV, cells, lanes),
            vmem(NV, rows * (width + 8), lanes),
            vmem(NV, cells + width, lanes),
            vmem(NV, cells, lanes),
            vmem(NV, cells, lanes), vmem(NV, cells, lanes), vmem(NV, cells, lanes),
            vmem(slabs, 1, lanes), vmem(3, 1, lanes), vmem(wedges, 1, lanes),
            vmem(3, 8, lanes), vmem(16, lanes), vmem(8, lanes), pltpu.SMEM((1,), f32),
            dma(4), dma(8), dma(8), dma(inner // 2), dma(inner // 2), dma(2), dma(2),
            pltpu.SemaphoreType.DMA, pltpu.SemaphoreType.DMA,
            pltpu.SemaphoreType.REGULAR, pltpu.SemaphoreType.REGULAR,
        ],
        compiler_params=pltpu.CompilerParams(
            collective_id=0, has_side_effects=True, vmem_limit_bytes=12 << 20
        ),
    )(in_hbm(conserved.reshape(NV, cells, lanes)), core_mass, in_hbm(angles))
    advanced, enclosed = pl.pallas_call(
        put_out,
        out_shape=(
            jax.ShapeDtypeStruct((NV, cells, lanes), f32),
            jax.ShapeDtypeStruct((1, rows), f32),
        ),
        in_specs=[pl.BlockSpec(memory_space=pltpu.VMEM)] * 2,
        out_specs=[pl.BlockSpec(memory_space=pltpu.HBM)] * 2,
        scratch_shapes=[dma(2)],
        compiler_params=pltpu.CompilerParams(vmem_limit_bytes=4 << 20),
    )(advanced, enclosed)
    return advanced.reshape(conserved.shape), enclosed.reshape(rows)


def solution(mesh):
    in_specs = (P(None, "radial", "phi", None), P())
    out_specs = (P(None, "radial", "phi", None), P("radial"))
    return jax.shard_map(
        functools.partial(body, 4), mesh=mesh, in_specs=in_specs, out_specs=out_specs,
        check_vma=False,
    )
```

```python
import functools
import math

import jax
import jax.numpy as jnp
import numpy as np
from jax import lax
from jax.experimental import pallas as pl
from jax.experimental.pallas import tpu as pltpu
from jax.sharding import PartitionSpec as P

ADIABATIC = 4.0 / 3.0
INNER_RADIUS = 1.0
OUTER_RADIUS = 2.0
COURANT = 0.4
GRAVITY_KICK = 0.004
MINIMUM_DENSITY = 0.05
PRESSURE_FLOOR = 0.01

NV = 8
MESH = pl.DeviceIdType.MESH


def step_sizes(radial_total, phi_total, theta_total):
    theta_step = math.pi / theta_total
    phi_step = 2.0 * math.pi / phi_total
    polar_width = INNER_RADIUS * math.sin(0.5 * theta_step) * phi_step
    radial_step = min(2.0 * polar_width, (OUTER_RADIUS - INNER_RADIUS) / radial_total)
    timestep = COURANT * min(radial_step, polar_width)
    return (radial_step, theta_step, phi_step, timestep)


def half_slope(low, high):
    return jnp.maximum(jnp.minimum(low, high), jnp.minimum(jnp.maximum(low, high), 0.0))


def face_side(state, component):
    density = jnp.maximum(state[0], MINIMUM_DENSITY)
    inverse = 1.0 / density
    squares = state[1] * state[1] + state[2] * state[2] + state[3] * state[3]
    pressure = jnp.maximum(
        (ADIABATIC - 1.0) * (state[4] - 0.5 * squares * inverse), PRESSURE_FLOOR * density
    )
    normal = state[component] * inverse
    square = ADIABATIC * pressure * inverse
    sound = square * lax.rsqrt(square)
    return pressure, normal, jnp.abs(normal) + sound


def twice_flux(left, right, component):
    left_p, left_v, left_s = face_side(left, component)
    right_p, right_v, right_s = face_side(right, component)
    signal = jnp.maximum(left_s, right_s)
    left_w, right_w = left_v + signal, right_v - signal
    flux = [left[k] * left_w + right[k] * right_w for k in range(NV)]
    flux[component] = flux[component] + (left_p + right_p)
    flux[4] = flux[4] + (left_p * left_v + right_p * right_v)
    return flux


def edge_pair(cells, component):
    lefts, rights = [], []
    for k in range(NV):
        halves = [0.5 * (cells[i + 1][k] - cells[i][k]) for i in range(4)]
        slopes = [half_slope(halves[i], halves[i + 1]) for i in range(3)]
        lefts.append((cells[1][k] + slopes[0], cells[2][k] + slopes[1]))
        rights.append((cells[2][k] - slopes[1], cells[3][k] - slopes[2]))
    return [
        twice_flux([a[i] for a in lefts], [b[i] for b in rights], component) for i in range(2)
    ]


def sources(cells, cotangent):
    density = jnp.maximum(cells[0], MINIMUM_DENSITY)
    inverse = 1.0 / density
    speed = [None] + [cells[m] * inverse for m in (1, 2, 3)]
    squares = cells[1] * speed[1] + cells[2] * speed[2] + cells[3] * speed[3]
    pressure = jnp.maximum(
        (ADIABATIC - 1.0) * (cells[4] - 0.5 * squares), PRESSURE_FLOOR * density
    )
    spin = cells[3] * speed[3]
    source = [None] * NV
    source[1] = 2.0 * pressure + (cells[2] * speed[2] + spin)
    source[2] = (pressure + spin) * cotangent - cells[1] * speed[2]
    source[3] = -speed[3] * (cells[1] + cells[2] * cotangent)
    return source


def kernel(
    sizes, state_hbm, mass_hbm, angles_hbm,
    outv, enclosed_ref,
    u0, u1, hr0, hr1, hp0, hp1, pk0, pk1, sr, acc, fp, fr, sl, lt, rt, th,
    shared, below_above, wedge_rows, tab, grav, ct, core,
    in_sem, halo_send, halo_recv, shared_send, shared_recv, side_send, side_recv,
    wedge_send, wedge_recv, from_later,
):
    rows, width, slabs, wedges, groups, radial_step, theta_step, phi_step, timestep = sizes
    strength = GRAVITY_KICK / timestep
    place = lax.axis_index("radial")
    wedge = lax.axis_index("phi")
    inner = slabs // groups
    levels = inner // 2
    group, member = place // inner, lax.rem(place, inner)
    level, core_index = member // 2, lax.rem(member, 2)
    span = width + 8
    last = slabs - 1

    def at(radial, phi):
        return {"radial": radial, "phi": phi}

    def signal(semaphore, radial, phi):
        pl.semaphore_signal(semaphore, inc=1, device_id=at(radial, phi), device_id_type=MESH)

    east, west = lax.rem(wedge + 1, wedges), lax.rem(wedge + wedges - 1, wedges)

    fetch_mass = pltpu.make_async_copy(mass_hbm, core, in_sem.at[3])
    fetch_density = pltpu.make_async_copy(
        state_hbm.at[pl.ds(0, 1)], u0.at[pl.ds(0, 1), pl.ds(8, rows * width), :], in_sem.at[0]
    )
    fetch = pltpu.make_async_copy(
        state_hbm.at[pl.ds(1, NV - 1)], u0.at[pl.ds(1, NV - 1), pl.ds(8, rows * width), :],
        in_sem.at[1],
    )
    fetch_angles = pltpu.make_async_copy(angles_hbm, ct, in_sem.at[2])
    for copy in (fetch_density, fetch_angles, fetch, fetch_mass):
        copy.start()

    barrier = pltpu.get_barrier_semaphore()
    for step in range(1, wedges):
        signal(barrier, place, lax.rem(wedge + step, wedges))
    pl.when(place < last)(lambda: signal(barrier, place + 1, wedge))
    pl.when(place > 0)(lambda: signal(barrier, place - 1, wedge))

    def greet(x_start, x_stop, z_start, z_stop, semaphore):
        def one_level(z, carry):
            def one_group(x, inner_carry):
                for c in range(2):
                    signal(semaphore, x * inner + z * 2 + c, wedge)
                return inner_carry

            return lax.fori_loop(x_start, x_stop, one_group, carry)

        lax.fori_loop(z_start, z_stop, one_level, 0)

    middle = levels // 2
    early = level < middle

    def greet_after(semaphore):
        @pl.when(early)
        def _():
            greet(group + 1, groups, level, level + 1, semaphore)
            greet(0, groups, level + 1, levels, semaphore)

        @pl.when(jnp.logical_not(early))
        def _():
            greet(group, group + 1, level + 1, levels, semaphore)
            greet(group + 1, groups, middle, levels, semaphore)

    def greet_before(semaphore):
        @pl.when(early)
        def _():
            greet(0, group, level, level + 1, semaphore)
            greet(0, groups, 0, level, semaphore)

        @pl.when(jnp.logical_not(early))
        def _():
            greet(0, groups, 0, middle, semaphore)
            greet(0, group, middle, levels, semaphore)
            greet(group, group + 1, middle, level, semaphore)

    before_me = 2 * jnp.where(
        early,
        groups * level + group,
        groups * middle + group * (levels - middle) + level - middle,
    )
    after_me = 2 * (groups * levels - 1) - before_me
    greet_after(barrier)
    greetings = (
        wedges - 1 + before_me + jnp.where(place > 0, 1, 0) + jnp.where(place < last, 1, 0)
    )

    row = lax.broadcasted_iota(jnp.int32, (8, 128), 0)
    lane = lax.broadcasted_iota(jnp.int32, (8, 128), 1)
    first = place * rows

    def radius_of(index):
        return INNER_RADIUS + (index.astype(jnp.float32) + 0.5) * radial_step

    radius = radius_of(first + row)
    inverse_radius = 1.0 / radius
    low_face, high_face = radius - 0.5 * radial_step, radius + 0.5 * radial_step
    area = inverse_radius * inverse_radius * (0.5 * timestep / radial_step)
    tab[0] = timestep * inverse_radius
    tab[1] = low_face * low_face * area
    tab[2] = high_face * high_face * area

    with jax.named_scope("fetch_wait"):
        fetch_angles.wait()
        fetch_density.wait()
    total = u0[0, pl.ds(8, 8, stride=width), :]
    for f in range(1, width):
        total = total + u0[0, pl.ds(8 + f, 8, stride=width), :]
    shells = jnp.sum(total * ct[3:4, :], axis=1, keepdims=True) * (
        radius * radius * (radial_step * theta_step * phi_step)
    )
    wedge_rows[0] = jnp.sum(jnp.where(lane == row, shells, 0.0), axis=0, keepdims=True)
    fetch.wait()

    def pack(source, packed):
        for side, zones in enumerate(((width - 2, width - 1), (0, 1))):
            for k in range(NV):
                for i, zone in enumerate(zones):
                    packed[side, k, i] = source[k, pl.ds(8 + zone, 8, stride=width), :]

    pack(u0, pk0)
    with jax.named_scope("barrier_wait"):
        pl.semaphore_wait(barrier, greetings)

    def copy_of(source, target, send, recv, radial, phi):
        return pltpu.make_async_remote_copy(
            src_ref=source, dst_ref=target, send_sem=send, recv_sem=recv,
            device_id=at(radial, phi), device_id_type=MESH,
        )

    def mass_copy(source, x, z, c):
        return copy_of(
            source, shared.at[level * 2 * groups + group * 2 + core_index],
            shared_send.at[z], shared_recv.at[level], x * inner + z * 2 + c, wedge,
        )

    def send_masses(source, x_start, z_start, z_stop):
        def one_group(x, carry):
            def one_level(z, inner_carry):
                for c in range(2):
                    mass_copy(source, x, z, c).start()
                return inner_carry

            return lax.fori_loop(z_start, z_stop, one_level, carry)

        lax.fori_loop(x_start, groups, one_group, 0)

    def many(count, z):
        rows_of = shared.at[pl.ds(z * 2 * groups, count)]
        return copy_of(rows_of, rows_of, shared_send.at[z], shared_recv.at[z], place, wedge)

    def await_masses(counts, z_start, z_stop, act):
        for x in range(groups):
            if counts[x]:

                @pl.when(group == x)
                def _(count=counts[x]):
                    def one_level(z, carry):
                        act(many(count, z))
                        return carry

                    lax.fori_loop(z_start, z_stop, one_level, 0)

    def wedge_copy(step):
        return copy_of(
            wedge_rows.at[0], wedge_rows.at[step], wedge_send, wedge_recv, place,
            lax.rem(wedge + step, wedges),
        )

    def wedge_all():
        others = wedge_rows.at[pl.ds(1, wedges - 1)]
        return copy_of(others, others, wedge_send, wedge_recv, place, east)

    def side_copy(side):
        target = jnp.minimum(place + 1, last) if side == 0 else jnp.maximum(place - 1, 0)
        return copy_of(
            below_above.at[2], below_above.at[side], side_send.at[side], side_recv.at[side],
            target, wedge,
        )

    for step in range(1, wedges):
        wedge_copy(step).start()

    def halo_copies(number, high_rows, low_rows, packed, radial_halo, phi_halo):
        def copy(which, source, target, peer):
            return pltpu.make_async_remote_copy(
                src_ref=source, dst_ref=target, send_sem=halo_send.at[4 * number + which],
                recv_sem=halo_recv.at[4 * number + which], device_id=peer, device_id_type=MESH,
            )

        return (
            copy(0, high_rows, radial_halo.at[0], at(jnp.minimum(place + 1, last), wedge)),
            copy(1, low_rows, radial_halo.at[1], at(jnp.maximum(place - 1, 0), wedge)),
            copy(2, packed.at[0], phi_halo.at[0], at(place, east)),
            copy(3, packed.at[1], phi_halo.at[1], at(place, west)),
        )

    def start_halos(copies, radial_halo, low_row, high_row):
        pl.when(place < last)(lambda: copies[0].start())
        pl.when(place > 0)(lambda: copies[1].start())
        copies[2].start()
        copies[3].start()

        @pl.when(place == 0)
        def _():
            for k in range(NV):
                for i in range(2):
                    radial_halo[0, k, pl.ds(width * i, width), :] = low_row(k)

        @pl.when(place == last)
        def _():
            for k in range(NV):
                for i in range(2):
                    radial_halo[1, k, pl.ds(width * i, width), :] = high_row(k)

    def wait_radial(copies):
        pl.when(place > 0)(lambda: copies[0].wait_recv())
        pl.when(place < last)(lambda: copies[1].wait_recv())

    def wait_sent(copies):
        pl.when(place < last)(lambda: copies[0].wait_send())
        pl.when(place > 0)(lambda: copies[1].wait_send())
        copies[2].wait_send()
        copies[3].wait_send()

    first_halos = halo_copies(
        0, u0.at[:, pl.ds(8 + (rows - 2) * width, 2 * width), :], u0.at[:, pl.ds(8, 2 * width), :],
        pk0, hr0, hp0,
    )
    start_halos(
        first_halos, hr0,
        lambda k: u0[k, pl.ds(8, width), :],
        lambda k: u0[k, pl.ds(8 + (rows - 1) * width, width), :],
    )

    greet_before(from_later)

    wide_lane = lax.broadcasted_iota(jnp.int32, (width, 128), 1)

    def polar_and_azimuth(u):
        def one_step(i, carry):
            sine, inverse_sine, cotangent, mask = ct[0:1, :], ct[1:2, :], ct[2:3, :], ct[4:5, :]
            r = jnp.maximum(i - 2, 0)
            store = pl.ds(pl.multiple_of(r * width, 8), width)
            scale = tab[0, pl.ds(r, 1), :]
            cells = [u[k, pl.ds(pl.multiple_of(8 + r * width, 8), width), :] for k in range(NV)]
            source = sources(cells, cotangent)
            for k in range(NV):
                through = th[k, store, :]
                change = (pltpu.roll(through, 1, 1) - through) * inverse_sine
                if source[k] is not None:
                    change = change + source[k]
                acc[k, store, :] = cells[k] + scale * change
            r = jnp.clip(i - 1, 0, rows - 1)
            store = pl.ds(pl.multiple_of(r * width, 8), width)
            left = [lt[k, store, :] for k in range(NV)]
            right = []
            for k in range(NV):
                value = rt[k, store, :]
                cell = u[k, pl.ds(pl.multiple_of(8 + r * width, 8), width), :]
                right.append(jnp.where(wide_lane == 127, cell, pltpu.roll(value, 127, 1)))
            flux = twice_flux(left, right, 2)
            for k in range(NV):
                th[k, store, :] = flux[k] * sine
            r = jnp.minimum(i, rows - 1)
            base = pl.multiple_of(8 + r * width, 8)
            store = pl.ds(pl.multiple_of(r * width, 8), width)
            cells = [u[k, pl.ds(base, width), :] for k in range(NV)]
            for k in range(NV):
                high = (pltpu.roll(cells[k], 127, 1) - cells[k]) * mask
                low = (cells[k] - pltpu.roll(cells[k], 1, 1)) * ct[5:6, :]
                slope = half_slope(low, high)
                lt[k, store, :] = cells[k] + slope
                rt[k, store, :] = cells[k] - slope
            left, right = [], []
            for k in range(NV):
                low = 0.5 * (cells[k] - u[k, pl.ds(base - 1, width), :])
                high = 0.5 * (u[k, pl.ds(base + 1, width), :] - cells[k])
                slope = half_slope(low, high)
                left.append(pltpu.roll(cells[k] + slope, 1, 0))
                right.append(cells[k] - slope)
            flux = twice_flux(left, right, 3)
            for k in range(NV):
                fp[k, pl.ds(pl.multiple_of(r * span, 8), width), :] = flux[k]
            return carry

        lax.fori_loop(0, rows + 2, one_step, 0)

    def inner_radial(u):
        def one_row(r, carry):
            base = pl.multiple_of(8 + r * width, 8)
            store = pl.multiple_of(r * width, 8)
            right = []
            left = []
            for k in range(NV):
                cell = u[k, pl.ds(base, width), :]
                low = 0.5 * (cell - u[k, pl.ds(base - width, width), :])
                high = 0.5 * (u[k, pl.ds(base + width, width), :] - cell)
                slope = half_slope(low, high)
                right.append(cell - slope)
                left.append(sl[k, pl.ds(store - width, width), :])
                sl[k, pl.ds(store, width), :] = cell + slope
            flux = twice_flux(left, right, 1)
            for k in range(NV):
                fr[k, pl.ds(store, width), :] = flux[k]
            return carry

        lax.fori_loop(1, rows - 1, one_row, 0)

    def edge_azimuth(u, halo):
        for side in range(2):
            own = (0, 1, 2) if side == 0 else (width - 3, width - 2, width - 1)
            inside = [
                [u[k, pl.ds(8 + f, 8, stride=width), :] for k in range(NV)] for f in own
            ]
            outside = [[halo[side, k, i] for k in range(NV)] for i in range(2)]
            cells = outside + inside if side == 0 else inside + outside
            fluxes = edge_pair(cells, 3)
            faces = (0, 1) if side == 0 else (width - 1, width)
            for face, flux in zip(faces, fluxes):
                for k in range(NV):
                    fp[k, pl.ds(face, 8, stride=span), :] = flux[k]

    def edge_radial(u, halo):
        for side in range(2):
            own = (0, 1, 2) if side == 0 else (rows - 3, rows - 2, rows - 1)
            inside = [[u[k, pl.ds(8 + r * width, width), :] for k in range(NV)] for r in own]
            outside = [
                [halo[side, k, pl.ds(width * i, width), :] for k in range(NV)] for i in range(2)
            ]
            cells = outside + inside if side == 0 else inside + outside
            fluxes = edge_pair(cells, 1)
            faces = (0, 1) if side == 0 else (rows - 1, rows)
            for face, flux in zip(faces, fluxes):
                for k in range(NV):
                    fr[k, pl.ds(face * width, width), :] = flux[k]

    azimuth_scale = 0.5 / phi_step

    def advanced_row(r):
        store = pl.multiple_of(r * width, 8)
        low_area, high_area = tab[1, pl.ds(r, 1), :], tab[2, pl.ds(r, 1), :]
        across = tab[0, pl.ds(r, 1), :] * ct[1:2, :] * azimuth_scale
        below = pl.multiple_of(r * span, 8)
        values = []
        for k in range(NV):
            values.append(
                acc[k, pl.ds(store, width), :]
                + across * (fp[k, pl.ds(below, width), :] - fp[k, pl.ds(below + 1, width), :])
                + low_area * fr[k, pl.ds(store, width), :]
                - high_area * fr[k, pl.ds(pl.multiple_of(store + width, 8), width), :]
            )
        return values

    with jax.named_scope("pre1"):
        polar_and_azimuth(u0)
    with jax.named_scope("rad1"):
        inner_radial(u0)

    with jax.named_scope("wedge_wait"):
        wedge_all().wait_recv()
    shell_row = wedge_rows[0]
    for j in range(1, wedges):
        shell_row = shell_row + wedge_rows[j]
    below_above[2] = shell_row
    pl.when(place < last)(lambda: side_copy(0).start())
    pl.when(place > 0)(lambda: side_copy(1).start())
    send_masses(below_above.at[2], group + 1, 0, jnp.minimum(level, middle))

    with jax.named_scope("h1_phi_wait"):
        first_halos[2].wait_recv()
        first_halos[3].wait_recv()
    with jax.named_scope("edge_phi1"):
        edge_azimuth(u0, hp0)
    with jax.named_scope("h1_rad_wait"):
        wait_radial(first_halos)
    with jax.named_scope("edge_rad1"):
        edge_radial(u0, hr0)

    def section_one_row(r, carry):
        values = advanced_row(r)
        for k in range(NV):
            u1[k, pl.ds(pl.multiple_of(8 + r * width, 8), width), :] = values[k]
        return carry

    with jax.named_scope("final1"):
        lax.fori_loop(0, rows, section_one_row, 0)
    pack(u1, pk1)
    for k in range(NV):
        sr[0, k] = u1[k, pl.ds(8 + (rows - 2) * width, 2 * width), :]
        sr[1, k] = u1[k, pl.ds(8, 2 * width), :]
    second_halos = halo_copies(1, sr.at[0], sr.at[1], pk1, hr1, hp1)
    start_halos(
        second_halos, hr1,
        lambda k: sr[1, k, pl.ds(0, width), :],
        lambda k: sr[0, k, pl.ds(width, width), :],
    )

    with jax.named_scope("asc_wait"):
        pl.when(after_me > 0)(lambda: pl.semaphore_wait(from_later, after_me))
    send_masses(below_above.at[2], group + 1, jnp.minimum(level, middle), level + 1)
    send_masses(below_above.at[2], group, level + 1, levels)

    from_all = [2 * x for x in range(groups)]
    from_lower = [2 * x + 2 for x in range(groups)]

    def mass_between(z_start, z_stop, count):
        def one_level(z, value):
            part = shared[pl.ds(z * 2 * groups, 2 * groups)]
            return value + jnp.sum(jnp.where(slot < count, part, 0.0), axis=0)

        return lax.fori_loop(z_start, z_stop, one_level, jnp.zeros((1, 128), jnp.float32))

    slot = lax.broadcasted_iota(jnp.int32, (2 * groups, 1, 128), 0)
    with jax.named_scope("m1_wait"):
        await_masses(from_all, level, levels, lambda copy: copy.wait_recv())
        await_masses(from_lower, 0, level, lambda copy: copy.wait_recv())
        pl.when(place > 0)(lambda: side_copy(0).wait_recv())
        pl.when(place < last)(lambda: side_copy(1).wait_recv())
    below, above, own = below_above[0], below_above[1], below_above[2]
    half_of = lambda index: jnp.where(lane < index, 1.0, jnp.where(lane == index, 0.5, 0.0))
    none = jnp.zeros((8, 128), jnp.float32)
    lower = jnp.where(row < 2, jnp.where(place == 0, half_of(0), none), 0.0)
    upper = jnp.where(row < 2, none, jnp.where(place == last, half_of(rows - 1), 1.0))
    minus = jnp.where(lane >= rows, 0.0, half_of(rows - 2 + row) - 1.0)
    minus = jnp.where(row < 2, minus, none)
    plus = jnp.where(row < 2, none, half_of(row - 2))
    inside = (
        mass_between(level, levels, 2 * group)
        + mass_between(0, level, 2 * group + 2)
        + jnp.where(core_index == 1, below, 0.0)
    )
    table = (
        inside + half_of(row) * own,
        inside
        + (lower + upper) * own
        + jnp.where(place > 0, minus * below, none)
        + jnp.where(place < last, plus * above, none),
    )
    beyond = jnp.clip(first + jnp.where(row < 2, row - 2, rows - 2 + row), 0, slabs * rows - 1)
    fetch_mass.wait()
    for i, target in enumerate((first + row, beyond)):
        enclosed = jnp.sum(table[i], axis=1, keepdims=True) + core[0]
        inverse = 1.0 / radius_of(target)
        grav[8 * i : 8 * i + 8, :] = (timestep * strength) * enclosed * inverse * inverse
        if i == 0:
            enclosed_ref[...] = jnp.sum(
                jnp.where(lane == row, enclosed, 0.0), axis=0, keepdims=True
            )[:, :rows]

    def gravity_row(r, carry):
        base = pl.ds(pl.multiple_of(8 + r * width, 8), width)
        pull = grav[pl.ds(r, 1), :]
        u1[1, base, :] = u1[1, base, :] - pull * jnp.maximum(u0[0, base, :], MINIMUM_DENSITY)
        u1[4, base, :] = u1[4, base, :] - pull * u0[1, base, :]
        return carry

    with jax.named_scope("grav"):
        lax.fori_loop(0, rows, gravity_row, 0)

    with jax.named_scope("pre2"):
        polar_and_azimuth(u1)
    with jax.named_scope("rad2"):
        inner_radial(u1)
    with jax.named_scope("h2_phi_wait"):
        second_halos[2].wait_recv()
        second_halos[3].wait_recv()
    pull = grav[0:8, :]
    for side in range(2):
        for i in range(2):
            hp1[side, 1, i] = hp1[side, 1, i] - pull * jnp.maximum(
                hp0[side, 0, i], MINIMUM_DENSITY
            )
            hp1[side, 4, i] = hp1[side, 4, i] - pull * hp0[side, 1, i]
    with jax.named_scope("edge_phi2"):
        edge_azimuth(u1, hp1)
    with jax.named_scope("h2_rad_wait"):
        wait_radial(second_halos)
    for side in range(2):
        for i in range(2):
            which = pl.ds(width * i, width)
            pull = grav[8 + 2 * side + i : 9 + 2 * side + i, :]
            hr1[side, 1, which, :] = hr1[side, 1, which, :] - pull * jnp.maximum(
                hr0[side, 0, which, :], MINIMUM_DENSITY
            )
            hr1[side, 4, which, :] = hr1[side, 4, which, :] - pull * hr0[side, 1, which, :]
    with jax.named_scope("edge_rad2"):
        edge_radial(u1, hr1)

    def section_two_row(r, carry):
        values = advanced_row(r)
        base = pl.ds(pl.multiple_of(8 + r * width, 8), width)
        pull = grav[pl.ds(r, 1), :]
        values[1] = values[1] - pull * jnp.maximum(u1[0, base, :], MINIMUM_DENSITY)
        values[4] = values[4] - pull * u1[1, base, :]
        for k in range(NV):
            outv[k, pl.ds(pl.multiple_of(r * width, 8), width), :] = 0.5 * (
                u0[k, base, :] + values[k]
            )
        return carry

    with jax.named_scope("final2"):
        lax.fori_loop(0, rows, section_two_row, 0)
    with jax.named_scope("drain"):
        to_larger = [2 * (groups - 1 - x) for x in range(groups)]
        to_same = [2 * (groups - x) for x in range(groups)]
        await_masses(to_larger, 0, level + 1, lambda copy: copy.wait_send())
        await_masses(to_same, level + 1, levels, lambda copy: copy.wait_send())
        wedge_all().wait_send()
        pl.when(place < last)(lambda: side_copy(0).wait_send())
        pl.when(place > 0)(lambda: side_copy(1).wait_send())
        wait_sent(first_halos)
        wait_sent(second_halos)


def put_out(advanced, enclosed, advanced_hbm, enclosed_hbm, sem):
    copies = [
        pltpu.make_async_copy(advanced, advanced_hbm, sem.at[0]),
        pltpu.make_async_copy(enclosed, enclosed_hbm, sem.at[1]),
    ]
    for copy in copies:
        copy.start()
    for copy in copies:
        copy.wait()


def body(groups, conserved, core_mass):
    _, rows, width, lanes = conserved.shape
    slabs, wedges = lax.axis_size("radial"), lax.axis_size("phi")
    inner = slabs // groups
    radial_step, theta_step, phi_step, timestep = step_sizes(rows * slabs, width * wedges, lanes)
    centers = (np.arange(lanes) + 0.5) * theta_step
    faces = (np.arange(lanes) + 1.0) * theta_step
    angles = np.zeros((8, lanes))
    angles[0] = np.sin(faces) * (0.5 / theta_step)
    angles[1] = 1.0 / np.sin(centers)
    angles[2] = np.cos(centers) / np.sin(centers)
    angles[3] = np.sin(centers)
    angles[4] = np.where(np.arange(lanes) == lanes - 1, 0.0, 0.5)
    angles[5] = np.where(np.arange(lanes) == 0, 0.0, 0.5)
    angles = jnp.asarray(angles.astype(np.float32))
    sizes = (rows, width, slabs, wedges, groups, radial_step, theta_step, phi_step, timestep)
    f32 = jnp.float32
    vmem = lambda *shape: pltpu.VMEM(shape, f32)
    dma = lambda count: pltpu.SemaphoreType.DMA((count,))
    in_hbm = lambda value: pltpu.with_memory_space_constraint(value, pltpu.HBM)
    cells = rows * width
    advanced, enclosed = pl.pallas_call(
        functools.partial(kernel, sizes),
        out_shape=(
            jax.ShapeDtypeStruct((NV, cells, lanes), f32),
            jax.ShapeDtypeStruct((1, rows), f32),
        ),
        in_specs=[
            pl.BlockSpec(memory_space=pltpu.HBM),
            pl.BlockSpec(memory_space=pltpu.HBM),
            pl.BlockSpec(memory_space=pltpu.HBM),
        ],
        out_specs=(
            pl.BlockSpec(memory_space=pltpu.VMEM),
            pl.BlockSpec(memory_space=pltpu.VMEM),
        ),
        scratch_shapes=[
            vmem(NV, cells + 16, lanes), vmem(NV, cells + 16, lanes),
            vmem(2, NV, 2 * width, lanes), vmem(2, NV, 2 * width, lanes),
            vmem(2, NV, 2, 8, lanes), vmem(2, NV, 2, 8, lanes),
            vmem(2, NV, 2, 8, lanes), vmem(2, NV, 2, 8, lanes),
            vmem(2, NV, 2 * width, lanes),
            vmem(NV, cells, lanes),
            vmem(NV, rows * (width + 8), lanes),
            vmem(NV, cells + width, lanes),
            vmem(NV, cells, lanes),
            vmem(NV, cells, lanes), vmem(NV, cells, lanes), vmem(NV, cells, lanes),
            vmem(slabs, 1, lanes), vmem(3, 1, lanes), vmem(wedges, 1, lanes),
            vmem(3, 8, lanes), vmem(16, lanes), vmem(8, lanes), pltpu.SMEM((1,), f32),
            dma(4), dma(8), dma(8), dma(inner // 2), dma(inner // 2), dma(2), dma(2),
            pltpu.SemaphoreType.DMA, pltpu.SemaphoreType.DMA,
            pltpu.SemaphoreType.REGULAR,
        ],
        compiler_params=pltpu.CompilerParams(
            collective_id=0, has_side_effects=True, vmem_limit_bytes=12 << 20
        ),
    )(in_hbm(conserved.reshape(NV, cells, lanes)), core_mass, in_hbm(angles))
    advanced, enclosed = pl.pallas_call(
        put_out,
        out_shape=(
            jax.ShapeDtypeStruct((NV, cells, lanes), f32),
            jax.ShapeDtypeStruct((1, rows), f32),
        ),
        in_specs=[pl.BlockSpec(memory_space=pltpu.VMEM)] * 2,
        out_specs=[pl.BlockSpec(memory_space=pltpu.HBM)] * 2,
        scratch_shapes=[dma(2)],
        compiler_params=pltpu.CompilerParams(vmem_limit_bytes=4 << 20),
    )(advanced, enclosed)
    return advanced.reshape(conserved.shape), enclosed.reshape(rows)


def solution(mesh):
    in_specs = (P(None, "radial", "phi", None), P())
    out_specs = (P(None, "radial", "phi", None), P("radial"))
    return jax.shard_map(
        functools.partial(body, 4), mesh=mesh, in_specs=in_specs, out_specs=out_specs,
        check_vma=False,
    )
```

```python
import functools
import math

import jax
import jax.numpy as jnp
import numpy as np
from jax import lax
from jax.experimental import pallas as pl
from jax.experimental.pallas import tpu as pltpu
from jax.sharding import PartitionSpec as P

ADIABATIC = 4.0 / 3.0
INNER_RADIUS = 1.0
OUTER_RADIUS = 2.0
COURANT = 0.4
GRAVITY_KICK = 0.004
MINIMUM_DENSITY = 0.05
PRESSURE_FLOOR = 0.01

NV = 8
STEADY = (0, 2, 3, 5, 6, 7)
MOVED = (1, 4)
MESH = pl.DeviceIdType.MESH


def step_sizes(radial_total, phi_total, theta_total):
    theta_step = math.pi / theta_total
    phi_step = 2.0 * math.pi / phi_total
    polar_width = INNER_RADIUS * math.sin(0.5 * theta_step) * phi_step
    radial_step = min(2.0 * polar_width, (OUTER_RADIUS - INNER_RADIUS) / radial_total)
    timestep = COURANT * min(radial_step, polar_width)
    return (radial_step, theta_step, phi_step, timestep)


def half_slope(low, high):
    return jnp.maximum(jnp.minimum(low, high), jnp.minimum(jnp.maximum(low, high), 0.0))


def face_side(state, component, ready=None):
    density = jnp.maximum(state[0], MINIMUM_DENSITY)
    if ready is None:
        inverse, squares = 1.0 / density, state[2] * state[2] + state[3] * state[3]
    else:
        inverse, squares = ready
    squares = state[1] * state[1] + squares
    pressure = jnp.maximum(
        (ADIABATIC - 1.0) * (state[4] - 0.5 * squares * inverse), PRESSURE_FLOOR * density
    )
    normal = state[component] * inverse
    square = ADIABATIC * pressure * inverse
    sound = square * lax.rsqrt(square)
    return pressure, normal, jnp.abs(normal) + sound


def twice_flux(left, right, component, ready=(None, None)):
    left_p, left_v, left_s = face_side(left, component, ready[0])
    right_p, right_v, right_s = face_side(right, component, ready[1])
    signal = jnp.maximum(left_s, right_s)
    left_w, right_w = left_v + signal, right_v - signal
    flux = [left[k] * left_w + right[k] * right_w for k in range(NV)]
    flux[component] = flux[component] + (left_p + right_p)
    flux[4] = flux[4] + (left_p * left_v + right_p * right_v)
    return flux


def edge_pair(cells, component):
    lefts, rights = [], []
    for k in range(NV):
        halves = [0.5 * (cells[i + 1][k] - cells[i][k]) for i in range(4)]
        slopes = [half_slope(halves[i], halves[i + 1]) for i in range(3)]
        lefts.append((cells[1][k] + slopes[0], cells[2][k] + slopes[1]))
        rights.append((cells[2][k] - slopes[1], cells[3][k] - slopes[2]))
    return [
        twice_flux([a[i] for a in lefts], [b[i] for b in rights], component) for i in range(2)
    ]


def sources(cells, cotangent):
    density = jnp.maximum(cells[0], MINIMUM_DENSITY)
    inverse = 1.0 / density
    speed = [None] + [cells[m] * inverse for m in (1, 2, 3)]
    squares = cells[1] * speed[1] + cells[2] * speed[2] + cells[3] * speed[3]
    pressure = jnp.maximum(
        (ADIABATIC - 1.0) * (cells[4] - 0.5 * squares), PRESSURE_FLOOR * density
    )
    spin = cells[3] * speed[3]
    source = [None] * NV
    source[1] = 2.0 * pressure + (cells[2] * speed[2] + spin)
    source[2] = (pressure + spin) * cotangent - cells[1] * speed[2]
    source[3] = -speed[3] * (cells[1] + cells[2] * cotangent)
    return source


def kernel(
    sizes, state_hbm, mass_hbm, angles_hbm,
    outv, enclosed_ref,
    u0, u1, hr0, hr1, hp0, hp1, pk0, pk1, sr, acc, fp, fr, sl, lt, rt, th, prep,
    shared, below_above, wedge_rows, tab, grav, ct, core,
    in_sem, halo_send, halo_recv, shared_send, shared_recv, side_send, side_recv,
    wedge_send, wedge_recv, from_later,
):
    rows, width, slabs, wedges, groups, radial_step, theta_step, phi_step, timestep = sizes
    strength = GRAVITY_KICK / timestep
    place = lax.axis_index("radial")
    wedge = lax.axis_index("phi")
    inner = slabs // groups
    levels = inner // 2
    group, member = place // inner, lax.rem(place, inner)
    level, core_index = member // 2, lax.rem(member, 2)
    span = width + 8
    last = slabs - 1

    def at(radial, phi):
        return {"radial": radial, "phi": phi}

    def signal(semaphore, radial, phi):
        pl.semaphore_signal(semaphore, inc=1, device_id=at(radial, phi), device_id_type=MESH)

    east, west = lax.rem(wedge + 1, wedges), lax.rem(wedge + wedges - 1, wedges)

    fetch_mass = pltpu.make_async_copy(mass_hbm, core, in_sem.at[3])
    fetch_density = pltpu.make_async_copy(
        state_hbm.at[pl.ds(0, 1)], u0.at[pl.ds(0, 1), pl.ds(8, rows * width), :], in_sem.at[0]
    )
    fetch = pltpu.make_async_copy(
        state_hbm.at[pl.ds(1, NV - 1)], u0.at[pl.ds(1, NV - 1), pl.ds(8, rows * width), :],
        in_sem.at[1],
    )
    fetch_angles = pltpu.make_async_copy(angles_hbm, ct, in_sem.at[2])
    for copy in (fetch_density, fetch_angles, fetch, fetch_mass):
        copy.start()

    barrier = pltpu.get_barrier_semaphore()
    for step in range(1, wedges):
        signal(barrier, place, lax.rem(wedge + step, wedges))
    pl.when(place < last)(lambda: signal(barrier, place + 1, wedge))
    pl.when(place > 0)(lambda: signal(barrier, place - 1, wedge))

    def greet(x_start, x_stop, z_start, z_stop, semaphore):
        def one_level(z, carry):
            def one_group(x, inner_carry):
                for c in range(2):
                    signal(semaphore, x * inner + z * 2 + c, wedge)
                return inner_carry

            return lax.fori_loop(x_start, x_stop, one_group, carry)

        lax.fori_loop(z_start, z_stop, one_level, 0)

    middle = levels // 2
    early = level < middle

    def greet_after(semaphore):
        @pl.when(early)
        def _():
            greet(group + 1, groups, level, level + 1, semaphore)
            greet(0, groups, level + 1, levels, semaphore)

        @pl.when(jnp.logical_not(early))
        def _():
            greet(group, group + 1, level + 1, levels, semaphore)
            greet(group + 1, groups, middle, levels, semaphore)

    def greet_before(semaphore):
        @pl.when(early)
        def _():
            greet(0, group, level, level + 1, semaphore)
            greet(0, groups, 0, level, semaphore)

        @pl.when(jnp.logical_not(early))
        def _():
            greet(0, groups, 0, middle, semaphore)
            greet(0, group, middle, levels, semaphore)
            greet(group, group + 1, middle, level, semaphore)

    before_me = 2 * jnp.where(
        early,
        groups * level + group,
        groups * middle + group * (levels - middle) + level - middle,
    )
    after_me = 2 * (groups * levels - 1) - before_me
    greet_after(barrier)
    greetings = (
        wedges - 1 + before_me + jnp.where(place > 0, 1, 0) + jnp.where(place < last, 1, 0)
    )

    row = lax.broadcasted_iota(jnp.int32, (8, 128), 0)
    lane = lax.broadcasted_iota(jnp.int32, (8, 128), 1)
    first = place * rows

    def radius_of(index):
        return INNER_RADIUS + (index.astype(jnp.float32) + 0.5) * radial_step

    radius = radius_of(first + row)
    inverse_radius = 1.0 / radius
    low_face, high_face = radius - 0.5 * radial_step, radius + 0.5 * radial_step
    area = inverse_radius * inverse_radius * (0.5 * timestep / radial_step)
    tab[0] = timestep * inverse_radius
    tab[1] = low_face * low_face * area
    tab[2] = high_face * high_face * area

    with jax.named_scope("fetch_wait"):
        fetch_angles.wait()
        fetch_density.wait()
    total = u0[0, pl.ds(8, 8, stride=width), :]
    for f in range(1, width):
        total = total + u0[0, pl.ds(8 + f, 8, stride=width), :]
    shells = jnp.sum(total * ct[3:4, :], axis=1, keepdims=True) * (
        radius * radius * (radial_step * theta_step * phi_step)
    )
    wedge_rows[0] = jnp.sum(jnp.where(lane == row, shells, 0.0), axis=0, keepdims=True)
    fetch.wait()

    def pack(source, packed):
        for side, zones in enumerate(((width - 2, width - 1), (0, 1))):
            for k in range(NV):
                for i, zone in enumerate(zones):
                    packed[side, k, i] = source[k, pl.ds(8 + zone, 8, stride=width), :]

    pack(u0, pk0)
    with jax.named_scope("barrier_wait"):
        pl.semaphore_wait(barrier, greetings)

    def copy_of(source, target, send, recv, radial, phi):
        return pltpu.make_async_remote_copy(
            src_ref=source, dst_ref=target, send_sem=send, recv_sem=recv,
            device_id=at(radial, phi), device_id_type=MESH,
        )

    def mass_copy(source, x, z, c):
        return copy_of(
            source, shared.at[level * 2 * groups + group * 2 + core_index],
            shared_send.at[z], shared_recv.at[level], x * inner + z * 2 + c, wedge,
        )

    def send_masses(source, x_start, z_start, z_stop):
        def one_group(x, carry):
            def one_level(z, inner_carry):
                for c in range(2):
                    mass_copy(source, x, z, c).start()
                return inner_carry

            return lax.fori_loop(z_start, z_stop, one_level, carry)

        lax.fori_loop(x_start, groups, one_group, 0)

    def many(count, z):
        rows_of = shared.at[pl.ds(z * 2 * groups, count)]
        return copy_of(rows_of, rows_of, shared_send.at[z], shared_recv.at[z], place, wedge)

    def await_masses(counts, z_start, z_stop, act):
        for x in range(groups):
            if counts[x]:

                @pl.when(group == x)
                def _(count=counts[x]):
                    def one_level(z, carry):
                        act(many(count, z))
                        return carry

                    lax.fori_loop(z_start, z_stop, one_level, 0)

    def wedge_copy(step):
        return copy_of(
            wedge_rows.at[0], wedge_rows.at[step], wedge_send, wedge_recv, place,
            lax.rem(wedge + step, wedges),
        )

    def wedge_all():
        others = wedge_rows.at[pl.ds(1, wedges - 1)]
        return copy_of(others, others, wedge_send, wedge_recv, place, east)

    def side_copy(side):
        target = jnp.minimum(place + 1, last) if side == 0 else jnp.maximum(place - 1, 0)
        return copy_of(
            below_above.at[2], below_above.at[side], side_send.at[side], side_recv.at[side],
            target, wedge,
        )

    for step in range(1, wedges):
        wedge_copy(step).start()

    def halo_copies(number, high_rows, low_rows, packed, radial_halo, phi_halo):
        def copy(which, source, target, peer):
            return pltpu.make_async_remote_copy(
                src_ref=source, dst_ref=target, send_sem=halo_send.at[4 * number + which],
                recv_sem=halo_recv.at[4 * number + which], device_id=peer, device_id_type=MESH,
            )

        return (
            copy(0, high_rows, radial_halo.at[0], at(jnp.minimum(place + 1, last), wedge)),
            copy(1, low_rows, radial_halo.at[1], at(jnp.maximum(place - 1, 0), wedge)),
            copy(2, packed.at[0], phi_halo.at[0], at(place, east)),
            copy(3, packed.at[1], phi_halo.at[1], at(place, west)),
        )

    def start_halos(copies, radial_halo, low_row, high_row):
        pl.when(place < last)(lambda: copies[0].start())
        pl.when(place > 0)(lambda: copies[1].start())
        copies[2].start()
        copies[3].start()

        @pl.when(place == 0)
        def _():
            for k in range(NV):
                for i in range(2):
                    radial_halo[0, k, pl.ds(width * i, width), :] = low_row(k)

        @pl.when(place == last)
        def _():
            for k in range(NV):
                for i in range(2):
                    radial_halo[1, k, pl.ds(width * i, width), :] = high_row(k)

    def wait_radial(copies):
        pl.when(place > 0)(lambda: copies[0].wait_recv())
        pl.when(place < last)(lambda: copies[1].wait_recv())

    def wait_sent(copies):
        pl.when(place < last)(lambda: copies[0].wait_send())
        pl.when(place > 0)(lambda: copies[1].wait_send())
        copies[2].wait_send()
        copies[3].wait_send()

    first_halos = halo_copies(
        0, u0.at[:, pl.ds(8 + (rows - 2) * width, 2 * width), :], u0.at[:, pl.ds(8, 2 * width), :],
        pk0, hr0, hp0,
    )
    start_halos(
        first_halos, hr0,
        lambda k: u0[k, pl.ds(8, width), :],
        lambda k: u0[k, pl.ds(8 + (rows - 1) * width, width), :],
    )

    greet_before(from_later)

    wide_lane = lax.broadcasted_iota(jnp.int32, (width, 128), 1)

    def keep(direction, side, where, state):
        for n, k in enumerate(STEADY):
            prep[direction, side, n, where, :] = state[k]
        prep[direction, side, len(STEADY), where, :] = 1.0 / jnp.maximum(
            state[0], MINIMUM_DENSITY
        )
        prep[direction, side, len(STEADY) + 1, where, :] = (
            state[2] * state[2] + state[3] * state[3]
        )

    def kept(direction, where, left, right):
        ready = []
        for side, state in enumerate((left, right)):
            for n, k in enumerate(STEADY):
                state[k] = prep[direction, side, n, where, :]
            ready.append(tuple(prep[direction, side, len(STEADY) + n, where, :] for n in (0, 1)))
        return ready

    def prepare(u):
        def one_row(r, carry):
            base = pl.multiple_of(8 + r * width, 8)
            where = pl.ds(pl.multiple_of(r * width, 8), width)
            left, right = {}, {}
            for k in STEADY:
                cell = u[k, pl.ds(base, width), :]
                high = (pltpu.roll(cell, 127, 1) - cell) * ct[4:5, :]
                low = (cell - pltpu.roll(cell, 1, 1)) * ct[5:6, :]
                slope = half_slope(low, high)
                left[k] = cell + slope
                right[k] = jnp.where(wide_lane == 127, cell, pltpu.roll(cell - slope, 127, 1))
            keep(0, 0, where, left)
            keep(0, 1, where, right)
            for k in STEADY:
                cell = u[k, pl.ds(base, width), :]
                low = 0.5 * (cell - u[k, pl.ds(base - 1, width), :])
                high = 0.5 * (u[k, pl.ds(base + 1, width), :] - cell)
                slope = half_slope(low, high)
                left[k] = pltpu.roll(cell + slope, 1, 0)
                right[k] = cell - slope
            keep(1, 0, where, left)
            keep(1, 1, where, right)
            return carry

        lax.fori_loop(0, rows, one_row, 0)

        def one_inner_row(r, carry):
            base = pl.multiple_of(8 + r * width, 8)
            where = pl.multiple_of(r * width, 8)
            left, right = {}, {}
            for k in STEADY:
                cell = u[k, pl.ds(base, width), :]
                low = 0.5 * (cell - u[k, pl.ds(base - width, width), :])
                high = 0.5 * (u[k, pl.ds(base + width, width), :] - cell)
                slope = half_slope(low, high)
                left[k], right[k] = cell + slope, cell - slope
            keep(2, 0, pl.ds(pl.multiple_of(where + width, 8), width), left)
            keep(2, 1, pl.ds(where, width), right)
            return carry

        lax.fori_loop(1, rows - 1, one_inner_row, 0)

    def polar_and_azimuth(u, prepared=False):
        moving = MOVED if prepared else range(NV)

        together = 2 if prepared else 1
        sine, inverse_sine, cotangent, mask = ct[0:1, :], ct[1:2, :], ct[2:3, :], ct[4:5, :]

        def third(i, n):
            r = jnp.maximum((i - 2) * together, 0) + n
            store = pl.ds(pl.multiple_of(r * width, 8), width)
            scale = tab[0, pl.ds(r, 1), :]
            cells = [u[k, pl.ds(pl.multiple_of(8 + r * width, 8), width), :] for k in range(NV)]
            source = sources(cells, cotangent)
            for k in range(NV):
                through = th[k, store, :]
                change = (pltpu.roll(through, 1, 1) - through) * inverse_sine
                if source[k] is not None:
                    change = change + source[k]
                acc[k, store, :] = cells[k] + scale * change

        def second(i, n):
            r = jnp.clip((i - 1) * together, 0, rows - together) + n
            store = pl.ds(pl.multiple_of(r * width, 8), width)
            left = {k: lt[k, store, :] for k in moving}
            right = {}
            for k in moving:
                value = rt[k, store, :]
                cell = u[k, pl.ds(pl.multiple_of(8 + r * width, 8), width), :]
                right[k] = jnp.where(wide_lane == 127, cell, pltpu.roll(value, 127, 1))
            ready = kept(0, store, left, right) if prepared else (None, None)
            flux = twice_flux(left, right, 2, ready)
            for k in range(NV):
                th[k, store, :] = flux[k] * sine

        def first(i, n):
            r = jnp.minimum(i * together, rows - together) + n
            base = pl.multiple_of(8 + r * width, 8)
            store = pl.ds(pl.multiple_of(r * width, 8), width)
            cells = {k: u[k, pl.ds(base, width), :] for k in moving}
            for k in moving:
                high = (pltpu.roll(cells[k], 127, 1) - cells[k]) * mask
                low = (cells[k] - pltpu.roll(cells[k], 1, 1)) * ct[5:6, :]
                slope = half_slope(low, high)
                lt[k, store, :] = cells[k] + slope
                rt[k, store, :] = cells[k] - slope
            left, right = {}, {}
            for k in moving:
                low = 0.5 * (cells[k] - u[k, pl.ds(base - 1, width), :])
                high = 0.5 * (u[k, pl.ds(base + 1, width), :] - cells[k])
                slope = half_slope(low, high)
                left[k] = pltpu.roll(cells[k] + slope, 1, 0)
                right[k] = cells[k] - slope
            ready = kept(1, store, left, right) if prepared else (None, None)
            flux = twice_flux(left, right, 3, ready)
            for k in range(NV):
                fp[k, pl.ds(pl.multiple_of(r * span, 8), width), :] = flux[k]

        def one_step(i, carry):
            for stage in (third, second, first):
                for n in range(together):
                    stage(i, n)
            return carry

        lax.fori_loop(0, rows // together + 2, one_step, 0)

    def inner_radial(u, prepared=False):
        moving = MOVED if prepared else range(NV)

        def one_row(r, carry):
            base = pl.multiple_of(8 + r * width, 8)
            store = pl.multiple_of(r * width, 8)
            left, right = {}, {}
            for k in moving:
                cell = u[k, pl.ds(base, width), :]
                low = 0.5 * (cell - u[k, pl.ds(base - width, width), :])
                high = 0.5 * (u[k, pl.ds(base + width, width), :] - cell)
                slope = half_slope(low, high)
                right[k] = cell - slope
                left[k] = sl[k, pl.ds(store - width, width), :]
                sl[k, pl.ds(store, width), :] = cell + slope
            ready = kept(2, pl.ds(store, width), left, right) if prepared else (None, None)
            flux = twice_flux(left, right, 1, ready)
            for k in range(NV):
                fr[k, pl.ds(store, width), :] = flux[k]
            return carry

        lax.fori_loop(1, rows - 1, one_row, 0)

    def edge_azimuth(u, halo):
        for side in range(2):
            own = (0, 1, 2) if side == 0 else (width - 3, width - 2, width - 1)
            inside = [
                [u[k, pl.ds(8 + f, 8, stride=width), :] for k in range(NV)] for f in own
            ]
            outside = [[halo[side, k, i] for k in range(NV)] for i in range(2)]
            cells = outside + inside if side == 0 else inside + outside
            fluxes = edge_pair(cells, 3)
            faces = (0, 1) if side == 0 else (width - 1, width)
            for face, flux in zip(faces, fluxes):
                for k in range(NV):
                    fp[k, pl.ds(face, 8, stride=span), :] = flux[k]

    def edge_radial(u, halo):
        for side in range(2):
            own = (0, 1, 2) if side == 0 else (rows - 3, rows - 2, rows - 1)
            inside = [[u[k, pl.ds(8 + r * width, width), :] for k in range(NV)] for r in own]
            outside = [
                [halo[side, k, pl.ds(width * i, width), :] for k in range(NV)] for i in range(2)
            ]
            cells = outside + inside if side == 0 else inside + outside
            fluxes = edge_pair(cells, 1)
            faces = (0, 1) if side == 0 else (rows - 1, rows)
            for face, flux in zip(faces, fluxes):
                for k in range(NV):
                    fr[k, pl.ds(face * width, width), :] = flux[k]

    azimuth_scale = 0.5 / phi_step

    def advanced_row(r):
        store = pl.multiple_of(r * width, 8)
        low_area, high_area = tab[1, pl.ds(r, 1), :], tab[2, pl.ds(r, 1), :]
        across = tab[0, pl.ds(r, 1), :] * ct[1:2, :] * azimuth_scale
        below = pl.multiple_of(r * span, 8)
        values = []
        for k in range(NV):
            values.append(
                acc[k, pl.ds(store, width), :]
                + across * (fp[k, pl.ds(below, width), :] - fp[k, pl.ds(below + 1, width), :])
                + low_area * fr[k, pl.ds(store, width), :]
                - high_area * fr[k, pl.ds(pl.multiple_of(store + width, 8), width), :]
            )
        return values

    with jax.named_scope("pre1"):
        polar_and_azimuth(u0)
    with jax.named_scope("rad1"):
        inner_radial(u0)

    with jax.named_scope("wedge_wait"):
        wedge_all().wait_recv()
    shell_row = wedge_rows[0]
    for j in range(1, wedges):
        shell_row = shell_row + wedge_rows[j]
    below_above[2] = shell_row
    pl.when(place < last)(lambda: side_copy(0).start())
    pl.when(place > 0)(lambda: side_copy(1).start())
    send_masses(below_above.at[2], group + 1, 0, jnp.minimum(level, middle))

    with jax.named_scope("h1_phi_wait"):
        first_halos[2].wait_recv()
        first_halos[3].wait_recv()
    with jax.named_scope("edge_phi1"):
        edge_azimuth(u0, hp0)
    with jax.named_scope("h1_rad_wait"):
        wait_radial(first_halos)
    with jax.named_scope("edge_rad1"):
        edge_radial(u0, hr0)

    def section_one_row(r, carry):
        values = advanced_row(r)
        for k in range(NV):
            u1[k, pl.ds(pl.multiple_of(8 + r * width, 8), width), :] = values[k]
        return carry

    with jax.named_scope("final1"):
        lax.fori_loop(0, rows, section_one_row, 0)
    pack(u1, pk1)
    for k in range(NV):
        sr[0, k] = u1[k, pl.ds(8 + (rows - 2) * width, 2 * width), :]
        sr[1, k] = u1[k, pl.ds(8, 2 * width), :]
    second_halos = halo_copies(1, sr.at[0], sr.at[1], pk1, hr1, hp1)
    start_halos(
        second_halos, hr1,
        lambda k: sr[1, k, pl.ds(0, width), :],
        lambda k: sr[0, k, pl.ds(width, width), :],
    )

    with jax.named_scope("asc_wait"):
        pl.when(after_me > 0)(lambda: pl.semaphore_wait(from_later, after_me))
    send_masses(below_above.at[2], group + 1, jnp.minimum(level, middle), level + 1)
    send_masses(below_above.at[2], group, level + 1, levels)

    from_all = [2 * x for x in range(groups)]
    from_lower = [2 * x + 2 for x in range(groups)]

    def mass_between(z_start, z_stop, count):
        def one_level(z, value):
            part = shared[pl.ds(z * 2 * groups, 2 * groups)]
            return value + jnp.sum(jnp.where(slot < count, part, 0.0), axis=0)

        return lax.fori_loop(z_start, z_stop, one_level, jnp.zeros((1, 128), jnp.float32))

    slot = lax.broadcasted_iota(jnp.int32, (2 * groups, 1, 128), 0)
    with jax.named_scope("prepare"):
        prepare(u1)
    with jax.named_scope("m1_wait"):
        await_masses(from_all, level, levels, lambda copy: copy.wait_recv())
        await_masses(from_lower, 0, level, lambda copy: copy.wait_recv())
        pl.when(place > 0)(lambda: side_copy(0).wait_recv())
        pl.when(place < last)(lambda: side_copy(1).wait_recv())
    below, above, own = below_above[0], below_above[1], below_above[2]
    half_of = lambda index: jnp.where(lane < index, 1.0, jnp.where(lane == index, 0.5, 0.0))
    none = jnp.zeros((8, 128), jnp.float32)
    lower = jnp.where(row < 2, jnp.where(place == 0, half_of(0), none), 0.0)
    upper = jnp.where(row < 2, none, jnp.where(place == last, half_of(rows - 1), 1.0))
    minus = jnp.where(lane >= rows, 0.0, half_of(rows - 2 + row) - 1.0)
    minus = jnp.where(row < 2, minus, none)
    plus = jnp.where(row < 2, none, half_of(row - 2))
    inside = (
        mass_between(level, levels, 2 * group)
        + mass_between(0, level, 2 * group + 2)
        + jnp.where(core_index == 1, below, 0.0)
    )
    table = (
        inside + half_of(row) * own,
        inside
        + (lower + upper) * own
        + jnp.where(place > 0, minus * below, none)
        + jnp.where(place < last, plus * above, none),
    )
    beyond = jnp.clip(first + jnp.where(row < 2, row - 2, rows - 2 + row), 0, slabs * rows - 1)
    fetch_mass.wait()
    for i, target in enumerate((first + row, beyond)):
        enclosed = jnp.sum(table[i], axis=1, keepdims=True) + core[0]
        inverse = 1.0 / radius_of(target)
        grav[8 * i : 8 * i + 8, :] = (timestep * strength) * enclosed * inverse * inverse
        if i == 0:
            enclosed_ref[...] = jnp.sum(
                jnp.where(lane == row, enclosed, 0.0), axis=0, keepdims=True
            )[:, :rows]

    def gravity_row(r, carry):
        base = pl.ds(pl.multiple_of(8 + r * width, 8), width)
        pull = grav[pl.ds(r, 1), :]
        u1[1, base, :] = u1[1, base, :] - pull * jnp.maximum(u0[0, base, :], MINIMUM_DENSITY)
        u1[4, base, :] = u1[4, base, :] - pull * u0[1, base, :]
        return carry

    with jax.named_scope("grav"):
        lax.fori_loop(0, rows, gravity_row, 0)

    with jax.named_scope("pre2"):
        polar_and_azimuth(u1, prepared=True)
    with jax.named_scope("rad2"):
        inner_radial(u1, prepared=True)
    with jax.named_scope("h2_phi_wait"):
        second_halos[2].wait_recv()
        second_halos[3].wait_recv()
    pull = grav[0:8, :]
    for side in range(2):
        for i in range(2):
            hp1[side, 1, i] = hp1[side, 1, i] - pull * jnp.maximum(
                hp0[side, 0, i], MINIMUM_DENSITY
            )
            hp1[side, 4, i] = hp1[side, 4, i] - pull * hp0[side, 1, i]
    with jax.named_scope("edge_phi2"):
        edge_azimuth(u1, hp1)
    with jax.named_scope("h2_rad_wait"):
        wait_radial(second_halos)
    for side in range(2):
        for i in range(2):
            which = pl.ds(width * i, width)
            pull = grav[8 + 2 * side + i : 9 + 2 * side + i, :]
            hr1[side, 1, which, :] = hr1[side, 1, which, :] - pull * jnp.maximum(
                hr0[side, 0, which, :], MINIMUM_DENSITY
            )
            hr1[side, 4, which, :] = hr1[side, 4, which, :] - pull * hr0[side, 1, which, :]
    with jax.named_scope("edge_rad2"):
        edge_radial(u1, hr1)

    def section_two_row(r, carry):
        values = advanced_row(r)
        base = pl.ds(pl.multiple_of(8 + r * width, 8), width)
        pull = grav[pl.ds(r, 1), :]
        values[1] = values[1] - pull * jnp.maximum(u1[0, base, :], MINIMUM_DENSITY)
        values[4] = values[4] - pull * u1[1, base, :]
        for k in range(NV):
            outv[k, pl.ds(pl.multiple_of(r * width, 8), width), :] = 0.5 * (
                u0[k, base, :] + values[k]
            )
        return carry

    with jax.named_scope("final2"):
        lax.fori_loop(0, rows, section_two_row, 0)
    with jax.named_scope("drain"):
        to_larger = [2 * (groups - 1 - x) for x in range(groups)]
        to_same = [2 * (groups - x) for x in range(groups)]
        await_masses(to_larger, 0, level + 1, lambda copy: copy.wait_send())
        await_masses(to_same, level + 1, levels, lambda copy: copy.wait_send())
        wedge_all().wait_send()
        pl.when(place < last)(lambda: side_copy(0).wait_send())
        pl.when(place > 0)(lambda: side_copy(1).wait_send())
        wait_sent(first_halos)
        wait_sent(second_halos)


def put_out(advanced, enclosed, advanced_hbm, enclosed_hbm, sem):
    copies = [
        pltpu.make_async_copy(advanced, advanced_hbm, sem.at[0]),
        pltpu.make_async_copy(enclosed, enclosed_hbm, sem.at[1]),
    ]
    for copy in copies:
        copy.start()
    for copy in copies:
        copy.wait()


def body(groups, conserved, core_mass):
    _, rows, width, lanes = conserved.shape
    slabs, wedges = lax.axis_size("radial"), lax.axis_size("phi")
    inner = slabs // groups
    radial_step, theta_step, phi_step, timestep = step_sizes(rows * slabs, width * wedges, lanes)
    centers = (np.arange(lanes) + 0.5) * theta_step
    faces = (np.arange(lanes) + 1.0) * theta_step
    angles = np.zeros((8, lanes))
    angles[0] = np.sin(faces) * (0.5 / theta_step)
    angles[1] = 1.0 / np.sin(centers)
    angles[2] = np.cos(centers) / np.sin(centers)
    angles[3] = np.sin(centers)
    angles[4] = np.where(np.arange(lanes) == lanes - 1, 0.0, 0.5)
    angles[5] = np.where(np.arange(lanes) == 0, 0.0, 0.5)
    angles = jnp.asarray(angles.astype(np.float32))
    sizes = (rows, width, slabs, wedges, groups, radial_step, theta_step, phi_step, timestep)
    f32 = jnp.float32
    vmem = lambda *shape: pltpu.VMEM(shape, f32)
    dma = lambda count: pltpu.SemaphoreType.DMA((count,))
    in_hbm = lambda value: pltpu.with_memory_space_constraint(value, pltpu.HBM)
    cells = rows * width
    advanced, enclosed = pl.pallas_call(
        functools.partial(kernel, sizes),
        out_shape=(
            jax.ShapeDtypeStruct((NV, cells, lanes), f32),
            jax.ShapeDtypeStruct((1, rows), f32),
        ),
        in_specs=[
            pl.BlockSpec(memory_space=pltpu.HBM),
            pl.BlockSpec(memory_space=pltpu.HBM),
            pl.BlockSpec(memory_space=pltpu.HBM),
        ],
        out_specs=(
            pl.BlockSpec(memory_space=pltpu.VMEM),
            pl.BlockSpec(memory_space=pltpu.VMEM),
        ),
        scratch_shapes=[
            vmem(NV, cells + 16, lanes), vmem(NV, cells + 16, lanes),
            vmem(2, NV, 2 * width, lanes), vmem(2, NV, 2 * width, lanes),
            vmem(2, NV, 2, 8, lanes), vmem(2, NV, 2, 8, lanes),
            vmem(2, NV, 2, 8, lanes), vmem(2, NV, 2, 8, lanes),
            vmem(2, NV, 2 * width, lanes),
            vmem(NV, cells, lanes),
            vmem(NV, rows * (width + 8), lanes),
            vmem(NV, cells + width, lanes),
            vmem(NV, cells, lanes),
            vmem(NV, cells, lanes), vmem(NV, cells, lanes), vmem(NV, cells, lanes),
            vmem(3, 2, len(STEADY) + 2, cells, lanes),
            vmem(slabs, 1, lanes), vmem(3, 1, lanes), vmem(wedges, 1, lanes),
            vmem(3, 8, lanes), vmem(16, lanes), vmem(8, lanes), pltpu.SMEM((1,), f32),
            dma(4), dma(8), dma(8), dma(inner // 2), dma(inner // 2), dma(2), dma(2),
            pltpu.SemaphoreType.DMA, pltpu.SemaphoreType.DMA,
            pltpu.SemaphoreType.REGULAR,
        ],
        compiler_params=pltpu.CompilerParams(
            collective_id=0, has_side_effects=True, vmem_limit_bytes=12 << 20
        ),
    )(in_hbm(conserved.reshape(NV, cells, lanes)), core_mass, in_hbm(angles))
    advanced, enclosed = pl.pallas_call(
        put_out,
        out_shape=(
            jax.ShapeDtypeStruct((NV, cells, lanes), f32),
            jax.ShapeDtypeStruct((1, rows), f32),
        ),
        in_specs=[pl.BlockSpec(memory_space=pltpu.VMEM)] * 2,
        out_specs=[pl.BlockSpec(memory_space=pltpu.HBM)] * 2,
        scratch_shapes=[dma(2)],
        compiler_params=pltpu.CompilerParams(vmem_limit_bytes=4 << 20),
    )(advanced, enclosed)
    return advanced.reshape(conserved.shape), enclosed.reshape(rows)


def solution(mesh):
    in_specs = (P(None, "radial", "phi", None), P())
    out_specs = (P(None, "radial", "phi", None), P("radial"))
    return jax.shard_map(
        functools.partial(body, 4), mesh=mesh, in_specs=in_specs, out_specs=out_specs,
        check_vma=False,
    )
```

```python
import functools
import math

import jax
import jax.numpy as jnp
import numpy as np
from jax import lax
from jax.experimental import pallas as pl
from jax.experimental.pallas import tpu as pltpu
from jax.sharding import PartitionSpec as P

ADIABATIC = 4.0 / 3.0
INNER_RADIUS = 1.0
OUTER_RADIUS = 2.0
COURANT = 0.4
GRAVITY_KICK = 0.004
MINIMUM_DENSITY = 0.05
PRESSURE_FLOOR = 0.01

NV = 8
STEADY = (0, 2, 3, 5, 6, 7)
MOVED = (1, 4)
MESH = pl.DeviceIdType.MESH


def step_sizes(radial_total, phi_total, theta_total):
    theta_step = math.pi / theta_total
    phi_step = 2.0 * math.pi / phi_total
    polar_width = INNER_RADIUS * math.sin(0.5 * theta_step) * phi_step
    radial_step = min(2.0 * polar_width, (OUTER_RADIUS - INNER_RADIUS) / radial_total)
    timestep = COURANT * min(radial_step, polar_width)
    return (radial_step, theta_step, phi_step, timestep)


def half_slope(low, high):
    return jnp.maximum(jnp.minimum(low, high), jnp.minimum(jnp.maximum(low, high), 0.0))


def face_side(state, component, ready=None):
    density = jnp.maximum(state[0], MINIMUM_DENSITY)
    if ready is None:
        inverse, squares = 1.0 / density, state[2] * state[2] + state[3] * state[3]
    else:
        inverse, squares = ready
    squares = state[1] * state[1] + squares
    pressure = jnp.maximum(
        (ADIABATIC - 1.0) * (state[4] - 0.5 * squares * inverse), PRESSURE_FLOOR * density
    )
    normal = state[component] * inverse
    square = ADIABATIC * pressure * inverse
    sound = square * lax.rsqrt(square)
    return pressure, normal, jnp.abs(normal) + sound


def twice_flux(left, right, component, ready=(None, None)):
    left_p, left_v, left_s = face_side(left, component, ready[0])
    right_p, right_v, right_s = face_side(right, component, ready[1])
    signal = jnp.maximum(left_s, right_s)
    left_w, right_w = left_v + signal, right_v - signal
    flux = [left[k] * left_w + right[k] * right_w for k in range(NV)]
    flux[component] = flux[component] + (left_p + right_p)
    flux[4] = flux[4] + (left_p * left_v + right_p * right_v)
    return flux


def edge_pair(cells, component):
    lefts, rights = [], []
    for k in range(NV):
        halves = [0.5 * (cells[i + 1][k] - cells[i][k]) for i in range(4)]
        slopes = [half_slope(halves[i], halves[i + 1]) for i in range(3)]
        lefts.append((cells[1][k] + slopes[0], cells[2][k] + slopes[1]))
        rights.append((cells[2][k] - slopes[1], cells[3][k] - slopes[2]))
    return [
        twice_flux([a[i] for a in lefts], [b[i] for b in rights], component) for i in range(2)
    ]


def sources(cells, cotangent):
    density = jnp.maximum(cells[0], MINIMUM_DENSITY)
    inverse = 1.0 / density
    speed = [None] + [cells[m] * inverse for m in (1, 2, 3)]
    squares = cells[1] * speed[1] + cells[2] * speed[2] + cells[3] * speed[3]
    pressure = jnp.maximum(
        (ADIABATIC - 1.0) * (cells[4] - 0.5 * squares), PRESSURE_FLOOR * density
    )
    spin = cells[3] * speed[3]
    source = [None] * NV
    source[1] = 2.0 * pressure + (cells[2] * speed[2] + spin)
    source[2] = (pressure + spin) * cotangent - cells[1] * speed[2]
    source[3] = -speed[3] * (cells[1] + cells[2] * cotangent)
    return source


def kernel(
    sizes, state_hbm, mass_hbm, angles_hbm,
    outv, enclosed_ref,
    u0, u1, hr0, hr1, hp0, hp1, pk0, pk1, sr, acc, fp, fr, sl, lt, rt, th, prep,
    shared, along, below_above, wedge_rows, chip_rows, inside_rows, weights, tab, grav, ct, core,
    in_sem, halo_send, halo_recv, shared_send, shared_recv, along_send, along_recv,
    side_send, side_recv, pass_send, pass_recv, wedge_send, wedge_recv, chip_send, chip_recv,
    from_near, from_far,
):
    rows, width, slabs, wedges, groups, radial_step, theta_step, phi_step, timestep = sizes
    strength = GRAVITY_KICK / timestep
    place = lax.axis_index("radial")
    wedge = lax.axis_index("phi")
    inner = slabs // groups
    levels = inner // 2
    group, member = place // inner, lax.rem(place, inner)
    level, core_index = member // 2, lax.rem(member, 2)
    span = width + 8
    last = slabs - 1

    def at(radial, phi):
        return {"radial": radial, "phi": phi}

    def signal(semaphore, radial, phi):
        pl.semaphore_signal(semaphore, inc=1, device_id=at(radial, phi), device_id_type=MESH)

    east, west = lax.rem(wedge + 1, wedges), lax.rem(wedge + wedges - 1, wedges)

    fetch_mass = pltpu.make_async_copy(mass_hbm, core, in_sem.at[3])
    fetch_density = pltpu.make_async_copy(
        state_hbm.at[pl.ds(0, 1)], u0.at[pl.ds(0, 1), pl.ds(8, rows * width), :], in_sem.at[0]
    )
    fetch = pltpu.make_async_copy(
        state_hbm.at[pl.ds(1, NV - 1)], u0.at[pl.ds(1, NV - 1), pl.ds(8, rows * width), :],
        in_sem.at[1],
    )
    fetch_angles = pltpu.make_async_copy(angles_hbm, ct, in_sem.at[2])
    for copy in (fetch_density, fetch_angles, fetch, fetch_mass):
        copy.start()

    for side in range(2):
        below_above[side] = jnp.zeros((1, 128), jnp.float32)

    barrier = pltpu.get_barrier_semaphore()
    for step in range(1, wedges):
        signal(barrier, place, lax.rem(wedge + step, wedges))
    pl.when(place < last)(lambda: signal(barrier, place + 1, wedge))
    pl.when(place > 0)(lambda: signal(barrier, place - 1, wedge))

    def greet(x_start, x_stop, z_start, z_stop, cores, semaphore):
        def one_level(back, carry):
            z = z_start + z_stop - 1 - back

            def one_group(x, inner_carry):
                for c in cores:
                    signal(semaphore, x * inner + z * 2 + c, wedge)
                return inner_carry

            return lax.fori_loop(x_start, x_stop, one_group, carry)

        lax.fori_loop(z_start, z_stop, one_level, 0)

    near = levels // 4
    is_near = level < near
    sender = core_index == 1
    both = (0, 1)

    pl.when(is_near)(lambda: greet(0, group, level + 1, levels, (1,), barrier))

    @pl.when(sender)
    def _():
        for step in range(1, wedges):
            signal(barrier, place - 1, lax.rem(wedge + step, wedges))
        greet(group, group + 1, level + 1, levels, both, barrier)
        pl.when(is_near)(lambda: greet(group + 1, groups, level, near, both, barrier))

    def answer():
        greet(group, group + 1, 0, level, (1,), from_far)
        pl.when(is_near)(lambda: greet(0, group, 0, level + 1, (1,), from_near))

    near_answers = jnp.where(
        jnp.logical_and(sender, is_near), 2 * (groups - 1 - group) * (near - level), 0
    )
    far_answers = jnp.where(sender, 2 * (levels - 1 - level), 0)
    greetings = (
        wedges - 1 + jnp.where(place > 0, 1, 0) + jnp.where(place < last, 1, 0) + level
        + jnp.where(is_near, group * (level + 1), 0)
        + jnp.where(sender, 2 * (groups - 1 - group) * jnp.minimum(level, near), wedges - 1)
    )

    row = lax.broadcasted_iota(jnp.int32, (8, 128), 0)
    lane = lax.broadcasted_iota(jnp.int32, (8, 128), 1)
    first = place * rows

    def radius_of(index):
        return INNER_RADIUS + (index.astype(jnp.float32) + 0.5) * radial_step

    radius = radius_of(first + row)
    inverse_radius = 1.0 / radius
    low_face, high_face = radius - 0.5 * radial_step, radius + 0.5 * radial_step
    area = inverse_radius * inverse_radius * (0.5 * timestep / radial_step)
    tab[0] = timestep * inverse_radius
    tab[1] = low_face * low_face * area
    tab[2] = high_face * high_face * area

    with jax.named_scope("fetch_wait"):
        fetch_angles.wait()
        fetch_density.wait()
    total = u0[0, pl.ds(8, 8, stride=width), :]
    for f in range(1, width):
        total = total + u0[0, pl.ds(8 + f, 8, stride=width), :]
    shells = jnp.sum(total * ct[3:4, :], axis=1, keepdims=True) * (
        radius * radius * (radial_step * theta_step * phi_step)
    )
    wedge_rows[0] = jnp.sum(jnp.where(lane == row, shells, 0.0), axis=0, keepdims=True)
    fetch.wait()

    def pack(source, packed):
        for side, zones in enumerate(((width - 2, width - 1), (0, 1))):
            for k in range(NV):
                for i, zone in enumerate(zones):
                    packed[side, k, i] = source[k, pl.ds(8 + zone, 8, stride=width), :]

    pack(u0, pk0)
    with jax.named_scope("barrier_wait"):
        pl.semaphore_wait(barrier, greetings)

    def copy_of(source, target, send, recv, radial, phi):
        return pltpu.make_async_remote_copy(
            src_ref=source, dst_ref=target, send_sem=send, recv_sem=recv,
            device_id=at(radial, phi), device_id_type=MESH,
        )

    def send_across(z_start, z_stop):
        def one_group(x, carry):
            def one_level(z, inner_carry):
                for c in both:
                    copy_of(
                        below_above.at[3], shared.at[level * groups + group], shared_send.at[z],
                        shared_recv.at[level], x * inner + z * 2 + c, wedge,
                    ).start()
                return inner_carry

            return lax.fori_loop(z_start, z_stop, one_level, carry)

        lax.fori_loop(group + 1, groups, one_group, 0)

    def send_along():
        def one_level(z, carry):
            for c in both:
                copy_of(
                    below_above.at[3], along.at[level], along_send.at[z], along_recv.at[level],
                    group * inner + z * 2 + c, wedge,
                ).start()
            return carry

        lax.fori_loop(level + 1, levels, one_level, 0)

    def many(count, send, recv):
        rows_of = shared.at[pl.ds(0, count)]
        return copy_of(rows_of, rows_of, send, recv, place, wedge)

    passers = (
        (near - 1, near, near + (levels - near + 1) // 2),
        (0, near + (levels - near + 1) // 2, levels),
    )

    def pass_copy(z, c):
        return copy_of(
            inside_rows.at[0], inside_rows.at[1], pass_send, pass_recv,
            group * inner + z * 2 + c, wedge,
        )

    def chip_copy(step):
        return copy_of(
            wedge_rows.at[0], chip_rows.at[step], chip_send, chip_recv,
            jnp.minimum(place + 1, last), lax.rem(wedge + step, wedges),
        )

    def wedge_copy(step):
        return copy_of(
            wedge_rows.at[0], wedge_rows.at[step], wedge_send, wedge_recv, place,
            lax.rem(wedge + step, wedges),
        )

    def wedge_all():
        others = wedge_rows.at[pl.ds(1, wedges - 1)]
        return copy_of(others, others, wedge_send, wedge_recv, place, east)

    def side_copy(side):
        target = jnp.minimum(place + 1, last) if side == 0 else jnp.maximum(place - 1, 0)
        return copy_of(
            below_above.at[2], below_above.at[side], side_send.at[side], side_recv.at[side],
            target, wedge,
        )

    @pl.when(jnp.logical_not(sender))
    def _():
        for step in range(wedges):
            chip_copy(step).start()

    for step in range(1, wedges):
        wedge_copy(step).start()

    def halo_copies(number, high_rows, low_rows, packed, radial_halo, phi_halo):
        def copy(which, source, target, peer):
            return pltpu.make_async_remote_copy(
                src_ref=source, dst_ref=target, send_sem=halo_send.at[4 * number + which],
                recv_sem=halo_recv.at[4 * number + which], device_id=peer, device_id_type=MESH,
            )

        return (
            copy(0, high_rows, radial_halo.at[0], at(jnp.minimum(place + 1, last), wedge)),
            copy(1, low_rows, radial_halo.at[1], at(jnp.maximum(place - 1, 0), wedge)),
            copy(2, packed.at[0], phi_halo.at[0], at(place, east)),
            copy(3, packed.at[1], phi_halo.at[1], at(place, west)),
        )

    def start_halos(copies, radial_halo, low_row, high_row):
        pl.when(place < last)(lambda: copies[0].start())
        pl.when(place > 0)(lambda: copies[1].start())
        copies[2].start()
        copies[3].start()

        @pl.when(place == 0)
        def _():
            for k in range(NV):
                for i in range(2):
                    radial_halo[0, k, pl.ds(width * i, width), :] = low_row(k)

        @pl.when(place == last)
        def _():
            for k in range(NV):
                for i in range(2):
                    radial_halo[1, k, pl.ds(width * i, width), :] = high_row(k)

    def wait_radial(copies):
        pl.when(place > 0)(lambda: copies[0].wait_recv())
        pl.when(place < last)(lambda: copies[1].wait_recv())

    def wait_sent(copies):
        pl.when(place < last)(lambda: copies[0].wait_send())
        pl.when(place > 0)(lambda: copies[1].wait_send())
        copies[2].wait_send()
        copies[3].wait_send()

    first_halos = halo_copies(
        0, u0.at[:, pl.ds(8 + (rows - 2) * width, 2 * width), :], u0.at[:, pl.ds(8, 2 * width), :],
        pk0, hr0, hp0,
    )
    start_halos(
        first_halos, hr0,
        lambda k: u0[k, pl.ds(8, width), :],
        lambda k: u0[k, pl.ds(8 + (rows - 1) * width, width), :],
    )

    answer()

    wide_lane = lax.broadcasted_iota(jnp.int32, (width, 128), 1)

    def keep(direction, side, where, state):
        for n, k in enumerate(STEADY):
            prep[direction, side, n, where, :] = state[k]
        prep[direction, side, len(STEADY), where, :] = 1.0 / jnp.maximum(
            state[0], MINIMUM_DENSITY
        )
        prep[direction, side, len(STEADY) + 1, where, :] = (
            state[2] * state[2] + state[3] * state[3]
        )

    def kept(direction, where, left, right):
        ready = []
        for side, state in enumerate((left, right)):
            for n, k in enumerate(STEADY):
                state[k] = prep[direction, side, n, where, :]
            ready.append(tuple(prep[direction, side, len(STEADY) + n, where, :] for n in (0, 1)))
        return ready

    def prepare(u):
        def one_row(r, carry):
            base = pl.multiple_of(8 + r * width, 8)
            where = pl.ds(pl.multiple_of(r * width, 8), width)
            left, right = {}, {}
            for k in STEADY:
                cell = u[k, pl.ds(base, width), :]
                high = (pltpu.roll(cell, 127, 1) - cell) * ct[4:5, :]
                low = (cell - pltpu.roll(cell, 1, 1)) * ct[5:6, :]
                slope = half_slope(low, high)
                left[k] = cell + slope
                right[k] = jnp.where(wide_lane == 127, cell, pltpu.roll(cell - slope, 127, 1))
            keep(0, 0, where, left)
            keep(0, 1, where, right)
            for k in STEADY:
                cell = u[k, pl.ds(base, width), :]
                low = 0.5 * (cell - u[k, pl.ds(base - 1, width), :])
                high = 0.5 * (u[k, pl.ds(base + 1, width), :] - cell)
                slope = half_slope(low, high)
                left[k] = pltpu.roll(cell + slope, 1, 0)
                right[k] = cell - slope
            keep(1, 0, where, left)
            keep(1, 1, where, right)
            return carry

        lax.fori_loop(0, rows, one_row, 0)

        def one_inner_row(r, carry):
            base = pl.multiple_of(8 + r * width, 8)
            where = pl.multiple_of(r * width, 8)
            left, right = {}, {}
            for k in STEADY:
                cell = u[k, pl.ds(base, width), :]
                low = 0.5 * (cell - u[k, pl.ds(base - width, width), :])
                high = 0.5 * (u[k, pl.ds(base + width, width), :] - cell)
                slope = half_slope(low, high)
                left[k], right[k] = cell + slope, cell - slope
            keep(2, 0, pl.ds(pl.multiple_of(where + width, 8), width), left)
            keep(2, 1, pl.ds(where, width), right)
            return carry

        lax.fori_loop(1, rows - 1, one_inner_row, 0)

    def polar_and_azimuth(u, prepared=False):
        moving = MOVED if prepared else range(NV)

        together = 2 if prepared else 1
        sine, inverse_sine, cotangent, mask = ct[0:1, :], ct[1:2, :], ct[2:3, :], ct[4:5, :]

        def third(i, n):
            r = jnp.maximum((i - 2) * together, 0) + n
            store = pl.ds(pl.multiple_of(r * width, 8), width)
            scale = tab[0, pl.ds(r, 1), :]
            cells = [u[k, pl.ds(pl.multiple_of(8 + r * width, 8), width), :] for k in range(NV)]
            source = sources(cells, cotangent)
            for k in range(NV):
                through = th[k, store, :]
                change = (pltpu.roll(through, 1, 1) - through) * inverse_sine
                if source[k] is not None:
                    change = change + source[k]
                acc[k, store, :] = cells[k] + scale * change

        def second(i, n):
            r = jnp.clip((i - 1) * together, 0, rows - together) + n
            store = pl.ds(pl.multiple_of(r * width, 8), width)
            left = {k: lt[k, store, :] for k in moving}
            right = {}
            for k in moving:
                value = rt[k, store, :]
                cell = u[k, pl.ds(pl.multiple_of(8 + r * width, 8), width), :]
                right[k] = jnp.where(wide_lane == 127, cell, pltpu.roll(value, 127, 1))
            ready = kept(0, store, left, right) if prepared else (None, None)
            flux = twice_flux(left, right, 2, ready)
            for k in range(NV):
                th[k, store, :] = flux[k] * sine

        def first(i, n):
            r = jnp.minimum(i * together, rows - together) + n
            base = pl.multiple_of(8 + r * width, 8)
            store = pl.ds(pl.multiple_of(r * width, 8), width)
            cells = {k: u[k, pl.ds(base, width), :] for k in moving}
            for k in moving:
                high = (pltpu.roll(cells[k], 127, 1) - cells[k]) * mask
                low = (cells[k] - pltpu.roll(cells[k], 1, 1)) * ct[5:6, :]
                slope = half_slope(low, high)
                lt[k, store, :] = cells[k] + slope
                rt[k, store, :] = cells[k] - slope
            left, right = {}, {}
            for k in moving:
                low = 0.5 * (cells[k] - u[k, pl.ds(base - 1, width), :])
                high = 0.5 * (u[k, pl.ds(base + 1, width), :] - cells[k])
                slope = half_slope(low, high)
                left[k] = pltpu.roll(cells[k] + slope, 1, 0)
                right[k] = cells[k] - slope
            ready = kept(1, store, left, right) if prepared else (None, None)
            flux = twice_flux(left, right, 3, ready)
            for k in range(NV):
                fp[k, pl.ds(pl.multiple_of(r * span, 8), width), :] = flux[k]

        def run(i, stages):
            for stage in stages:
                for n in range(together):
                    stage(i, n)

        def one_step(i, carry):
            run(i, (third, second, first))
            return carry

        steps = rows // together
        if prepared:
            run(0, (first,))
            run(1, (second, first))
            lax.fori_loop(2, steps, one_step, 0)
            run(steps, (third, second))
            run(steps + 1, (third,))
        else:
            lax.fori_loop(0, steps + 2, one_step, 0)

    def inner_radial(u, prepared=False):
        moving = MOVED if prepared else range(NV)

        def one_row(r, carry):
            base = pl.multiple_of(8 + r * width, 8)
            store = pl.multiple_of(r * width, 8)
            left, right = {}, {}
            for k in moving:
                cell = u[k, pl.ds(base, width), :]
                low = 0.5 * (cell - u[k, pl.ds(base - width, width), :])
                high = 0.5 * (u[k, pl.ds(base + width, width), :] - cell)
                slope = half_slope(low, high)
                right[k] = cell - slope
                left[k] = sl[k, pl.ds(store - width, width), :]
                sl[k, pl.ds(store, width), :] = cell + slope
            ready = kept(2, pl.ds(store, width), left, right) if prepared else (None, None)
            flux = twice_flux(left, right, 1, ready)
            for k in range(NV):
                fr[k, pl.ds(store, width), :] = flux[k]
            return carry

        lax.fori_loop(1, rows - 1, one_row, 0)

    def edge_azimuth(u, halo):
        for side in range(2):
            own = (0, 1, 2) if side == 0 else (width - 3, width - 2, width - 1)
            inside = [
                [u[k, pl.ds(8 + f, 8, stride=width), :] for k in range(NV)] for f in own
            ]
            outside = [[halo[side, k, i] for k in range(NV)] for i in range(2)]
            cells = outside + inside if side == 0 else inside + outside
            fluxes = edge_pair(cells, 3)
            faces = (0, 1) if side == 0 else (width - 1, width)
            for face, flux in zip(faces, fluxes):
                for k in range(NV):
                    fp[k, pl.ds(face, 8, stride=span), :] = flux[k]

    def edge_radial(u, halo):
        for side in range(2):
            own = (0, 1, 2) if side == 0 else (rows - 3, rows - 2, rows - 1)
            inside = [[u[k, pl.ds(8 + r * width, width), :] for k in range(NV)] for r in own]
            outside = [
                [halo[side, k, pl.ds(width * i, width), :] for k in range(NV)] for i in range(2)
            ]
            cells = outside + inside if side == 0 else inside + outside
            fluxes = edge_pair(cells, 1)
            faces = (0, 1) if side == 0 else (rows - 1, rows)
            for face, flux in zip(faces, fluxes):
                for k in range(NV):
                    fr[k, pl.ds(face * width, width), :] = flux[k]

    azimuth_scale = 0.5 / phi_step

    def advanced_row(r):
        store = pl.multiple_of(r * width, 8)
        low_area, high_area = tab[1, pl.ds(r, 1), :], tab[2, pl.ds(r, 1), :]
        across = tab[0, pl.ds(r, 1), :] * ct[1:2, :] * azimuth_scale
        below = pl.multiple_of(r * span, 8)
        values = []
        for k in range(NV):
            values.append(
                acc[k, pl.ds(store, width), :]
                + across * (fp[k, pl.ds(below, width), :] - fp[k, pl.ds(below + 1, width), :])
                + low_area * fr[k, pl.ds(store, width), :]
                - high_area * fr[k, pl.ds(pl.multiple_of(store + width, 8), width), :]
            )
        return values

    with jax.named_scope("pre1"):
        polar_and_azimuth(u0)
    with jax.named_scope("rad1"):
        inner_radial(u0)

    with jax.named_scope("wedge_wait"):
        wedge_all().wait_recv()
    shell_row = wedge_rows[0]
    for j in range(1, wedges):
        shell_row = shell_row + wedge_rows[j]
    below_above[2] = shell_row
    pl.when(place < last)(lambda: side_copy(0).start())
    pl.when(place > 0)(lambda: side_copy(1).start())

    @pl.when(sender)
    def _():
        many(wedges, chip_send, chip_recv).wait_recv()
        chip_row = shell_row
        for j in range(wedges):
            chip_row = chip_row + chip_rows[j]
        below_above[3] = chip_row
        send_across(0, jnp.minimum(level, near))
        pl.when(near_answers > 0)(lambda: pl.semaphore_wait(from_near, near_answers))
        send_across(jnp.minimum(level, near), near)

    with jax.named_scope("h1_phi_wait"):
        first_halos[2].wait_recv()
        first_halos[3].wait_recv()
    with jax.named_scope("edge_phi1"):
        edge_azimuth(u0, hp0)
    with jax.named_scope("h1_rad_wait"):
        wait_radial(first_halos)
    with jax.named_scope("edge_rad1"):
        edge_radial(u0, hr0)

    def section_one_row(r, carry):
        values = advanced_row(r)
        for k in range(NV):
            u1[k, pl.ds(pl.multiple_of(8 + r * width, 8), width), :] = values[k]
        return carry

    with jax.named_scope("final1"):
        lax.fori_loop(0, rows, section_one_row, 0)
    pack(u1, pk1)
    for k in range(NV):
        sr[0, k] = u1[k, pl.ds(8 + (rows - 2) * width, 2 * width), :]
        sr[1, k] = u1[k, pl.ds(8, 2 * width), :]
    second_halos = halo_copies(1, sr.at[0], sr.at[1], pk1, hr1, hp1)
    start_halos(
        second_halos, hr1,
        lambda k: sr[1, k, pl.ds(0, width), :],
        lambda k: sr[0, k, pl.ds(width, width), :],
    )

    with jax.named_scope("asc_wait"):
        pl.when(far_answers > 0)(lambda: pl.semaphore_wait(from_far, far_answers))
    pl.when(sender)(send_along)

    def gather_across():
        for x in range(1, groups):

            @pl.when(group == x)
            def _(count=x):
                def one_level(z, value):
                    many(count, shared_send.at[0], shared_recv.at[z]).wait_recv()
                    for n in range(count):
                        value = value + shared[z * groups + n]
                    return value

                inside_rows[0] = lax.fori_loop(
                    0, levels, one_level, jnp.zeros((1, 128), jnp.float32)
                )
                for passer, z_start, z_stop in passers:

                    @pl.when(jnp.logical_and(sender, level == passer))
                    def _(z_start=z_start, z_stop=z_stop):
                        for z in range(z_start, z_stop):
                            for c in both:
                                pass_copy(z, c).start()

    def gather_along():
        def one_level(z, value):
            many(1, along_send.at[0], along_recv.at[z]).wait_recv()
            return value + along[z]

        return lax.fori_loop(0, level, one_level, jnp.zeros((1, 128), jnp.float32))

    half_of = lambda index: jnp.where(lane < index, 1.0, jnp.where(lane == index, 0.5, 0.0))
    none = jnp.zeros((8, 128), jnp.float32)
    lower = jnp.where(row < 2, jnp.where(place == 0, half_of(0), none), 0.0)
    upper = jnp.where(row < 2, none, jnp.where(place == last, half_of(rows - 1), 1.0))
    minus = jnp.where(lane >= rows, 0.0, half_of(rows - 2 + row) - 1.0)
    minus = jnp.where(jnp.logical_and(row < 2, place > 0), minus, none)
    plus = jnp.where(jnp.logical_or(row < 2, place == last), none, half_of(row - 2))
    beyond = jnp.clip(first + jnp.where(row < 2, row - 2, rows - 2 + row), 0, slabs * rows - 1)
    weights[0] = half_of(row)
    weights[1] = lower + upper
    weights[2] = minus
    weights[3] = plus
    for i, target in enumerate((first + row, beyond)):
        inverse = 1.0 / radius_of(target)
        weights[4 + i] = (timestep * strength) * inverse * inverse
    fetch_mass.wait()

    with jax.named_scope("prepare"):
        prepare(u1)
    with jax.named_scope("m1_wait"):
        pl.when(is_near)(gather_across)
        inside = gather_along()
        pl.when(jnp.logical_and(group > 0, jnp.logical_not(is_near)))(
            lambda: pass_copy(levels - 1, 1).wait_recv()
        )
        pl.when(place > 0)(lambda: side_copy(0).wait_recv())
        pl.when(place < last)(lambda: side_copy(1).wait_recv())
    below, above, own = below_above[0], below_above[1], below_above[2]
    smaller_x = jnp.where(is_near, inside_rows[0], inside_rows[1])
    inside = inside + jnp.where(group > 0, smaller_x, 0.0) + jnp.where(core_index == 1, below, 0.0)
    table = (
        inside + weights[0] * own,
        inside + weights[1] * own + weights[2] * below + weights[3] * above,
    )
    for i in range(2):
        enclosed = jnp.sum(table[i], axis=1, keepdims=True) + core[0]
        grav[8 * i : 8 * i + 8, :] = weights[4 + i] * enclosed
        if i == 0:
            enclosed_ref[...] = jnp.sum(
                jnp.where(lane == row, enclosed, 0.0), axis=0, keepdims=True
            )[:, :rows]

    def gravity_row(r, carry):
        base = pl.ds(pl.multiple_of(8 + r * width, 8), width)
        pull = grav[pl.ds(r, 1), :]
        u1[1, base, :] = u1[1, base, :] - pull * jnp.maximum(u0[0, base, :], MINIMUM_DENSITY)
        u1[4, base, :] = u1[4, base, :] - pull * u0[1, base, :]
        return carry

    with jax.named_scope("grav"):
        lax.fori_loop(0, rows, gravity_row, 0)

    with jax.named_scope("pre2"):
        polar_and_azimuth(u1, prepared=True)
    with jax.named_scope("rad2"):
        inner_radial(u1, prepared=True)
    with jax.named_scope("h2_phi_wait"):
        second_halos[2].wait_recv()
        second_halos[3].wait_recv()
    pull = grav[0:8, :]
    for side in range(2):
        for i in range(2):
            hp1[side, 1, i] = hp1[side, 1, i] - pull * jnp.maximum(
                hp0[side, 0, i], MINIMUM_DENSITY
            )
            hp1[side, 4, i] = hp1[side, 4, i] - pull * hp0[side, 1, i]
    with jax.named_scope("edge_phi2"):
        edge_azimuth(u1, hp1)
    with jax.named_scope("h2_rad_wait"):
        wait_radial(second_halos)
    for side in range(2):
        for i in range(2):
            which = pl.ds(width * i, width)
            pull = grav[8 + 2 * side + i : 9 + 2 * side + i, :]
            hr1[side, 1, which, :] = hr1[side, 1, which, :] - pull * jnp.maximum(
                hr0[side, 0, which, :], MINIMUM_DENSITY
            )
            hr1[side, 4, which, :] = hr1[side, 4, which, :] - pull * hr0[side, 1, which, :]
    with jax.named_scope("edge_rad2"):
        edge_radial(u1, hr1)

    def section_two_row(r, carry):
        values = advanced_row(r)
        base = pl.ds(pl.multiple_of(8 + r * width, 8), width)
        pull = grav[pl.ds(r, 1), :]
        values[1] = values[1] - pull * jnp.maximum(u1[0, base, :], MINIMUM_DENSITY)
        values[4] = values[4] - pull * u1[1, base, :]
        for k in range(NV):
            outv[k, pl.ds(pl.multiple_of(r * width, 8), width), :] = 0.5 * (
                u0[k, base, :] + values[k]
            )
        return carry

    with jax.named_scope("final2"):
        lax.fori_loop(0, rows, section_two_row, 0)
    with jax.named_scope("drain"):
        @pl.when(sender)
        def _():
            for x in range(groups - 1):

                @pl.when(group == x)
                def _(count=2 * (groups - 1 - x)):
                    for z in range(near):
                        many(count, shared_send.at[z], shared_recv.at[0]).wait_send()

            def sent_along(z, carry):
                many(2, along_send.at[z], along_recv.at[0]).wait_send()
                return carry

            lax.fori_loop(level + 1, levels, sent_along, 0)
            for passer, z_start, z_stop in passers:
                pl.when(jnp.logical_and(group > 0, level == passer))(
                    lambda count=2 * (z_stop - z_start): many(
                        count, pass_send, pass_recv
                    ).wait_send()
                )

        pl.when(jnp.logical_not(sender))(lambda: many(wedges, chip_send, chip_recv).wait_send())
        wedge_all().wait_send()
        pl.when(place < last)(lambda: side_copy(0).wait_send())
        pl.when(place > 0)(lambda: side_copy(1).wait_send())
        wait_sent(first_halos)
        wait_sent(second_halos)


def put_out(advanced, enclosed, advanced_hbm, enclosed_hbm, sem):
    copies = [
        pltpu.make_async_copy(advanced.at[k], advanced_hbm.at[k], sem.at[k]) for k in range(NV)
    ] + [pltpu.make_async_copy(enclosed, enclosed_hbm, sem.at[NV])]
    for copy in copies:
        copy.start()
    for copy in copies:
        copy.wait()


def body(groups, conserved, core_mass):
    _, rows, width, lanes = conserved.shape
    slabs, wedges = lax.axis_size("radial"), lax.axis_size("phi")
    inner = slabs // groups
    radial_step, theta_step, phi_step, timestep = step_sizes(rows * slabs, width * wedges, lanes)
    centers = (np.arange(lanes) + 0.5) * theta_step
    faces = (np.arange(lanes) + 1.0) * theta_step
    angles = np.zeros((8, lanes))
    angles[0] = np.sin(faces) * (0.5 / theta_step)
    angles[1] = 1.0 / np.sin(centers)
    angles[2] = np.cos(centers) / np.sin(centers)
    angles[3] = np.sin(centers)
    angles[4] = np.where(np.arange(lanes) == lanes - 1, 0.0, 0.5)
    angles[5] = np.where(np.arange(lanes) == 0, 0.0, 0.5)
    angles = jnp.asarray(angles.astype(np.float32))
    sizes = (rows, width, slabs, wedges, groups, radial_step, theta_step, phi_step, timestep)
    f32 = jnp.float32
    vmem = lambda *shape: pltpu.VMEM(shape, f32)
    dma = lambda count: pltpu.SemaphoreType.DMA((count,))
    in_hbm = lambda value: pltpu.with_memory_space_constraint(value, pltpu.HBM)
    cells = rows * width
    advanced, enclosed = pl.pallas_call(
        functools.partial(kernel, sizes),
        out_shape=(
            jax.ShapeDtypeStruct((NV, cells, lanes), f32),
            jax.ShapeDtypeStruct((1, rows), f32),
        ),
        in_specs=[
            pl.BlockSpec(memory_space=pltpu.HBM),
            pl.BlockSpec(memory_space=pltpu.HBM),
            pl.BlockSpec(memory_space=pltpu.HBM),
        ],
        out_specs=(
            pl.BlockSpec(memory_space=pltpu.VMEM),
            pl.BlockSpec(memory_space=pltpu.VMEM),
        ),
        scratch_shapes=[
            vmem(NV, cells + 16, lanes), vmem(NV, cells + 16, lanes),
            vmem(2, NV, 2 * width, lanes), vmem(2, NV, 2 * width, lanes),
            vmem(2, NV, 2, 8, lanes), vmem(2, NV, 2, 8, lanes),
            vmem(2, NV, 2, 8, lanes), vmem(2, NV, 2, 8, lanes),
            vmem(2, NV, 2 * width, lanes),
            vmem(NV, cells, lanes),
            vmem(NV, rows * (width + 8), lanes),
            vmem(NV, cells + width, lanes),
            vmem(NV, cells, lanes),
            vmem(NV, cells, lanes), vmem(NV, cells, lanes), vmem(NV, cells, lanes),
            vmem(3, 2, len(STEADY) + 2, cells, lanes),
            vmem(slabs // 2, 1, lanes), vmem(inner // 2, 1, lanes), vmem(4, 1, lanes), vmem(wedges, 1, lanes),
            vmem(wedges, 1, lanes), vmem(2, 1, lanes), vmem(6, 8, lanes),
            vmem(3, 8, lanes), vmem(16, lanes), vmem(8, lanes), pltpu.SMEM((1,), f32),
            dma(4), dma(8), dma(8), dma(inner // 8), dma(inner // 2),
            dma(inner // 2), dma(inner // 2), dma(2), dma(2),
            pltpu.SemaphoreType.DMA, pltpu.SemaphoreType.DMA,
            pltpu.SemaphoreType.DMA, pltpu.SemaphoreType.DMA,
            pltpu.SemaphoreType.DMA, pltpu.SemaphoreType.DMA,
            pltpu.SemaphoreType.REGULAR, pltpu.SemaphoreType.REGULAR,
        ],
        compiler_params=pltpu.CompilerParams(
            collective_id=0, has_side_effects=True, vmem_limit_bytes=12 << 20
        ),
    )(in_hbm(conserved.reshape(NV, cells, lanes)), core_mass, in_hbm(angles))
    advanced, enclosed = pl.pallas_call(
        put_out,
        out_shape=(
            jax.ShapeDtypeStruct((NV, cells, lanes), f32),
            jax.ShapeDtypeStruct((1, rows), f32),
        ),
        in_specs=[pl.BlockSpec(memory_space=pltpu.VMEM)] * 2,
        out_specs=[pl.BlockSpec(memory_space=pltpu.HBM)] * 2,
        scratch_shapes=[dma(NV + 1)],
        compiler_params=pltpu.CompilerParams(vmem_limit_bytes=4 << 20),
    )(advanced, enclosed)
    return advanced.reshape(conserved.shape), enclosed.reshape(rows)


def solution(mesh):
    in_specs = (P(None, "radial", "phi", None), P())
    out_specs = (P(None, "radial", "phi", None), P("radial"))
    return jax.shard_map(
        functools.partial(body, 4), mesh=mesh, in_specs=in_specs, out_specs=out_specs,
        check_vma=False,
    )
```

```python
import functools
import math

import jax
import jax.numpy as jnp
import numpy as np
from jax import lax
from jax.experimental import pallas as pl
from jax.experimental.pallas import tpu as pltpu
from jax.sharding import PartitionSpec as P

ADIABATIC = 4.0 / 3.0
INNER_RADIUS = 1.0
OUTER_RADIUS = 2.0
COURANT = 0.4
GRAVITY_KICK = 0.004
MINIMUM_DENSITY = 0.05
PRESSURE_FLOOR = 0.01

NV = 8
STEADY = (0, 2, 3, 5, 6, 7)
MOVED = (1, 4)
MESH = pl.DeviceIdType.MESH


def step_sizes(radial_total, phi_total, theta_total):
    theta_step = math.pi / theta_total
    phi_step = 2.0 * math.pi / phi_total
    polar_width = INNER_RADIUS * math.sin(0.5 * theta_step) * phi_step
    radial_step = min(2.0 * polar_width, (OUTER_RADIUS - INNER_RADIUS) / radial_total)
    timestep = COURANT * min(radial_step, polar_width)
    return (radial_step, theta_step, phi_step, timestep)


def half_slope(low, high):
    return jnp.maximum(jnp.minimum(low, high), jnp.minimum(jnp.maximum(low, high), 0.0))


def side_ready(state):
    density = jnp.maximum(state[0], MINIMUM_DENSITY)
    squares = state[2] * state[2] + state[3] * state[3]
    return 1.0 / density, squares, PRESSURE_FLOOR * density


def face_side(state, component, ready=None):
    if ready is None:
        ready = side_ready(state)
    inverse, squares, floor = ready
    squares = state[1] * state[1] + squares
    pressure = jnp.maximum((ADIABATIC - 1.0) * (state[4] - 0.5 * squares * inverse), floor)
    normal = state[component] * inverse
    square = ADIABATIC * pressure * inverse
    sound = square * lax.rsqrt(square)
    return pressure, normal, jnp.abs(normal) + sound


def twice_flux(left, right, component, ready=(None, None), factor=None):
    left_p, left_v, left_s = face_side(left, component, ready[0])
    right_p, right_v, right_s = face_side(right, component, ready[1])
    signal = jnp.maximum(left_s, right_s)
    left_w, right_w = left_v + signal, right_v - signal
    if factor is not None:
        left_w, right_w = left_w * factor, right_w * factor
        left_p, right_p = left_p * factor, right_p * factor
    flux = [left[k] * left_w + right[k] * right_w for k in range(NV)]
    flux[component] = flux[component] + (left_p + right_p)
    flux[4] = flux[4] + (left_p * left_v + right_p * right_v)
    return flux


def edge_pair(cells, component):
    lefts, rights = [], []
    for k in range(NV):
        halves = [0.5 * (cells[i + 1][k] - cells[i][k]) for i in range(4)]
        slopes = [half_slope(halves[i], halves[i + 1]) for i in range(3)]
        lefts.append((cells[1][k] + slopes[0], cells[2][k] + slopes[1]))
        rights.append((cells[2][k] - slopes[1], cells[3][k] - slopes[2]))
    return [
        twice_flux([a[i] for a in lefts], [b[i] for b in rights], component) for i in range(2)
    ]


def two_at_a_time(start, stop, one_row):
    def two_rows(i, carry):
        for n in range(2):
            one_row(start + 2 * i + n, carry)
        return carry

    lax.fori_loop(0, (stop - start) // 2, two_rows, 0)


def sources(cells, cotangent):
    density = jnp.maximum(cells[0], MINIMUM_DENSITY)
    inverse = 1.0 / density
    speed = [None] + [cells[m] * inverse for m in (1, 2, 3)]
    squares = cells[1] * speed[1] + cells[2] * speed[2] + cells[3] * speed[3]
    pressure = jnp.maximum(
        (ADIABATIC - 1.0) * (cells[4] - 0.5 * squares), PRESSURE_FLOOR * density
    )
    spin = cells[3] * speed[3]
    source = [None] * NV
    source[1] = 2.0 * pressure + (cells[2] * speed[2] + spin)
    source[2] = (pressure + spin) * cotangent - cells[1] * speed[2]
    source[3] = -speed[3] * (cells[1] + cells[2] * cotangent)
    return source


def kernel(
    sizes, state_hbm, mass_hbm, angles_hbm,
    outv, enclosed_ref,
    u0, u1, hr0, hr1, hp0, hp1, pk0, pk1, sr, acc, fp, fr, sl, lt, rt, th, prep,
    shared, along, below_above, wedge_rows, chip_rows, inside_rows, weights, tab, grav, ct, core,
    in_sem, halo_send, halo_recv, shared_send, shared_recv, along_send, along_recv,
    side_send, side_recv, pass_send, pass_recv, wedge_send, wedge_recv, chip_send, chip_recv,
    from_near, from_far,
):
    rows, width, slabs, wedges, groups, radial_step, theta_step, phi_step, timestep = sizes
    strength = GRAVITY_KICK / timestep
    place = lax.axis_index("radial")
    wedge = lax.axis_index("phi")
    inner = slabs // groups
    levels = inner // 2
    group, member = place // inner, lax.rem(place, inner)
    level, core_index = member // 2, lax.rem(member, 2)
    span = width + 8
    last = slabs - 1

    def at(radial, phi):
        return {"radial": radial, "phi": phi}

    def signal(semaphore, radial, phi):
        pl.semaphore_signal(semaphore, inc=1, device_id=at(radial, phi), device_id_type=MESH)

    east, west = lax.rem(wedge + 1, wedges), lax.rem(wedge + wedges - 1, wedges)

    fetch_mass = pltpu.make_async_copy(mass_hbm, core, in_sem.at[3])
    fetch_density = pltpu.make_async_copy(
        state_hbm.at[pl.ds(0, 1)], u0.at[pl.ds(0, 1), pl.ds(8, rows * width), :], in_sem.at[0]
    )
    fetch = pltpu.make_async_copy(
        state_hbm.at[pl.ds(1, NV - 1)], u0.at[pl.ds(1, NV - 1), pl.ds(8, rows * width), :],
        in_sem.at[1],
    )
    fetch_angles = pltpu.make_async_copy(angles_hbm, ct, in_sem.at[2])
    for copy in (fetch_density, fetch_angles, fetch, fetch_mass):
        copy.start()

    for side in range(2):
        below_above[side] = jnp.zeros((1, 128), jnp.float32)

    barrier = pltpu.get_barrier_semaphore()
    for step in range(1, wedges):
        signal(barrier, place, lax.rem(wedge + step, wedges))
    pl.when(place < last)(lambda: signal(barrier, place + 1, wedge))
    pl.when(place > 0)(lambda: signal(barrier, place - 1, wedge))

    def greet(x_start, x_stop, z_start, z_stop, cores, semaphore):
        def one_level(back, carry):
            z = z_start + z_stop - 1 - back

            def one_group(x, inner_carry):
                for c in cores:
                    signal(semaphore, x * inner + z * 2 + c, wedge)
                return inner_carry

            return lax.fori_loop(x_start, x_stop, one_group, carry)

        lax.fori_loop(z_start, z_stop, one_level, 0)

    near = levels // 4
    is_near = level < near
    sender = core_index == 1
    both = (0, 1)

    pl.when(is_near)(lambda: greet(0, group, level + 1, levels, (1,), barrier))

    @pl.when(sender)
    def _():
        for step in range(1, wedges):
            signal(barrier, place - 1, lax.rem(wedge + step, wedges))
        greet(group, group + 1, level + 1, levels, both, barrier)
        pl.when(is_near)(lambda: greet(group + 1, groups, level, near, both, barrier))

    def answer():
        greet(group, group + 1, 0, level, (1,), from_far)
        pl.when(is_near)(lambda: greet(0, group, 0, level + 1, (1,), from_near))

    near_answers = jnp.where(
        jnp.logical_and(sender, is_near), 2 * (groups - 1 - group) * (near - level), 0
    )
    far_answers = jnp.where(sender, 2 * (levels - 1 - level), 0)
    greetings = (
        wedges - 1 + jnp.where(place > 0, 1, 0) + jnp.where(place < last, 1, 0) + level
        + jnp.where(is_near, group * (level + 1), 0)
        + jnp.where(sender, 2 * (groups - 1 - group) * jnp.minimum(level, near), wedges - 1)
    )

    row = lax.broadcasted_iota(jnp.int32, (8, 128), 0)
    lane = lax.broadcasted_iota(jnp.int32, (8, 128), 1)
    first = place * rows

    def radius_of(index):
        return INNER_RADIUS + (index.astype(jnp.float32) + 0.5) * radial_step

    radius = radius_of(first + row)
    inverse_radius = 1.0 / radius
    low_face, high_face = radius - 0.5 * radial_step, radius + 0.5 * radial_step
    area = inverse_radius * inverse_radius * (0.5 * timestep / radial_step)
    tab[0] = timestep * inverse_radius
    tab[1] = low_face * low_face * area
    tab[2] = high_face * high_face * area

    with jax.named_scope("fetch_wait"):
        fetch_angles.wait()
        fetch_density.wait()
    total = u0[0, pl.ds(8, 8, stride=width), :]
    for f in range(1, width):
        total = total + u0[0, pl.ds(8 + f, 8, stride=width), :]
    shells = jnp.sum(total * ct[3:4, :], axis=1, keepdims=True) * (
        radius * radius * (radial_step * theta_step * phi_step)
    )
    wedge_rows[0] = jnp.sum(jnp.where(lane == row, shells, 0.0), axis=0, keepdims=True)
    fetch.wait()

    def pack(source, packed):
        for side, zones in enumerate(((width - 2, width - 1), (0, 1))):
            for k in range(NV):
                for i, zone in enumerate(zones):
                    packed[side, k, i] = source[k, pl.ds(8 + zone, 8, stride=width), :]

    pack(u0, pk0)
    with jax.named_scope("barrier_wait"):
        pl.semaphore_wait(barrier, greetings)

    def copy_of(source, target, send, recv, radial, phi):
        return pltpu.make_async_remote_copy(
            src_ref=source, dst_ref=target, send_sem=send, recv_sem=recv,
            device_id=at(radial, phi), device_id_type=MESH,
        )

    def send_across(z_start, z_stop):
        def one_group(x, carry):
            def one_level(z, inner_carry):
                for c in both:
                    copy_of(
                        below_above.at[3], shared.at[level * groups + group], shared_send,
                        shared_recv, x * inner + z * 2 + c, wedge,
                    ).start()
                return inner_carry

            return lax.fori_loop(z_start, z_stop, one_level, carry)

        lax.fori_loop(group + 1, groups, one_group, 0)

    def send_along():
        def one_level(z, carry):
            for c in both:
                copy_of(
                    below_above.at[3], along.at[level], along_send, along_recv,
                    group * inner + z * 2 + c, wedge,
                ).start()
            return carry

        lax.fori_loop(level + 1, levels, one_level, 0)

    def many(count, send, recv):
        rows_of = shared.at[pl.ds(0, count)]
        return copy_of(rows_of, rows_of, send, recv, place, wedge)

    passers = (
        (near - 1, near, near + (levels - near + 1) // 2),
        (0, near + (levels - near + 1) // 2, levels),
    )

    def pass_copy(z, c):
        return copy_of(
            inside_rows.at[0], inside_rows.at[1], pass_send, pass_recv,
            group * inner + z * 2 + c, wedge,
        )

    def chip_copy(step):
        return copy_of(
            wedge_rows.at[0], chip_rows.at[step], chip_send, chip_recv,
            jnp.minimum(place + 1, last), lax.rem(wedge + step, wedges),
        )

    def wedge_copy(step):
        return copy_of(
            wedge_rows.at[0], wedge_rows.at[step], wedge_send, wedge_recv, place,
            lax.rem(wedge + step, wedges),
        )

    def wedge_all():
        others = wedge_rows.at[pl.ds(1, wedges - 1)]
        return copy_of(others, others, wedge_send, wedge_recv, place, east)

    def side_copy(side):
        target = jnp.minimum(place + 1, last) if side == 0 else jnp.maximum(place - 1, 0)
        return copy_of(
            below_above.at[2], below_above.at[side], side_send.at[side], side_recv.at[side],
            target, wedge,
        )

    @pl.when(jnp.logical_not(sender))
    def _():
        for step in range(wedges):
            chip_copy(step).start()

    for step in range(1, wedges):
        wedge_copy(step).start()

    def halo_copies(number, high_rows, low_rows, packed, radial_halo, phi_halo):
        def copy(which, source, target, peer):
            return pltpu.make_async_remote_copy(
                src_ref=source, dst_ref=target, send_sem=halo_send.at[which],
                recv_sem=halo_recv.at[4 * number + which], device_id=peer, device_id_type=MESH,
            )

        return (
            copy(0, high_rows, radial_halo.at[0], at(jnp.minimum(place + 1, last), wedge)),
            copy(1, low_rows, radial_halo.at[1], at(jnp.maximum(place - 1, 0), wedge)),
            copy(2, packed.at[0], phi_halo.at[0], at(place, east)),
            copy(3, packed.at[1], phi_halo.at[1], at(place, west)),
        )

    def start_halos(copies, radial_halo, low_row, high_row):
        pl.when(place < last)(lambda: copies[0].start())
        pl.when(place > 0)(lambda: copies[1].start())
        copies[2].start()
        copies[3].start()

        @pl.when(place == 0)
        def _():
            for k in range(NV):
                for i in range(2):
                    radial_halo[0, k, pl.ds(width * i, width), :] = low_row(k)

        @pl.when(place == last)
        def _():
            for k in range(NV):
                for i in range(2):
                    radial_halo[1, k, pl.ds(width * i, width), :] = high_row(k)

    def wait_radial(copies):
        pl.when(place > 0)(lambda: copies[0].wait_recv())
        pl.when(place < last)(lambda: copies[1].wait_recv())

    def wait_sent(copies):
        pl.when(place < last)(lambda: copies[0].wait_send())
        pl.when(place > 0)(lambda: copies[1].wait_send())
        copies[2].wait_send()
        copies[3].wait_send()

    first_halos = halo_copies(
        0, u0.at[:, pl.ds(8 + (rows - 2) * width, 2 * width), :], u0.at[:, pl.ds(8, 2 * width), :],
        pk0, hr0, hp0,
    )
    start_halos(
        first_halos, hr0,
        lambda k: u0[k, pl.ds(8, width), :],
        lambda k: u0[k, pl.ds(8 + (rows - 1) * width, width), :],
    )

    answer()

    wide_lane = lax.broadcasted_iota(jnp.int32, (width, 128), 1)

    def keep(direction, side, where, state):
        for n, k in enumerate(STEADY):
            prep[direction, side, n, where, :] = state[k]
        for n, value in enumerate(side_ready(state)):
            prep[direction, side, len(STEADY) + n, where, :] = value

    def kept(direction, where, left, right):
        ready = []
        for side, state in enumerate((left, right)):
            for n, k in enumerate(STEADY):
                state[k] = prep[direction, side, n, where, :]
            ready.append(tuple(prep[direction, side, len(STEADY) + n, where, :] for n in range(3)))
        return ready

    def prepare(u):
        def one_row(r, carry):
            base = pl.multiple_of(8 + r * width, 8)
            where = pl.ds(pl.multiple_of(r * width, 8), width)
            left, right = {}, {}
            for k in STEADY:
                cell = u[k, pl.ds(base, width), :]
                high = (pltpu.roll(cell, 127, 1) - cell) * ct[4:5, :]
                low = (cell - pltpu.roll(cell, 1, 1)) * ct[5:6, :]
                slope = half_slope(low, high)
                left[k] = cell + slope
                right[k] = jnp.where(wide_lane == 127, cell, pltpu.roll(cell - slope, 127, 1))
            keep(0, 0, where, left)
            keep(0, 1, where, right)
            for k in STEADY:
                cell = u[k, pl.ds(base, width), :]
                low = 0.5 * (cell - u[k, pl.ds(base - 1, width), :])
                high = 0.5 * (u[k, pl.ds(base + 1, width), :] - cell)
                slope = half_slope(low, high)
                left[k] = pltpu.roll(cell + slope, 1, 0)
                right[k] = cell - slope
            keep(1, 0, where, left)
            keep(1, 1, where, right)
            return carry

        lax.fori_loop(0, rows, one_row, 0)

        def one_inner_row(r, carry):
            base = pl.multiple_of(8 + r * width, 8)
            where = pl.multiple_of(r * width, 8)
            left, right = {}, {}
            for k in STEADY:
                cell = u[k, pl.ds(base, width), :]
                low = 0.5 * (cell - u[k, pl.ds(base - width, width), :])
                high = 0.5 * (u[k, pl.ds(base + width, width), :] - cell)
                slope = half_slope(low, high)
                left[k], right[k] = cell + slope, cell - slope
            keep(2, 0, pl.ds(pl.multiple_of(where + width, 8), width), left)
            keep(2, 1, pl.ds(where, width), right)
            return carry

        lax.fori_loop(1, rows - 1, one_inner_row, 0)

    def polar_and_azimuth(u, prepared=False):
        moving = MOVED if prepared else range(NV)

        together = 2 if prepared else 1
        sine, inverse_sine, cotangent, mask = ct[0:1, :], ct[1:2, :], ct[2:3, :], ct[4:5, :]

        def third(i, n):
            r = jnp.maximum((i - 2) * together, 0) + n
            store = pl.ds(pl.multiple_of(r * width, 8), width)
            scale = tab[0, pl.ds(r, 1), :]
            cells = [u[k, pl.ds(pl.multiple_of(8 + r * width, 8), width), :] for k in range(NV)]
            source = sources(cells, cotangent)
            across = scale * inverse_sine
            for k in range(NV):
                through = th[k, store, :]
                value = cells[k] + across * (pltpu.roll(through, 1, 1) - through)
                if source[k] is not None:
                    value = value + scale * source[k]
                acc[k, store, :] = value

        def second(i, n):
            r = jnp.clip((i - 1) * together, 0, rows - together) + n
            store = pl.ds(pl.multiple_of(r * width, 8), width)
            left = {k: lt[k, store, :] for k in moving}
            right = {}
            for k in moving:
                value = rt[k, store, :]
                cell = u[k, pl.ds(pl.multiple_of(8 + r * width, 8), width), :]
                right[k] = jnp.where(wide_lane == 127, cell, pltpu.roll(value, 127, 1))
            ready = kept(0, store, left, right) if prepared else (None, None)
            flux = twice_flux(left, right, 2, ready, sine)
            for k in range(NV):
                th[k, store, :] = flux[k]

        def first(i, n):
            r = jnp.minimum(i * together, rows - together) + n
            base = pl.multiple_of(8 + r * width, 8)
            store = pl.ds(pl.multiple_of(r * width, 8), width)
            cells = {k: u[k, pl.ds(base, width), :] for k in moving}
            for k in moving:
                high = (pltpu.roll(cells[k], 127, 1) - cells[k]) * mask
                low = (cells[k] - pltpu.roll(cells[k], 1, 1)) * ct[5:6, :]
                slope = half_slope(low, high)
                lt[k, store, :] = cells[k] + slope
                rt[k, store, :] = cells[k] - slope
            left, right = {}, {}
            for k in moving:
                low = 0.5 * (cells[k] - u[k, pl.ds(base - 1, width), :])
                high = 0.5 * (u[k, pl.ds(base + 1, width), :] - cells[k])
                slope = half_slope(low, high)
                left[k] = pltpu.roll(cells[k] + slope, 1, 0)
                right[k] = cells[k] - slope
            ready = kept(1, store, left, right) if prepared else (None, None)
            flux = twice_flux(left, right, 3, ready)
            for k in range(NV):
                fp[k, pl.ds(pl.multiple_of(r * span, 8), width), :] = flux[k]

        def run(i, stages):
            for stage in stages:
                for n in range(together):
                    stage(i, n)

        def one_step(i, carry):
            run(i, (third, second, first))
            return carry

        steps = rows // together
        if prepared:
            run(0, (first,))
            run(1, (second, first))
            lax.fori_loop(2, steps, one_step, 0)
            run(steps, (third, second))
            run(steps + 1, (third,))
        else:
            lax.fori_loop(0, steps + 2, one_step, 0)

    def inner_radial(u, prepared=False):
        moving = MOVED if prepared else range(NV)

        def one_row(r, carry):
            base = pl.multiple_of(8 + r * width, 8)
            store = pl.multiple_of(r * width, 8)
            left, right = {}, {}
            for k in moving:
                cell = u[k, pl.ds(base, width), :]
                low = 0.5 * (cell - u[k, pl.ds(base - width, width), :])
                high = 0.5 * (u[k, pl.ds(base + width, width), :] - cell)
                slope = half_slope(low, high)
                right[k] = cell - slope
                left[k] = sl[k, pl.ds(store - width, width), :]
                sl[k, pl.ds(store, width), :] = cell + slope
            ready = kept(2, pl.ds(store, width), left, right) if prepared else (None, None)
            flux = twice_flux(left, right, 1, ready)
            for k in range(NV):
                fr[k, pl.ds(store, width), :] = flux[k]
            return carry

        two_at_a_time(1, rows - 1, one_row)

    def edge_azimuth(u, halo):
        for side in range(2):
            own = (0, 1, 2) if side == 0 else (width - 3, width - 2, width - 1)
            inside = [
                [u[k, pl.ds(8 + f, 8, stride=width), :] for k in range(NV)] for f in own
            ]
            outside = [[halo[side, k, i] for k in range(NV)] for i in range(2)]
            cells = outside + inside if side == 0 else inside + outside
            fluxes = edge_pair(cells, 3)
            faces = (0, 1) if side == 0 else (width - 1, width)
            for face, flux in zip(faces, fluxes):
                for k in range(NV):
                    fp[k, pl.ds(face, 8, stride=span), :] = flux[k]

    def edge_radial(u, halo):
        for side in range(2):
            own = (0, 1, 2) if side == 0 else (rows - 3, rows - 2, rows - 1)
            inside = [[u[k, pl.ds(8 + r * width, width), :] for k in range(NV)] for r in own]
            outside = [
                [halo[side, k, pl.ds(width * i, width), :] for k in range(NV)] for i in range(2)
            ]
            cells = outside + inside if side == 0 else inside + outside
            fluxes = edge_pair(cells, 1)
            faces = (0, 1) if side == 0 else (rows - 1, rows)
            for face, flux in zip(faces, fluxes):
                for k in range(NV):
                    fr[k, pl.ds(face * width, width), :] = flux[k]

    azimuth_scale = 0.5 / phi_step

    def advanced_row(r):
        store = pl.multiple_of(r * width, 8)
        low_area, high_area = tab[1, pl.ds(r, 1), :], tab[2, pl.ds(r, 1), :]
        across = tab[0, pl.ds(r, 1), :] * ct[1:2, :] * azimuth_scale
        below = pl.multiple_of(r * span, 8)
        values = []
        for k in range(NV):
            values.append(
                acc[k, pl.ds(store, width), :]
                + across * (fp[k, pl.ds(below, width), :] - fp[k, pl.ds(below + 1, width), :])
                + low_area * fr[k, pl.ds(store, width), :]
                - high_area * fr[k, pl.ds(pl.multiple_of(store + width, 8), width), :]
            )
        return values

    with jax.named_scope("pre1"):
        polar_and_azimuth(u0)
    with jax.named_scope("rad1"):
        inner_radial(u0)

    with jax.named_scope("wedge_wait"):
        wedge_all().wait_recv()
    shell_row = wedge_rows[0]
    for j in range(1, wedges):
        shell_row = shell_row + wedge_rows[j]
    below_above[2] = shell_row
    pl.when(place < last)(lambda: side_copy(0).start())
    pl.when(place > 0)(lambda: side_copy(1).start())

    @pl.when(sender)
    def _():
        many(wedges, chip_send, chip_recv).wait_recv()
        chip_row = shell_row
        for j in range(wedges):
            chip_row = chip_row + chip_rows[j]
        below_above[3] = chip_row
        send_across(0, jnp.minimum(level, near))
        pl.when(near_answers > 0)(lambda: pl.semaphore_wait(from_near, near_answers))
        send_across(jnp.minimum(level, near), near)

    with jax.named_scope("h1_phi_wait"):
        first_halos[2].wait_recv()
        first_halos[3].wait_recv()
    with jax.named_scope("edge_phi1"):
        edge_azimuth(u0, hp0)
    with jax.named_scope("h1_rad_wait"):
        wait_radial(first_halos)
    with jax.named_scope("edge_rad1"):
        edge_radial(u0, hr0)

    def section_one_row(r, carry):
        values = advanced_row(r)
        for k in range(NV):
            u1[k, pl.ds(pl.multiple_of(8 + r * width, 8), width), :] = values[k]
        return carry

    with jax.named_scope("final1"):
        two_at_a_time(0, rows, section_one_row)
    for k in range(NV):
        sr[0, k] = u1[k, pl.ds(8 + (rows - 2) * width, 2 * width), :]
        sr[1, k] = u1[k, pl.ds(8, 2 * width), :]
    pack(u1, pk1)
    wait_sent(first_halos)
    second_halos = halo_copies(1, sr.at[0], sr.at[1], pk1, hr1, hp1)
    start_halos(
        second_halos, hr1,
        lambda k: sr[1, k, pl.ds(0, width), :],
        lambda k: sr[0, k, pl.ds(width, width), :],
    )

    with jax.named_scope("asc_wait"):
        pl.when(far_answers > 0)(lambda: pl.semaphore_wait(from_far, far_answers))
    pl.when(sender)(send_along)

    def gather_across():
        for x in range(1, groups):

            @pl.when(group == x)
            def _(count=x):
                many(count * levels, shared_send, shared_recv).wait_recv()
                value = [shared[n] for n in range(count)]
                for z in range(1, levels):
                    value = [value[n] + shared[z * groups + n] for n in range(count)]
                inside_rows[0] = functools.reduce(jnp.add, value)
                for passer, z_start, z_stop in passers:

                    @pl.when(jnp.logical_and(sender, level == passer))
                    def _(z_start=z_start, z_stop=z_stop):
                        for z in range(z_start, z_stop):
                            for c in both:
                                pass_copy(z, c).start()

    def gather_along():
        for z in range(1, levels):

            @pl.when(level == z)
            def _(z=z):
                many(z, along_send, along_recv).wait_recv()
                inside_rows[2] = functools.reduce(jnp.add, [along[n] for n in range(z)])

    half_of = lambda index: jnp.where(lane < index, 1.0, jnp.where(lane == index, 0.5, 0.0))
    none = jnp.zeros((8, 128), jnp.float32)
    lower = jnp.where(row < 2, jnp.where(place == 0, half_of(0), none), 0.0)
    upper = jnp.where(row < 2, none, jnp.where(place == last, half_of(rows - 1), 1.0))
    minus = jnp.where(lane >= rows, 0.0, half_of(rows - 2 + row) - 1.0)
    minus = jnp.where(jnp.logical_and(row < 2, place > 0), minus, none)
    plus = jnp.where(jnp.logical_or(row < 2, place == last), none, half_of(row - 2))
    beyond = jnp.clip(first + jnp.where(row < 2, row - 2, rows - 2 + row), 0, slabs * rows - 1)
    weights[0] = half_of(row)
    weights[1] = lower + upper
    weights[2] = minus
    weights[3] = plus
    for i, target in enumerate((first + row, beyond)):
        inverse = 1.0 / radius_of(target)
        weights[4 + i] = (timestep * strength) * inverse * inverse
    fetch_mass.wait()

    with jax.named_scope("prepare"):
        prepare(u1)
    with jax.named_scope("m1_wait"):
        pl.when(is_near)(gather_across)
        gather_along()
        pl.when(jnp.logical_and(group > 0, jnp.logical_not(is_near)))(
            lambda: pass_copy(levels - 1, 1).wait_recv()
        )
        pl.when(place > 0)(lambda: side_copy(0).wait_recv())
        pl.when(place < last)(lambda: side_copy(1).wait_recv())
    below, above, own = below_above[0], below_above[1], below_above[2]
    smaller_x = jnp.where(is_near, inside_rows[0], inside_rows[1])
    inside = jnp.where(level > 0, inside_rows[2], 0.0)
    inside = inside + jnp.where(group > 0, smaller_x, 0.0) + jnp.where(core_index == 1, below, 0.0)
    table = (
        inside + weights[0] * own,
        inside + weights[1] * own + weights[2] * below + weights[3] * above,
    )
    for i in range(2):
        enclosed = jnp.sum(table[i], axis=1, keepdims=True) + core[0]
        grav[8 * i : 8 * i + 8, :] = weights[4 + i] * enclosed
        if i == 0:
            enclosed_ref[...] = jnp.sum(
                jnp.where(lane == row, enclosed, 0.0), axis=0, keepdims=True
            )[:, :rows]

    def gravity_row(r, carry):
        base = pl.ds(pl.multiple_of(8 + r * width, 8), width)
        pull = grav[pl.ds(r, 1), :]
        u1[1, base, :] = u1[1, base, :] - pull * jnp.maximum(u0[0, base, :], MINIMUM_DENSITY)
        u1[4, base, :] = u1[4, base, :] - pull * u0[1, base, :]
        return carry

    with jax.named_scope("grav"):
        two_at_a_time(0, rows, gravity_row)

    with jax.named_scope("pre2"):
        polar_and_azimuth(u1, prepared=True)
    with jax.named_scope("rad2"):
        inner_radial(u1, prepared=True)
    with jax.named_scope("h2_phi_wait"):
        second_halos[2].wait_recv()
        second_halos[3].wait_recv()
    pull = grav[0:8, :]
    for side in range(2):
        for i in range(2):
            hp1[side, 1, i] = hp1[side, 1, i] - pull * jnp.maximum(
                hp0[side, 0, i], MINIMUM_DENSITY
            )
            hp1[side, 4, i] = hp1[side, 4, i] - pull * hp0[side, 1, i]
    with jax.named_scope("edge_phi2"):
        edge_azimuth(u1, hp1)
    with jax.named_scope("h2_rad_wait"):
        wait_radial(second_halos)
    for side in range(2):
        for i in range(2):
            which = pl.ds(width * i, width)
            pull = grav[8 + 2 * side + i : 9 + 2 * side + i, :]
            hr1[side, 1, which, :] = hr1[side, 1, which, :] - pull * jnp.maximum(
                hr0[side, 0, which, :], MINIMUM_DENSITY
            )
            hr1[side, 4, which, :] = hr1[side, 4, which, :] - pull * hr0[side, 1, which, :]
    with jax.named_scope("edge_rad2"):
        edge_radial(u1, hr1)

    def section_two_row(r, carry):
        values = advanced_row(r)
        base = pl.ds(pl.multiple_of(8 + r * width, 8), width)
        pull = grav[pl.ds(r, 1), :]
        values[1] = values[1] - pull * jnp.maximum(u1[0, base, :], MINIMUM_DENSITY)
        values[4] = values[4] - pull * u1[1, base, :]
        for k in range(NV):
            outv[k, pl.ds(pl.multiple_of(r * width, 8), width), :] = 0.5 * (
                u0[k, base, :] + values[k]
            )
        return carry

    with jax.named_scope("final2"):
        two_at_a_time(0, rows, section_two_row)
    with jax.named_scope("drain"):
        @pl.when(sender)
        def _():
            for x in range(groups - 1):

                @pl.when(group == x)
                def _(count=2 * near * (groups - 1 - x)):
                    many(count, shared_send, shared_recv).wait_send()

            for z in range(levels - 1):
                pl.when(level == z)(
                    lambda count=2 * (levels - 1 - z): many(
                        count, along_send, along_recv
                    ).wait_send()
                )
            for passer, z_start, z_stop in passers:
                pl.when(jnp.logical_and(group > 0, level == passer))(
                    lambda count=2 * (z_stop - z_start): many(
                        count, pass_send, pass_recv
                    ).wait_send()
                )

        pl.when(jnp.logical_not(sender))(lambda: many(wedges, chip_send, chip_recv).wait_send())
        wedge_all().wait_send()
        pl.when(place < last)(lambda: side_copy(0).wait_send())
        pl.when(place > 0)(lambda: side_copy(1).wait_send())
        wait_sent(second_halos)


def put_out(advanced, enclosed, advanced_hbm, enclosed_hbm, sem):
    copies = [
        pltpu.make_async_copy(advanced, advanced_hbm, sem.at[0]),
        pltpu.make_async_copy(enclosed, enclosed_hbm, sem.at[1]),
    ]
    for copy in copies:
        copy.start()
    for copy in copies:
        copy.wait()


def body(groups, conserved, core_mass):
    _, rows, width, lanes = conserved.shape
    slabs, wedges = lax.axis_size("radial"), lax.axis_size("phi")
    inner = slabs // groups
    radial_step, theta_step, phi_step, timestep = step_sizes(rows * slabs, width * wedges, lanes)
    centers = (np.arange(lanes) + 0.5) * theta_step
    faces = (np.arange(lanes) + 1.0) * theta_step
    angles = np.zeros((8, lanes))
    angles[0] = np.sin(faces) * (0.5 / theta_step)
    angles[1] = 1.0 / np.sin(centers)
    angles[2] = np.cos(centers) / np.sin(centers)
    angles[3] = np.sin(centers)
    angles[4] = np.where(np.arange(lanes) == lanes - 1, 0.0, 0.5)
    angles[5] = np.where(np.arange(lanes) == 0, 0.0, 0.5)
    angles = jnp.asarray(angles.astype(np.float32))
    sizes = (rows, width, slabs, wedges, groups, radial_step, theta_step, phi_step, timestep)
    f32 = jnp.float32
    vmem = lambda *shape: pltpu.VMEM(shape, f32)
    dma = lambda count: pltpu.SemaphoreType.DMA((count,))
    in_hbm = lambda value: pltpu.with_memory_space_constraint(value, pltpu.HBM)
    cells = rows * width
    advanced, enclosed = pl.pallas_call(
        functools.partial(kernel, sizes),
        out_shape=(
            jax.ShapeDtypeStruct((NV, cells, lanes), f32),
            jax.ShapeDtypeStruct((1, rows), f32),
        ),
        in_specs=[
            pl.BlockSpec(memory_space=pltpu.HBM),
            pl.BlockSpec(memory_space=pltpu.HBM),
            pl.BlockSpec(memory_space=pltpu.HBM),
        ],
        out_specs=(
            pl.BlockSpec(memory_space=pltpu.VMEM),
            pl.BlockSpec(memory_space=pltpu.VMEM),
        ),
        scratch_shapes=[
            vmem(NV, cells + 16, lanes), vmem(NV, cells + 16, lanes),
            vmem(2, NV, 2 * width, lanes), vmem(2, NV, 2 * width, lanes),
            vmem(2, NV, 2, 8, lanes), vmem(2, NV, 2, 8, lanes),
            vmem(2, NV, 2, 8, lanes), vmem(2, NV, 2, 8, lanes),
            vmem(2, NV, 2 * width, lanes),
            vmem(NV, cells, lanes),
            vmem(NV, rows * (width + 8), lanes),
            vmem(NV, cells + width, lanes),
            vmem(NV, cells, lanes),
            vmem(NV, cells, lanes), vmem(NV, cells, lanes), vmem(NV, cells, lanes),
            vmem(3, 2, len(STEADY) + 3, cells, lanes),
            vmem(slabs // 2, 1, lanes), vmem(inner // 2, 1, lanes), vmem(4, 1, lanes), vmem(wedges, 1, lanes),
            vmem(wedges, 1, lanes), vmem(3, 1, lanes), vmem(6, 8, lanes),
            vmem(3, 8, lanes), vmem(16, lanes), vmem(8, lanes), pltpu.SMEM((1,), f32),
            dma(4), dma(4), dma(8), *[pltpu.SemaphoreType.DMA] * 4, dma(2), dma(2),
            pltpu.SemaphoreType.DMA, pltpu.SemaphoreType.DMA,
            pltpu.SemaphoreType.DMA, pltpu.SemaphoreType.DMA,
            pltpu.SemaphoreType.DMA, pltpu.SemaphoreType.DMA,
            pltpu.SemaphoreType.REGULAR, pltpu.SemaphoreType.REGULAR,
        ],
        compiler_params=pltpu.CompilerParams(
            collective_id=0, has_side_effects=True, vmem_limit_bytes=12 << 20
        ),
    )(in_hbm(conserved.reshape(NV, cells, lanes)), core_mass, in_hbm(angles))
    advanced, enclosed = pl.pallas_call(
        put_out,
        out_shape=(
            jax.ShapeDtypeStruct((NV, cells, lanes), f32),
            jax.ShapeDtypeStruct((1, rows), f32),
        ),
        in_specs=[pl.BlockSpec(memory_space=pltpu.VMEM)] * 2,
        out_specs=[pl.BlockSpec(memory_space=pltpu.HBM)] * 2,
        scratch_shapes=[dma(2)],
        compiler_params=pltpu.CompilerParams(vmem_limit_bytes=4 << 20),
    )(advanced, enclosed)
    return advanced.reshape(conserved.shape), enclosed.reshape(rows)


def solution(mesh):
    in_specs = (P(None, "radial", "phi", None), P())
    out_specs = (P(None, "radial", "phi", None), P("radial"))
    return jax.shard_map(
        functools.partial(body, 4), mesh=mesh, in_specs=in_specs, out_specs=out_specs,
        check_vma=False,
    )
```

```python
import functools
import math

import jax
import jax.numpy as jnp
import numpy as np
from jax import lax
from jax.experimental import pallas as pl
from jax.experimental.pallas import tpu as pltpu
from jax.sharding import PartitionSpec as P

ADIABATIC = 4.0 / 3.0
INNER_RADIUS = 1.0
OUTER_RADIUS = 2.0
COURANT = 0.4
GRAVITY_KICK = 0.004
MINIMUM_DENSITY = 0.05
PRESSURE_FLOOR = 0.01

NV = 8
STEADY = (0, 2, 3, 5, 6, 7)
MOVED = (1, 4)
MESH = pl.DeviceIdType.MESH


def step_sizes(radial_total, phi_total, theta_total):
    theta_step = math.pi / theta_total
    phi_step = 2.0 * math.pi / phi_total
    polar_width = INNER_RADIUS * math.sin(0.5 * theta_step) * phi_step
    radial_step = min(2.0 * polar_width, (OUTER_RADIUS - INNER_RADIUS) / radial_total)
    timestep = COURANT * min(radial_step, polar_width)
    return (radial_step, theta_step, phi_step, timestep)


def half_slope(low, high):
    return jnp.maximum(jnp.minimum(low, high), jnp.minimum(jnp.maximum(low, high), 0.0))


def side_ready(state):
    density = jnp.maximum(state[0], MINIMUM_DENSITY)
    squares = state[2] * state[2] + state[3] * state[3]
    return 1.0 / density, squares, PRESSURE_FLOOR * density


def face_side(state, component, ready=None):
    if ready is None:
        ready = side_ready(state)
    inverse, squares, floor = ready
    squares = state[1] * state[1] + squares
    pressure = jnp.maximum((ADIABATIC - 1.0) * (state[4] - 0.5 * squares * inverse), floor)
    normal = state[component] * inverse
    square = ADIABATIC * pressure * inverse
    sound = square * lax.rsqrt(square)
    return pressure, normal, jnp.abs(normal) + sound


def twice_flux(left, right, component, ready=(None, None), factor=None):
    left_p, left_v, left_s = face_side(left, component, ready[0])
    right_p, right_v, right_s = face_side(right, component, ready[1])
    signal = jnp.maximum(left_s, right_s)
    left_w, right_w = left_v + signal, right_v - signal
    if factor is not None:
        left_w, right_w = left_w * factor, right_w * factor
        left_p, right_p = left_p * factor, right_p * factor
    flux = [left[k] * left_w + right[k] * right_w for k in range(NV)]
    flux[component] = flux[component] + (left_p + right_p)
    flux[4] = flux[4] + (left_p * left_v + right_p * right_v)
    return flux


def edge_pair(cells, component):
    lefts, rights = [], []
    for k in range(NV):
        halves = [0.5 * (cells[i + 1][k] - cells[i][k]) for i in range(4)]
        slopes = [half_slope(halves[i], halves[i + 1]) for i in range(3)]
        lefts.append((cells[1][k] + slopes[0], cells[2][k] + slopes[1]))
        rights.append((cells[2][k] - slopes[1], cells[3][k] - slopes[2]))
    return [
        twice_flux([a[i] for a in lefts], [b[i] for b in rights], component) for i in range(2)
    ]


def two_at_a_time(start, stop, one_row):
    def two_rows(i, carry):
        for n in range(2):
            one_row(start + 2 * i + n, carry)
        return carry

    lax.fori_loop(0, (stop - start) // 2, two_rows, 0)


def row_sum(r, part, width, acc, fp, fr, tab, ct):
    store = r * width if isinstance(r, int) else pl.multiple_of(r * width, 8)
    below = r * (width + 8) if isinstance(r, int) else pl.multiple_of(r * (width + 8), 8)
    following = store + width if isinstance(r, int) else pl.multiple_of(store + width, 8)
    low_area, high_area = part * tab[1, pl.ds(r, 1), :], part * tab[2, pl.ds(r, 1), :]
    across = part * tab[0, pl.ds(r, 1), :] * ct[6:7, :]
    return [
        acc[k, pl.ds(store, width), :]
        + across * (fp[k, pl.ds(below, width), :] - fp[k, pl.ds(below + 1, width), :])
        + low_area * fr[k, pl.ds(store, width), :]
        - high_area * fr[k, pl.ds(following, width), :]
        for k in range(NV)
    ]


def sources(cells, cotangent):
    density = jnp.maximum(cells[0], MINIMUM_DENSITY)
    inverse = 1.0 / density
    speed = [None] + [cells[m] * inverse for m in (1, 2, 3)]
    squares = cells[1] * speed[1] + cells[2] * speed[2] + cells[3] * speed[3]
    pressure = jnp.maximum(
        (ADIABATIC - 1.0) * (cells[4] - 0.5 * squares), PRESSURE_FLOOR * density
    )
    spin = cells[3] * speed[3]
    source = [None] * NV
    source[1] = 2.0 * pressure + (cells[2] * speed[2] + spin)
    source[2] = (pressure + spin) * cotangent - cells[1] * speed[2]
    source[3] = -speed[3] * (cells[1] + cells[2] * cotangent)
    return source, density


def kernel(
    sizes, state_hbm, mass_hbm, angles_hbm,
    acc, fp, fr, tab, ct, enclosed_ref,
    u0, u1, hr0, hr1, hp0, hp1, pk0, pk1, sr, sl, lt, rt, th, prep,
    shared, along, below_above, wedge_rows, chip_rows, inside_rows, weights, grav, core,
    in_sem, halo_send, halo_recv, shared_send, shared_recv, along_send, along_recv,
    side_send, side_recv, pass_send, pass_recv, wedge_send, wedge_recv, chip_send, chip_recv,
    from_near, from_far,
):
    rows, width, slabs, wedges, groups, radial_step, theta_step, phi_step, timestep = sizes
    strength = GRAVITY_KICK / timestep
    place = lax.axis_index("radial")
    wedge = lax.axis_index("phi")
    inner = slabs // groups
    levels = inner // 2
    group, member = place // inner, lax.rem(place, inner)
    level, core_index = member // 2, lax.rem(member, 2)
    span = width + 8
    last = slabs - 1

    def at(radial, phi):
        return {"radial": radial, "phi": phi}

    def signal(semaphore, radial, phi):
        pl.semaphore_signal(semaphore, inc=1, device_id=at(radial, phi), device_id_type=MESH)

    east, west = lax.rem(wedge + 1, wedges), lax.rem(wedge + wedges - 1, wedges)

    fetch_mass = pltpu.make_async_copy(mass_hbm, core, in_sem.at[3])
    fetch_density = pltpu.make_async_copy(
        state_hbm.at[pl.ds(0, 1)], u0.at[pl.ds(0, 1), pl.ds(8, rows * width), :], in_sem.at[0]
    )
    fetch = pltpu.make_async_copy(
        state_hbm.at[pl.ds(1, NV - 1)], u0.at[pl.ds(1, NV - 1), pl.ds(8, rows * width), :],
        in_sem.at[1],
    )
    fetch_angles = pltpu.make_async_copy(angles_hbm, ct, in_sem.at[2])
    for copy in (fetch_density, fetch_angles, fetch, fetch_mass):
        copy.start()

    for side in range(2):
        below_above[side] = jnp.zeros((1, 128), jnp.float32)

    barrier = pltpu.get_barrier_semaphore()
    for step in range(1, wedges):
        signal(barrier, place, lax.rem(wedge + step, wedges))
    pl.when(place < last)(lambda: signal(barrier, place + 1, wedge))
    pl.when(place > 0)(lambda: signal(barrier, place - 1, wedge))

    def greet(x_start, x_stop, z_start, z_stop, cores, semaphore):
        def one_level(back, carry):
            z = z_start + z_stop - 1 - back

            def one_group(x, inner_carry):
                for c in cores:
                    signal(semaphore, x * inner + z * 2 + c, wedge)
                return inner_carry

            return lax.fori_loop(x_start, x_stop, one_group, carry)

        lax.fori_loop(z_start, z_stop, one_level, 0)

    near = levels // 4
    is_near = level < near
    sender = core_index == 1
    both = (0, 1)

    pl.when(is_near)(lambda: greet(0, group, level + 1, levels, (1,), barrier))

    @pl.when(sender)
    def _():
        for step in range(1, wedges):
            signal(barrier, place - 1, lax.rem(wedge + step, wedges))
        greet(group, group + 1, level + 1, levels, both, barrier)
        pl.when(is_near)(lambda: greet(group + 1, groups, level, near, both, barrier))

    def answer():
        greet(group, group + 1, 0, level, (1,), from_far)
        pl.when(is_near)(lambda: greet(0, group, 0, level + 1, (1,), from_near))

    near_answers = jnp.where(
        jnp.logical_and(sender, is_near), 2 * (groups - 1 - group) * (near - level), 0
    )
    far_answers = jnp.where(sender, 2 * (levels - 1 - level), 0)
    greetings = (
        wedges - 1 + jnp.where(place > 0, 1, 0) + jnp.where(place < last, 1, 0) + level
        + jnp.where(is_near, group * (level + 1), 0)
        + jnp.where(sender, 2 * (groups - 1 - group) * jnp.minimum(level, near), wedges - 1)
    )

    row = lax.broadcasted_iota(jnp.int32, (8, 128), 0)
    lane = lax.broadcasted_iota(jnp.int32, (8, 128), 1)
    first = place * rows

    def radius_of(index):
        return INNER_RADIUS + (index.astype(jnp.float32) + 0.5) * radial_step

    radius = radius_of(first + row)
    inverse_radius = 1.0 / radius
    low_face, high_face = radius - 0.5 * radial_step, radius + 0.5 * radial_step
    area = inverse_radius * inverse_radius * (0.5 * timestep / radial_step)
    tab[0] = timestep * inverse_radius
    tab[1] = low_face * low_face * area
    tab[2] = high_face * high_face * area

    with jax.named_scope("fetch_wait"):
        fetch_angles.wait()
        fetch_density.wait()
    total = u0[0, pl.ds(8, 8, stride=width), :]
    for f in range(1, width):
        total = total + u0[0, pl.ds(8 + f, 8, stride=width), :]
    shells = jnp.sum(total * ct[3:4, :], axis=1, keepdims=True) * (
        radius * radius * (radial_step * theta_step * phi_step)
    )
    wedge_rows[0] = jnp.sum(jnp.where(lane == row, shells, 0.0), axis=0, keepdims=True)

    def pack(source, packed):
        for side, zones in enumerate(((width - 2, width - 1), (0, 1))):
            for k in range(NV):
                for i, zone in enumerate(zones):
                    packed[side, k, i] = source[k, pl.ds(8 + zone, 8, stride=width), :]

    with jax.named_scope("barrier_wait"):
        pl.semaphore_wait(barrier, greetings)

    def copy_of(source, target, send, recv, radial, phi):
        return pltpu.make_async_remote_copy(
            src_ref=source, dst_ref=target, send_sem=send, recv_sem=recv,
            device_id=at(radial, phi), device_id_type=MESH,
        )

    def send_across(z_start, z_stop):
        def one_group(x, carry):
            def one_level(z, inner_carry):
                for c in both:
                    copy_of(
                        below_above.at[3], shared.at[level * groups + group], shared_send,
                        shared_recv, x * inner + z * 2 + c, wedge,
                    ).start()
                return inner_carry

            return lax.fori_loop(z_start, z_stop, one_level, carry)

        lax.fori_loop(group + 1, groups, one_group, 0)

    def send_along():
        def one_level(z, carry):
            for c in both:
                copy_of(
                    below_above.at[3], along.at[level], along_send, along_recv,
                    group * inner + z * 2 + c, wedge,
                ).start()
            return carry

        lax.fori_loop(level + 1, levels, one_level, 0)

    def many(count, send, recv):
        rows_of = shared.at[pl.ds(0, count)]
        return copy_of(rows_of, rows_of, send, recv, place, wedge)

    passers = (
        (near - 1, near, near + (levels - near + 1) // 2),
        (0, near + (levels - near + 1) // 2, levels),
    )

    def pass_copy(z, c):
        return copy_of(
            inside_rows.at[0], inside_rows.at[1], pass_send, pass_recv,
            group * inner + z * 2 + c, wedge,
        )

    def chip_copy(step):
        return copy_of(
            wedge_rows.at[0], chip_rows.at[step], chip_send, chip_recv,
            jnp.minimum(place + 1, last), lax.rem(wedge + step, wedges),
        )

    def wedge_copy(step):
        return copy_of(
            wedge_rows.at[0], wedge_rows.at[step], wedge_send, wedge_recv, place,
            lax.rem(wedge + step, wedges),
        )

    def wedge_all():
        others = wedge_rows.at[pl.ds(1, wedges - 1)]
        return copy_of(others, others, wedge_send, wedge_recv, place, east)

    def side_copy(side):
        target = jnp.minimum(place + 1, last) if side == 0 else jnp.maximum(place - 1, 0)
        return copy_of(
            below_above.at[2], below_above.at[side], side_send.at[side], side_recv.at[side],
            target, wedge,
        )

    @pl.when(jnp.logical_not(sender))
    def _():
        for step in range(wedges):
            chip_copy(step).start()

    for step in range(1, wedges):
        wedge_copy(step).start()

    fetch.wait()
    pack(u0, pk0)

    def halo_copies(number, high_rows, low_rows, packed, radial_halo, phi_halo):
        def copy(which, source, target, peer):
            return pltpu.make_async_remote_copy(
                src_ref=source, dst_ref=target, send_sem=halo_send.at[which],
                recv_sem=halo_recv.at[4 * number + which], device_id=peer, device_id_type=MESH,
            )

        return (
            copy(0, high_rows, radial_halo.at[0], at(jnp.minimum(place + 1, last), wedge)),
            copy(1, low_rows, radial_halo.at[1], at(jnp.maximum(place - 1, 0), wedge)),
            copy(2, packed.at[0], phi_halo.at[0], at(place, east)),
            copy(3, packed.at[1], phi_halo.at[1], at(place, west)),
        )

    def start_halos(copies, radial_halo, low_row, high_row):
        pl.when(place < last)(lambda: copies[0].start())
        pl.when(place > 0)(lambda: copies[1].start())
        copies[2].start()
        copies[3].start()

        @pl.when(place == 0)
        def _():
            for k in range(NV):
                for i in range(2):
                    radial_halo[0, k, pl.ds(width * i, width), :] = low_row(k)

        @pl.when(place == last)
        def _():
            for k in range(NV):
                for i in range(2):
                    radial_halo[1, k, pl.ds(width * i, width), :] = high_row(k)

    def wait_radial(copies):
        pl.when(place > 0)(lambda: copies[0].wait_recv())
        pl.when(place < last)(lambda: copies[1].wait_recv())

    def wait_sent(copies):
        pl.when(place < last)(lambda: copies[0].wait_send())
        pl.when(place > 0)(lambda: copies[1].wait_send())
        copies[2].wait_send()
        copies[3].wait_send()

    first_halos = halo_copies(
        0, u0.at[:, pl.ds(8 + (rows - 2) * width, 2 * width), :], u0.at[:, pl.ds(8, 2 * width), :],
        pk0, hr0, hp0,
    )
    start_halos(
        first_halos, hr0,
        lambda k: u0[k, pl.ds(8, width), :],
        lambda k: u0[k, pl.ds(8 + (rows - 1) * width, width), :],
    )

    answer()

    wide_lane = lax.broadcasted_iota(jnp.int32, (width, 128), 1)

    def keep(direction, side, where, state):
        for n, k in enumerate(STEADY):
            prep[direction, side, n, where, :] = state[k]
        for n, value in enumerate(side_ready(state)):
            prep[direction, side, len(STEADY) + n, where, :] = value

    def kept(direction, where, left, right):
        ready = []
        for side, state in enumerate((left, right)):
            for n, k in enumerate(STEADY):
                state[k] = prep[direction, side, n, where, :]
            ready.append(tuple(prep[direction, side, len(STEADY) + n, where, :] for n in range(3)))
        return ready

    def prepare(u):
        def one_row(r, carry):
            base = pl.multiple_of(8 + r * width, 8)
            where = pl.ds(pl.multiple_of(r * width, 8), width)
            left, right = {}, {}
            for k in STEADY:
                cell = u[k, pl.ds(base, width), :]
                high = (pltpu.roll(cell, 127, 1) - cell) * ct[4:5, :]
                low = (cell - pltpu.roll(cell, 1, 1)) * ct[5:6, :]
                slope = half_slope(low, high)
                left[k] = cell + slope
                right[k] = jnp.where(wide_lane == 127, cell, pltpu.roll(cell - slope, 127, 1))
            keep(0, 0, where, left)
            keep(0, 1, where, right)
            for k in STEADY:
                cell = u[k, pl.ds(base, width), :]
                low = 0.5 * (cell - u[k, pl.ds(base - 1, width), :])
                high = 0.5 * (u[k, pl.ds(base + 1, width), :] - cell)
                slope = half_slope(low, high)
                left[k] = pltpu.roll(cell + slope, 1, 0)
                right[k] = cell - slope
            keep(1, 0, where, left)
            keep(1, 1, where, right)
            return carry

        lax.fori_loop(0, rows, one_row, 0)

        def one_inner_row(r, carry):
            base = pl.multiple_of(8 + r * width, 8)
            where = pl.multiple_of(r * width, 8)
            left, right = {}, {}
            for k in STEADY:
                cell = u[k, pl.ds(base, width), :]
                low = 0.5 * (cell - u[k, pl.ds(base - width, width), :])
                high = 0.5 * (u[k, pl.ds(base + width, width), :] - cell)
                slope = half_slope(low, high)
                left[k], right[k] = cell + slope, cell - slope
            keep(2, 0, pl.ds(pl.multiple_of(where + width, 8), width), left)
            keep(2, 1, pl.ds(where, width), right)
            return carry

        lax.fori_loop(1, rows - 1, one_inner_row, 0)

    def polar_and_azimuth(u, prepared=False):
        moving = MOVED if prepared else range(NV)

        together = 2 if prepared else 1
        sine, inverse_sine, cotangent, mask = ct[0:1, :], ct[1:2, :], ct[2:3, :], ct[4:5, :]

        def third(i, n):
            r = jnp.maximum((i - 2) * together, 0) + n
            store = pl.ds(pl.multiple_of(r * width, 8), width)
            scale = tab[0, pl.ds(r, 1), :]
            cells = [u[k, pl.ds(pl.multiple_of(8 + r * width, 8), width), :] for k in range(NV)]
            source, density = sources(cells, cotangent)
            pull = grav[pl.ds(r, 1), :]
            across = scale * inverse_sine
            for k in range(NV):
                through = th[k, store, :]
                value = cells[k] + across * (pltpu.roll(through, 1, 1) - through)
                if source[k] is not None:
                    value = value + scale * source[k]
                if prepared:
                    if k == 1:
                        value = value - pull * density
                    elif k == 4:
                        value = value - pull * cells[1]
                    before = u0[k, pl.ds(pl.multiple_of(8 + r * width, 8), width), :]
                    value = 0.5 * (before + value)
                acc[k, store, :] = value

        def second(i, n):
            r = jnp.clip((i - 1) * together, 0, rows - together) + n
            store = pl.ds(pl.multiple_of(r * width, 8), width)
            left = {k: lt[k, store, :] for k in moving}
            right = {}
            for k in moving:
                value = rt[k, store, :]
                cell = u[k, pl.ds(pl.multiple_of(8 + r * width, 8), width), :]
                right[k] = jnp.where(wide_lane == 127, cell, pltpu.roll(value, 127, 1))
            ready = kept(0, store, left, right) if prepared else (None, None)
            flux = twice_flux(left, right, 2, ready, sine)
            for k in range(NV):
                th[k, store, :] = flux[k]

        def first(i, n):
            r = jnp.minimum(i * together, rows - together) + n
            base = pl.multiple_of(8 + r * width, 8)
            store = pl.ds(pl.multiple_of(r * width, 8), width)
            cells = {k: u[k, pl.ds(base, width), :] for k in moving}
            for k in moving:
                high = (pltpu.roll(cells[k], 127, 1) - cells[k]) * mask
                low = (cells[k] - pltpu.roll(cells[k], 1, 1)) * ct[5:6, :]
                slope = half_slope(low, high)
                lt[k, store, :] = cells[k] + slope
                rt[k, store, :] = cells[k] - slope
            left, right = {}, {}
            for k in moving:
                low = 0.5 * (cells[k] - u[k, pl.ds(base - 1, width), :])
                high = 0.5 * (u[k, pl.ds(base + 1, width), :] - cells[k])
                slope = half_slope(low, high)
                left[k] = pltpu.roll(cells[k] + slope, 1, 0)
                right[k] = cells[k] - slope
            ready = kept(1, store, left, right) if prepared else (None, None)
            flux = twice_flux(left, right, 3, ready)
            for k in range(NV):
                fp[k, pl.ds(pl.multiple_of(r * span, 8), width), :] = flux[k]

        def run(i, stages):
            for stage in stages:
                for n in range(together):
                    stage(i, n)

        def one_step(i, carry):
            run(i, (third, second, first))
            return carry

        steps = rows // together
        if prepared:
            run(0, (first,))
            run(1, (second, first))
            lax.fori_loop(2, steps, one_step, 0)
            run(steps, (third, second))
            run(steps + 1, (third,))
        else:
            lax.fori_loop(0, steps + 2, one_step, 0)

    def inner_radial(u, prepared=False):
        moving = MOVED if prepared else range(NV)

        def one_row(r, carry):
            base = pl.multiple_of(8 + r * width, 8)
            store = pl.multiple_of(r * width, 8)
            left, right = {}, {}
            for k in moving:
                cell = u[k, pl.ds(base, width), :]
                low = 0.5 * (cell - u[k, pl.ds(base - width, width), :])
                high = 0.5 * (u[k, pl.ds(base + width, width), :] - cell)
                slope = half_slope(low, high)
                right[k] = cell - slope
                left[k] = sl[k, pl.ds(store - width, width), :]
                sl[k, pl.ds(store, width), :] = cell + slope
            ready = kept(2, pl.ds(store, width), left, right) if prepared else (None, None)
            flux = twice_flux(left, right, 1, ready)
            for k in range(NV):
                fr[k, pl.ds(store, width), :] = flux[k]
            return carry

        two_at_a_time(1, rows - 1, one_row)

    def edge_azimuth(u, halo):
        for side in range(2):
            own = (0, 1, 2) if side == 0 else (width - 3, width - 2, width - 1)
            inside = [
                [u[k, pl.ds(8 + f, 8, stride=width), :] for k in range(NV)] for f in own
            ]
            outside = [[halo[side, k, i] for k in range(NV)] for i in range(2)]
            cells = outside + inside if side == 0 else inside + outside
            fluxes = edge_pair(cells, 3)
            faces = (0, 1) if side == 0 else (width - 1, width)
            for face, flux in zip(faces, fluxes):
                for k in range(NV):
                    fp[k, pl.ds(face, 8, stride=span), :] = flux[k]

    def edge_radial(u, halo):
        for side in range(2):
            own = (0, 1, 2) if side == 0 else (rows - 3, rows - 2, rows - 1)
            inside = [[u[k, pl.ds(8 + r * width, width), :] for k in range(NV)] for r in own]
            outside = [
                [halo[side, k, pl.ds(width * i, width), :] for k in range(NV)] for i in range(2)
            ]
            cells = outside + inside if side == 0 else inside + outside
            fluxes = edge_pair(cells, 1)
            faces = (0, 1) if side == 0 else (rows - 1, rows)
            for face, flux in zip(faces, fluxes):
                for k in range(NV):
                    fr[k, pl.ds(face * width, width), :] = flux[k]

    def advanced_row(r):
        return row_sum(r, 1.0, width, acc, fp, fr, tab, ct)

    with jax.named_scope("pre1"):
        polar_and_azimuth(u0)
    with jax.named_scope("rad1"):
        inner_radial(u0)

    with jax.named_scope("wedge_wait"):
        wedge_all().wait_recv()
    shell_row = wedge_rows[0]
    for j in range(1, wedges):
        shell_row = shell_row + wedge_rows[j]
    below_above[2] = shell_row
    pl.when(place < last)(lambda: side_copy(0).start())
    pl.when(place > 0)(lambda: side_copy(1).start())

    @pl.when(sender)
    def _():
        many(wedges, chip_send, chip_recv).wait_recv()
        chip_row = shell_row
        for j in range(wedges):
            chip_row = chip_row + chip_rows[j]
        below_above[3] = chip_row
        send_across(0, jnp.minimum(level, near))
        pl.when(near_answers > 0)(lambda: pl.semaphore_wait(from_near, near_answers))
        send_across(jnp.minimum(level, near), near)

    with jax.named_scope("h1_phi_wait"):
        first_halos[2].wait_recv()
        first_halos[3].wait_recv()
    with jax.named_scope("edge_phi1"):
        edge_azimuth(u0, hp0)
    with jax.named_scope("h1_rad_wait"):
        wait_radial(first_halos)
    with jax.named_scope("edge_rad1"):
        edge_radial(u0, hr0)

    def section_one_row(r, carry):
        values = advanced_row(r)
        for k in range(NV):
            u1[k, pl.ds(pl.multiple_of(8 + r * width, 8), width), :] = values[k]
        return carry

    with jax.named_scope("final1"):
        two_at_a_time(0, rows, section_one_row)
    for k in range(NV):
        sr[0, k] = u1[k, pl.ds(8 + (rows - 2) * width, 2 * width), :]
        sr[1, k] = u1[k, pl.ds(8, 2 * width), :]
    pack(u1, pk1)
    wait_sent(first_halos)
    second_halos = halo_copies(1, sr.at[0], sr.at[1], pk1, hr1, hp1)
    start_halos(
        second_halos, hr1,
        lambda k: sr[1, k, pl.ds(0, width), :],
        lambda k: sr[0, k, pl.ds(width, width), :],
    )

    with jax.named_scope("asc_wait"):
        pl.when(far_answers > 0)(lambda: pl.semaphore_wait(from_far, far_answers))
    pl.when(sender)(send_along)

    def gather_across():
        for x in range(1, groups):

            @pl.when(group == x)
            def _(count=x):
                many(count * levels, shared_send, shared_recv).wait_recv()
                value = [shared[n] for n in range(count)]
                for z in range(1, levels):
                    value = [value[n] + shared[z * groups + n] for n in range(count)]
                inside_rows[0] = functools.reduce(jnp.add, value)
                for passer, z_start, z_stop in passers:

                    @pl.when(jnp.logical_and(sender, level == passer))
                    def _(z_start=z_start, z_stop=z_stop):
                        for z in range(z_start, z_stop):
                            for c in both:
                                pass_copy(z, c).start()

    def gather_along():
        for z in range(1, levels):

            @pl.when(level == z)
            def _(z=z):
                many(z, along_send, along_recv).wait_recv()
                inside_rows[2] = functools.reduce(jnp.add, [along[n] for n in range(z)])

    half_of = lambda index: jnp.where(lane < index, 1.0, jnp.where(lane == index, 0.5, 0.0))
    none = jnp.zeros((8, 128), jnp.float32)
    lower = jnp.where(row < 2, jnp.where(place == 0, half_of(0), none), 0.0)
    upper = jnp.where(row < 2, none, jnp.where(place == last, half_of(rows - 1), 1.0))
    minus = jnp.where(lane >= rows, 0.0, half_of(rows - 2 + row) - 1.0)
    minus = jnp.where(jnp.logical_and(row < 2, place > 0), minus, none)
    plus = jnp.where(jnp.logical_or(row < 2, place == last), none, half_of(row - 2))
    beyond = jnp.clip(first + jnp.where(row < 2, row - 2, rows - 2 + row), 0, slabs * rows - 1)
    weights[0] = half_of(row)
    weights[1] = lower + upper
    weights[2] = minus
    weights[3] = plus
    for i, target in enumerate((first + row, beyond)):
        inverse = 1.0 / radius_of(target)
        weights[4 + i] = (timestep * strength) * inverse * inverse
    fetch_mass.wait()

    with jax.named_scope("prepare"):
        prepare(u1)
    with jax.named_scope("m1_wait"):
        pl.when(is_near)(gather_across)
        gather_along()
        pl.when(jnp.logical_and(group > 0, jnp.logical_not(is_near)))(
            lambda: pass_copy(levels - 1, 1).wait_recv()
        )
        pl.when(place > 0)(lambda: side_copy(0).wait_recv())
        pl.when(place < last)(lambda: side_copy(1).wait_recv())
    below, above, own = below_above[0], below_above[1], below_above[2]
    smaller_x = jnp.where(is_near, inside_rows[0], inside_rows[1])
    inside = jnp.where(level > 0, inside_rows[2], 0.0)
    inside = inside + jnp.where(group > 0, smaller_x, 0.0) + jnp.where(core_index == 1, below, 0.0)
    table = (
        inside + weights[0] * own,
        inside + weights[1] * own + weights[2] * below + weights[3] * above,
    )
    for i in range(2):
        enclosed = jnp.sum(table[i], axis=1, keepdims=True) + core[0]
        grav[8 * i : 8 * i + 8, :] = weights[4 + i] * enclosed
        if i == 0:
            enclosed_ref[...] = jnp.sum(
                jnp.where(lane == row, enclosed, 0.0), axis=0, keepdims=True
            )[:, :rows]

    def gravity_row(r, carry):
        base = pl.ds(pl.multiple_of(8 + r * width, 8), width)
        pull = grav[pl.ds(r, 1), :]
        u1[1, base, :] = u1[1, base, :] - pull * jnp.maximum(u0[0, base, :], MINIMUM_DENSITY)
        u1[4, base, :] = u1[4, base, :] - pull * u0[1, base, :]
        return carry

    with jax.named_scope("grav"):
        two_at_a_time(0, rows, gravity_row)

    with jax.named_scope("pre2"):
        polar_and_azimuth(u1, prepared=True)
    with jax.named_scope("rad2"):
        inner_radial(u1, prepared=True)
    with jax.named_scope("h2_phi_wait"):
        second_halos[2].wait_recv()
        second_halos[3].wait_recv()
    pull = grav[0:8, :]
    for side in range(2):
        for i in range(2):
            hp1[side, 1, i] = hp1[side, 1, i] - pull * jnp.maximum(
                hp0[side, 0, i], MINIMUM_DENSITY
            )
            hp1[side, 4, i] = hp1[side, 4, i] - pull * hp0[side, 1, i]
    with jax.named_scope("edge_phi2"):
        edge_azimuth(u1, hp1)
    with jax.named_scope("h2_rad_wait"):
        wait_radial(second_halos)
    for side in range(2):
        for i in range(2):
            which = pl.ds(width * i, width)
            pull = grav[8 + 2 * side + i : 9 + 2 * side + i, :]
            hr1[side, 1, which, :] = hr1[side, 1, which, :] - pull * jnp.maximum(
                hr0[side, 0, which, :], MINIMUM_DENSITY
            )
            hr1[side, 4, which, :] = hr1[side, 4, which, :] - pull * hr0[side, 1, which, :]
    with jax.named_scope("edge_rad2"):
        edge_radial(u1, hr1)

    with jax.named_scope("drain"):
        @pl.when(sender)
        def _():
            for x in range(groups - 1):

                @pl.when(group == x)
                def _(count=2 * near * (groups - 1 - x)):
                    many(count, shared_send, shared_recv).wait_send()

            for z in range(levels - 1):
                pl.when(level == z)(
                    lambda count=2 * (levels - 1 - z): many(
                        count, along_send, along_recv
                    ).wait_send()
                )
            for passer, z_start, z_stop in passers:
                pl.when(jnp.logical_and(group > 0, level == passer))(
                    lambda count=2 * (z_stop - z_start): many(
                        count, pass_send, pass_recv
                    ).wait_send()
                )

        pl.when(jnp.logical_not(sender))(lambda: many(wedges, chip_send, chip_recv).wait_send())
        wedge_all().wait_send()
        pl.when(place < last)(lambda: side_copy(0).wait_send())
        pl.when(place > 0)(lambda: side_copy(1).wait_send())
        wait_sent(second_halos)


def put_out(
    rows, width, acc, fp, fr, tab, ct, enclosed, advanced_hbm, enclosed_hbm, outv, sem
):
    copies = [pltpu.make_async_copy(enclosed, enclosed_hbm, sem.at[rows // 2])]
    copies[0].start()
    for pair in range(rows // 2):
        for r in (2 * pair, 2 * pair + 1):
            for k, value in enumerate(row_sum(r, 0.5, width, acc, fp, fr, tab, ct)):
                outv[k, r * width : (r + 1) * width, :] = value
        where = pl.ds(2 * pair * width, 2 * width)
        copies.append(
            pltpu.make_async_copy(
                outv.at[:, where, :], advanced_hbm.at[:, where, :], sem.at[pair]
            )
        )
        copies[-1].start()
    for copy in copies:
        copy.wait()


def body(groups, conserved, core_mass):
    _, rows, width, lanes = conserved.shape
    slabs, wedges = lax.axis_size("radial"), lax.axis_size("phi")
    inner = slabs // groups
    radial_step, theta_step, phi_step, timestep = step_sizes(rows * slabs, width * wedges, lanes)
    centers = (np.arange(lanes) + 0.5) * theta_step
    faces = (np.arange(lanes) + 1.0) * theta_step
    angles = np.zeros((8, lanes))
    angles[0] = np.sin(faces) * (0.5 / theta_step)
    angles[1] = 1.0 / np.sin(centers)
    angles[2] = np.cos(centers) / np.sin(centers)
    angles[3] = np.sin(centers)
    angles[4] = np.where(np.arange(lanes) == lanes - 1, 0.0, 0.5)
    angles[6] = angles[1] * (0.5 / phi_step)
    angles[5] = np.where(np.arange(lanes) == 0, 0.0, 0.5)
    angles = jnp.asarray(angles.astype(np.float32))
    sizes = (rows, width, slabs, wedges, groups, radial_step, theta_step, phi_step, timestep)
    f32 = jnp.float32
    vmem = lambda *shape: pltpu.VMEM(shape, f32)
    dma = lambda count: pltpu.SemaphoreType.DMA((count,))
    in_hbm = lambda value: pltpu.with_memory_space_constraint(value, pltpu.HBM)
    cells = rows * width
    *parts, enclosed = pl.pallas_call(
        functools.partial(kernel, sizes),
        out_shape=[
            jax.ShapeDtypeStruct(shape, f32)
            for shape in (
                (NV, cells, lanes),
                (NV, rows * (width + 8), lanes),
                (NV, cells + width, lanes),
                (3, 8, lanes),
                (8, lanes),
                (1, rows),
            )
        ],
        in_specs=[
            pl.BlockSpec(memory_space=pltpu.HBM),
            pl.BlockSpec(memory_space=pltpu.HBM),
            pl.BlockSpec(memory_space=pltpu.HBM),
        ],
        out_specs=[pl.BlockSpec(memory_space=pltpu.VMEM)] * 6,
        scratch_shapes=[
            vmem(NV, cells + 16, lanes), vmem(NV, cells + 16, lanes),
            vmem(2, NV, 2 * width, lanes), vmem(2, NV, 2 * width, lanes),
            vmem(2, NV, 2, 8, lanes), vmem(2, NV, 2, 8, lanes),
            vmem(2, NV, 2, 8, lanes), vmem(2, NV, 2, 8, lanes),
            vmem(2, NV, 2 * width, lanes),
            vmem(NV, cells, lanes),
            vmem(NV, cells, lanes), vmem(NV, cells, lanes), vmem(NV, cells, lanes),
            vmem(3, 2, len(STEADY) + 3, cells, lanes),
            vmem(slabs // 2, 1, lanes), vmem(inner // 2, 1, lanes), vmem(4, 1, lanes), vmem(wedges, 1, lanes),
            vmem(wedges, 1, lanes), vmem(3, 1, lanes), vmem(6, 8, lanes),
            vmem(16, lanes), pltpu.SMEM((1,), f32),
            dma(4), dma(4), dma(8), *[pltpu.SemaphoreType.DMA] * 4, dma(2), dma(2),
            pltpu.SemaphoreType.DMA, pltpu.SemaphoreType.DMA,
            pltpu.SemaphoreType.DMA, pltpu.SemaphoreType.DMA,
            pltpu.SemaphoreType.DMA, pltpu.SemaphoreType.DMA,
            pltpu.SemaphoreType.REGULAR, pltpu.SemaphoreType.REGULAR,
        ],
        compiler_params=pltpu.CompilerParams(
            collective_id=0, has_side_effects=True, vmem_limit_bytes=12 << 20
        ),
    )(in_hbm(conserved.reshape(NV, cells, lanes)), core_mass, in_hbm(angles))
    advanced, enclosed = pl.pallas_call(
        functools.partial(put_out, rows, width),
        out_shape=(
            jax.ShapeDtypeStruct((NV, cells, lanes), f32),
            jax.ShapeDtypeStruct((1, rows), f32),
        ),
        in_specs=[pl.BlockSpec(memory_space=pltpu.VMEM)] * 6,
        out_specs=[pl.BlockSpec(memory_space=pltpu.HBM)] * 2,
        scratch_shapes=[vmem(NV, cells, lanes), dma(rows // 2 + 1)],
        compiler_params=pltpu.CompilerParams(vmem_limit_bytes=8 << 20),
    )(*parts, enclosed)
    return advanced.reshape(conserved.shape), enclosed.reshape(rows)


def solution(mesh):
    in_specs = (P(None, "radial", "phi", None), P())
    out_specs = (P(None, "radial", "phi", None), P("radial"))
    return jax.shard_map(
        functools.partial(body, 4), mesh=mesh, in_specs=in_specs, out_specs=out_specs,
        check_vma=False,
    )
```

```python
import functools
import math

import jax
import jax.numpy as jnp
import numpy as np
from jax import lax
from jax.experimental import pallas as pl
from jax.experimental.pallas import tpu as pltpu
from jax.sharding import PartitionSpec as P

ADIABATIC = 4.0 / 3.0
INNER_RADIUS = 1.0
OUTER_RADIUS = 2.0
COURANT = 0.4
GRAVITY_KICK = 0.004
MINIMUM_DENSITY = 0.05
PRESSURE_FLOOR = 0.01

NV = 8
STEADY = (0, 2, 3, 5, 6, 7)
MOVED = (1, 4)
MESH = pl.DeviceIdType.MESH


def step_sizes(radial_total, phi_total, theta_total):
    theta_step = math.pi / theta_total
    phi_step = 2.0 * math.pi / phi_total
    polar_width = INNER_RADIUS * math.sin(0.5 * theta_step) * phi_step
    radial_step = min(2.0 * polar_width, (OUTER_RADIUS - INNER_RADIUS) / radial_total)
    timestep = COURANT * min(radial_step, polar_width)
    return (radial_step, theta_step, phi_step, timestep)


def half_slope(low, high):
    return jnp.maximum(jnp.minimum(low, high), jnp.minimum(jnp.maximum(low, high), 0.0))


def side_ready(state):
    density = jnp.maximum(state[0], MINIMUM_DENSITY)
    squares = state[2] * state[2] + state[3] * state[3]
    return 1.0 / density, squares, PRESSURE_FLOOR * density


def face_side(state, component, ready=None):
    if ready is None:
        ready = side_ready(state)
    inverse, squares, floor = ready
    squares = state[1] * state[1] + squares
    pressure = jnp.maximum((ADIABATIC - 1.0) * (state[4] - 0.5 * squares * inverse), floor)
    normal = state[component] * inverse
    square = ADIABATIC * pressure * inverse
    sound = square * lax.rsqrt(square)
    return pressure, normal, jnp.abs(normal) + sound


def twice_flux(left, right, component, ready=(None, None), factor=None):
    left_p, left_v, left_s = face_side(left, component, ready[0])
    right_p, right_v, right_s = face_side(right, component, ready[1])
    signal = jnp.maximum(left_s, right_s)
    left_w, right_w = left_v + signal, right_v - signal
    if factor is not None:
        left_w, right_w = left_w * factor, right_w * factor
        left_p, right_p = left_p * factor, right_p * factor
    flux = [left[k] * left_w + right[k] * right_w for k in range(NV)]
    flux[component] = flux[component] + (left_p + right_p)
    flux[4] = flux[4] + (left_p * left_v + right_p * right_v)
    return flux


def edge_pair(cells, component):
    lefts, rights = [], []
    for k in range(NV):
        halves = [0.5 * (cells[i + 1][k] - cells[i][k]) for i in range(4)]
        slopes = [half_slope(halves[i], halves[i + 1]) for i in range(3)]
        lefts.append((cells[1][k] + slopes[0], cells[2][k] + slopes[1]))
        rights.append((cells[2][k] - slopes[1], cells[3][k] - slopes[2]))
    return [
        twice_flux([a[i] for a in lefts], [b[i] for b in rights], component) for i in range(2)
    ]


def two_at_a_time(start, stop, one_row):
    def two_rows(i, carry):
        for n in range(2):
            one_row(start + 2 * i + n, carry)
        return carry

    lax.fori_loop(0, (stop - start) // 2, two_rows, 0)


def row_sum(r, part, width, acc, fp, fr, tab, ct):
    store = r * width if isinstance(r, int) else pl.multiple_of(r * width, 8)
    below = r * (width + 8) if isinstance(r, int) else pl.multiple_of(r * (width + 8), 8)
    following = store + width if isinstance(r, int) else pl.multiple_of(store + width, 8)
    low_area, high_area = part * tab[1, pl.ds(r, 1), :], part * tab[2, pl.ds(r, 1), :]
    across = part * tab[0, pl.ds(r, 1), :] * ct[6:7, :]
    return [
        acc[k, pl.ds(store, width), :]
        + across * (fp[k, pl.ds(below, width), :] - fp[k, pl.ds(below + 1, width), :])
        + low_area * fr[k, pl.ds(store, width), :]
        - high_area * fr[k, pl.ds(following, width), :]
        for k in range(NV)
    ]


def sources(cells, cotangent):
    density = jnp.maximum(cells[0], MINIMUM_DENSITY)
    inverse = 1.0 / density
    speed = [None] + [cells[m] * inverse for m in (1, 2, 3)]
    squares = cells[1] * speed[1] + cells[2] * speed[2] + cells[3] * speed[3]
    pressure = jnp.maximum(
        (ADIABATIC - 1.0) * (cells[4] - 0.5 * squares), PRESSURE_FLOOR * density
    )
    spin = cells[3] * speed[3]
    source = [None] * NV
    source[1] = 2.0 * pressure + (cells[2] * speed[2] + spin)
    source[2] = (pressure + spin) * cotangent - cells[1] * speed[2]
    source[3] = -speed[3] * (cells[1] + cells[2] * cotangent)
    return source, density


def kernel(
    sizes, state_hbm, mass_hbm, angles_hbm,
    acc, fp, fr, tab, ct, enclosed_ref,
    u0, u1, hr0, hr1, hp0, hp1, pk0, pk1, sr, sl, lt, rt, th, prep,
    shared, along, below_above, wedge_rows, chip_rows, inside_rows, weights, grav, core,
    in_sem, halo_send, halo_recv, shared_send, shared_recv, along_send, along_recv,
    side_send, side_recv, pass_send, pass_recv, wedge_send, wedge_recv, chip_send, chip_recv,
    from_near, from_far,
):
    rows, width, slabs, wedges, groups, radial_step, theta_step, phi_step, timestep = sizes
    strength = GRAVITY_KICK / timestep
    place = lax.axis_index("radial")
    wedge = lax.axis_index("phi")
    inner = slabs // groups
    levels = inner // 2
    group, member = place // inner, lax.rem(place, inner)
    level, core_index = member // 2, lax.rem(member, 2)
    span = width + 8
    last = slabs - 1

    def at(radial, phi):
        return {"radial": radial, "phi": phi}

    def signal(semaphore, radial, phi):
        pl.semaphore_signal(semaphore, inc=1, device_id=at(radial, phi), device_id_type=MESH)

    east, west = lax.rem(wedge + 1, wedges), lax.rem(wedge + wedges - 1, wedges)

    fetch_mass = pltpu.make_async_copy(mass_hbm, core, in_sem.at[3])
    fetch_density = pltpu.make_async_copy(
        state_hbm.at[pl.ds(0, 1)], u0.at[pl.ds(0, 1), pl.ds(8, rows * width), :], in_sem.at[0]
    )
    fetch = pltpu.make_async_copy(
        state_hbm.at[pl.ds(1, NV - 1)], u0.at[pl.ds(1, NV - 1), pl.ds(8, rows * width), :],
        in_sem.at[1],
    )
    fetch_angles = pltpu.make_async_copy(angles_hbm, ct, in_sem.at[2])
    for copy in (fetch_density, fetch_angles, fetch, fetch_mass):
        copy.start()

    for side in range(2):
        below_above[side] = jnp.zeros((1, 128), jnp.float32)

    barrier = pltpu.get_barrier_semaphore()
    for step in range(1, wedges):
        signal(barrier, place, lax.rem(wedge + step, wedges))
    pl.when(place < last)(lambda: signal(barrier, place + 1, wedge))
    pl.when(place > 0)(lambda: signal(barrier, place - 1, wedge))

    def greet(x_start, x_stop, z_start, z_stop, cores, semaphore):
        def one_level(back, carry):
            z = z_start + z_stop - 1 - back

            def one_group(x, inner_carry):
                for c in cores:
                    signal(semaphore, x * inner + z * 2 + c, wedge)
                return inner_carry

            return lax.fori_loop(x_start, x_stop, one_group, carry)

        lax.fori_loop(z_start, z_stop, one_level, 0)

    near = levels // 4
    is_near = level < near
    sender = core_index == 1
    both = (0, 1)

    pl.when(is_near)(lambda: greet(0, group, level + 1, levels, (1,), barrier))

    @pl.when(sender)
    def _():
        for step in range(1, wedges):
            signal(barrier, place - 1, lax.rem(wedge + step, wedges))
        greet(group, group + 1, level + 1, levels, both, barrier)
        pl.when(is_near)(lambda: greet(group + 1, groups, level, near, both, barrier))

    def answer():
        greet(group, group + 1, 0, level, (1,), from_far)
        pl.when(is_near)(lambda: greet(0, group, 0, level + 1, (1,), from_near))

    near_answers = jnp.where(
        jnp.logical_and(sender, is_near), 2 * (groups - 1 - group) * (near - level), 0
    )
    far_answers = jnp.where(sender, 2 * (levels - 1 - level), 0)
    greetings = (
        wedges - 1 + jnp.where(place > 0, 1, 0) + jnp.where(place < last, 1, 0) + level
        + jnp.where(is_near, group * (level + 1), 0)
        + jnp.where(sender, 2 * (groups - 1 - group) * jnp.minimum(level, near), wedges - 1)
    )

    row = lax.broadcasted_iota(jnp.int32, (8, 128), 0)
    lane = lax.broadcasted_iota(jnp.int32, (8, 128), 1)
    first = place * rows

    def radius_of(index):
        return INNER_RADIUS + (index.astype(jnp.float32) + 0.5) * radial_step

    radius = radius_of(first + row)
    inverse_radius = 1.0 / radius
    low_face, high_face = radius - 0.5 * radial_step, radius + 0.5 * radial_step
    area = inverse_radius * inverse_radius * (0.5 * timestep / radial_step)
    tab[0] = timestep * inverse_radius
    tab[1] = low_face * low_face * area
    tab[2] = high_face * high_face * area

    with jax.named_scope("fetch_wait"):
        fetch_angles.wait()
        fetch_density.wait()
    total = u0[0, pl.ds(8, 8, stride=width), :]
    for f in range(1, width):
        total = total + u0[0, pl.ds(8 + f, 8, stride=width), :]
    shells = jnp.sum(total * ct[3:4, :], axis=1, keepdims=True) * (
        radius * radius * (radial_step * theta_step * phi_step)
    )
    wedge_rows[0] = jnp.sum(jnp.where(lane == row, shells, 0.0), axis=0, keepdims=True)

    def pack(source, packed):
        for side, zones in enumerate(((width - 2, width - 1), (0, 1))):
            for k in range(NV):
                for i, zone in enumerate(zones):
                    packed[side, k, i] = source[k, pl.ds(8 + zone, 8, stride=width), :]

    with jax.named_scope("barrier_wait"):
        pl.semaphore_wait(barrier, greetings)

    def copy_of(source, target, send, recv, radial, phi):
        return pltpu.make_async_remote_copy(
            src_ref=source, dst_ref=target, send_sem=send, recv_sem=recv,
            device_id=at(radial, phi), device_id_type=MESH,
        )

    def send_across(z_start, z_stop):
        def one_group(x, carry):
            def one_level(z, inner_carry):
                for c in both:
                    copy_of(
                        below_above.at[3], shared.at[level * groups + group], shared_send,
                        shared_recv, x * inner + z * 2 + c, wedge,
                    ).start()
                return inner_carry

            return lax.fori_loop(z_start, z_stop, one_level, carry)

        lax.fori_loop(group + 1, groups, one_group, 0)

    def send_along():
        def one_level(z, carry):
            for c in both:
                copy_of(
                    below_above.at[3], along.at[level], along_send, along_recv,
                    group * inner + z * 2 + c, wedge,
                ).start()
            return carry

        lax.fori_loop(level + 1, levels, one_level, 0)

    def many(count, send, recv):
        rows_of = shared.at[pl.ds(0, count)]
        return copy_of(rows_of, rows_of, send, recv, place, wedge)

    passers = (
        (near - 1, near, near + (levels - near + 1) // 2),
        (0, near + (levels - near + 1) // 2, levels),
    )

    def pass_copy(z, c):
        return copy_of(
            inside_rows.at[0], inside_rows.at[1], pass_send, pass_recv,
            group * inner + z * 2 + c, wedge,
        )

    def chip_copy(step):
        return copy_of(
            wedge_rows.at[0], chip_rows.at[step], chip_send, chip_recv,
            jnp.minimum(place + 1, last), lax.rem(wedge + step, wedges),
        )

    def wedge_copy(step):
        return copy_of(
            wedge_rows.at[0], wedge_rows.at[step], wedge_send, wedge_recv, place,
            lax.rem(wedge + step, wedges),
        )

    def wedge_all():
        others = wedge_rows.at[pl.ds(1, wedges - 1)]
        return copy_of(others, others, wedge_send, wedge_recv, place, east)

    def side_copy(side):
        target = jnp.minimum(place + 1, last) if side == 0 else jnp.maximum(place - 1, 0)
        return copy_of(
            below_above.at[2], below_above.at[side], side_send.at[side], side_recv.at[side],
            target, wedge,
        )

    @pl.when(jnp.logical_not(sender))
    def _():
        for step in range(wedges):
            chip_copy(step).start()

    for step in range(1, wedges):
        wedge_copy(step).start()

    fetch.wait()
    pack(u0, pk0)

    def halo_copies(number, high_rows, low_rows, packed, radial_halo, phi_halo):
        def copy(which, source, target, peer):
            return pltpu.make_async_remote_copy(
                src_ref=source, dst_ref=target, send_sem=halo_send.at[which],
                recv_sem=halo_recv.at[4 * number + which], device_id=peer, device_id_type=MESH,
            )

        return (
            copy(0, high_rows, radial_halo.at[0], at(jnp.minimum(place + 1, last), wedge)),
            copy(1, low_rows, radial_halo.at[1], at(jnp.maximum(place - 1, 0), wedge)),
            copy(2, packed.at[0], phi_halo.at[0], at(place, east)),
            copy(3, packed.at[1], phi_halo.at[1], at(place, west)),
        )

    def start_halos(copies, radial_halo, low_row, high_row):
        pl.when(place < last)(lambda: copies[0].start())
        pl.when(place > 0)(lambda: copies[1].start())
        copies[2].start()
        copies[3].start()

        @pl.when(place == 0)
        def _():
            for k in range(NV):
                for i in range(2):
                    radial_halo[0, k, pl.ds(width * i, width), :] = low_row(k)

        @pl.when(place == last)
        def _():
            for k in range(NV):
                for i in range(2):
                    radial_halo[1, k, pl.ds(width * i, width), :] = high_row(k)

    def wait_radial(copies):
        pl.when(place > 0)(lambda: copies[0].wait_recv())
        pl.when(place < last)(lambda: copies[1].wait_recv())

    def wait_sent(copies):
        pl.when(place < last)(lambda: copies[0].wait_send())
        pl.when(place > 0)(lambda: copies[1].wait_send())
        copies[2].wait_send()
        copies[3].wait_send()

    first_halos = halo_copies(
        0, u0.at[:, pl.ds(8 + (rows - 2) * width, 2 * width), :], u0.at[:, pl.ds(8, 2 * width), :],
        pk0, hr0, hp0,
    )
    start_halos(
        first_halos, hr0,
        lambda k: u0[k, pl.ds(8, width), :],
        lambda k: u0[k, pl.ds(8 + (rows - 1) * width, width), :],
    )

    answer()

    wide_lane = lax.broadcasted_iota(jnp.int32, (width, 128), 1)

    def keep(direction, side, where, state):
        for n, k in enumerate(STEADY):
            prep[direction, side, n, where, :] = state[k]
        for n, value in enumerate(side_ready(state)):
            prep[direction, side, len(STEADY) + n, where, :] = value

    def kept(direction, where, left, right):
        ready = []
        for side, state in enumerate((left, right)):
            for n, k in enumerate(STEADY):
                state[k] = prep[direction, side, n, where, :]
            ready.append(tuple(prep[direction, side, len(STEADY) + n, where, :] for n in range(3)))
        return ready

    def prepare(u):
        def one_row(r, carry):
            base = pl.multiple_of(8 + r * width, 8)
            where = pl.ds(pl.multiple_of(r * width, 8), width)
            left, right = {}, {}
            for k in STEADY:
                cell = u[k, pl.ds(base, width), :]
                high = (pltpu.roll(cell, 127, 1) - cell) * ct[4:5, :]
                low = (cell - pltpu.roll(cell, 1, 1)) * ct[5:6, :]
                slope = half_slope(low, high)
                left[k] = cell + slope
                right[k] = jnp.where(wide_lane == 127, cell, pltpu.roll(cell - slope, 127, 1))
            keep(0, 0, where, left)
            keep(0, 1, where, right)
            for k in STEADY:
                cell = u[k, pl.ds(base, width), :]
                low = 0.5 * (cell - u[k, pl.ds(base - 1, width), :])
                high = 0.5 * (u[k, pl.ds(base + 1, width), :] - cell)
                slope = half_slope(low, high)
                left[k] = pltpu.roll(cell + slope, 1, 0)
                right[k] = cell - slope
            keep(1, 0, where, left)
            keep(1, 1, where, right)
            return carry

        lax.fori_loop(0, rows, one_row, 0)

        def one_inner_row(r, carry):
            base = pl.multiple_of(8 + r * width, 8)
            where = pl.multiple_of(r * width, 8)
            left, right = {}, {}
            for k in STEADY:
                cell = u[k, pl.ds(base, width), :]
                low = 0.5 * (cell - u[k, pl.ds(base - width, width), :])
                high = 0.5 * (u[k, pl.ds(base + width, width), :] - cell)
                slope = half_slope(low, high)
                left[k], right[k] = cell + slope, cell - slope
            keep(2, 0, pl.ds(pl.multiple_of(where + width, 8), width), left)
            keep(2, 1, pl.ds(where, width), right)
            return carry

        lax.fori_loop(1, rows - 1, one_inner_row, 0)

    def inner_radial_row(u, prepared=False):
        moving = MOVED if prepared else range(NV)

        def one_row(r, carry=0):
            base = pl.multiple_of(8 + r * width, 8)
            store = pl.multiple_of(r * width, 8)
            left, right = {}, {}
            for k in moving:
                cell = u[k, pl.ds(base, width), :]
                low = 0.5 * (cell - u[k, pl.ds(base - width, width), :])
                high = 0.5 * (u[k, pl.ds(base + width, width), :] - cell)
                slope = half_slope(low, high)
                right[k] = cell - slope
                left[k] = sl[k, pl.ds(store - width, width), :]
                sl[k, pl.ds(store, width), :] = cell + slope
            ready = kept(2, pl.ds(store, width), left, right) if prepared else (None, None)
            flux = twice_flux(left, right, 1, ready)
            for k in range(NV):
                fr[k, pl.ds(store, width), :] = flux[k]
            return carry

        return one_row

    def inner_radial(u):
        two_at_a_time(1, rows - 1, inner_radial_row(u))

    def polar_and_azimuth(u, prepared=False):
        moving = MOVED if prepared else range(NV)
        radial_row = inner_radial_row(u, prepared)

        together = 2 if prepared else 1
        sine, inverse_sine, cotangent, mask = ct[0:1, :], ct[1:2, :], ct[2:3, :], ct[4:5, :]

        def third(i, n):
            r = jnp.maximum((i - 2) * together, 0) + n
            store = pl.ds(pl.multiple_of(r * width, 8), width)
            scale = tab[0, pl.ds(r, 1), :]
            cells = [u[k, pl.ds(pl.multiple_of(8 + r * width, 8), width), :] for k in range(NV)]
            source, density = sources(cells, cotangent)
            pull = grav[pl.ds(r, 1), :]
            across = scale * inverse_sine
            for k in range(NV):
                through = th[k, store, :]
                value = cells[k] + across * (pltpu.roll(through, 1, 1) - through)
                if source[k] is not None:
                    value = value + scale * source[k]
                if prepared:
                    if k == 1:
                        value = value - pull * density
                    elif k == 4:
                        value = value - pull * cells[1]
                    before = u0[k, pl.ds(pl.multiple_of(8 + r * width, 8), width), :]
                    value = 0.5 * (before + value)
                acc[k, store, :] = value

        def second(i, n):
            r = jnp.clip((i - 1) * together, 0, rows - together) + n
            store = pl.ds(pl.multiple_of(r * width, 8), width)
            left = {k: lt[k, store, :] for k in moving}
            right = {}
            for k in moving:
                value = rt[k, store, :]
                cell = u[k, pl.ds(pl.multiple_of(8 + r * width, 8), width), :]
                right[k] = jnp.where(wide_lane == 127, cell, pltpu.roll(value, 127, 1))
            ready = kept(0, store, left, right) if prepared else (None, None)
            flux = twice_flux(left, right, 2, ready, sine)
            for k in range(NV):
                th[k, store, :] = flux[k]

        def first(i, n):
            r = jnp.minimum(i * together, rows - together) + n
            base = pl.multiple_of(8 + r * width, 8)
            store = pl.ds(pl.multiple_of(r * width, 8), width)
            cells = {k: u[k, pl.ds(base, width), :] for k in moving}
            for k in moving:
                high = (pltpu.roll(cells[k], 127, 1) - cells[k]) * mask
                low = (cells[k] - pltpu.roll(cells[k], 1, 1)) * ct[5:6, :]
                slope = half_slope(low, high)
                lt[k, store, :] = cells[k] + slope
                rt[k, store, :] = cells[k] - slope
            left, right = {}, {}
            for k in moving:
                low = 0.5 * (cells[k] - u[k, pl.ds(base - 1, width), :])
                high = 0.5 * (u[k, pl.ds(base + 1, width), :] - cells[k])
                slope = half_slope(low, high)
                left[k] = pltpu.roll(cells[k] + slope, 1, 0)
                right[k] = cells[k] - slope
            ready = kept(1, store, left, right) if prepared else (None, None)
            flux = twice_flux(left, right, 3, ready)
            for k in range(NV):
                fp[k, pl.ds(pl.multiple_of(r * span, 8), width), :] = flux[k]

        def run(i, stages):
            for stage in stages:
                for n in range(together):
                    stage(i, n)

        def one_step(i, carry):
            run(i, (third, second, first))
            return carry

        steps = rows // together
        if prepared:
            third_part = (rows - 2) // 3
            run(0, (first,))
            for r in range(1, 1 + third_part):
                radial_row(jnp.int32(r))
            run(1, (second, first))
            lax.fori_loop(2, steps, one_step, 0)
            run(steps, (third, second))
            for r in range(1 + third_part, 1 + 2 * third_part):
                radial_row(jnp.int32(r))
            run(steps + 1, (third,))
            for r in range(1 + 2 * third_part, rows - 1):
                radial_row(jnp.int32(r))
        else:
            lax.fori_loop(0, steps + 2, one_step, 0)

    def edge_azimuth(u, halo):
        for side in range(2):
            own = (0, 1, 2) if side == 0 else (width - 3, width - 2, width - 1)
            inside = [
                [u[k, pl.ds(8 + f, 8, stride=width), :] for k in range(NV)] for f in own
            ]
            outside = [[halo[side, k, i] for k in range(NV)] for i in range(2)]
            cells = outside + inside if side == 0 else inside + outside
            fluxes = edge_pair(cells, 3)
            faces = (0, 1) if side == 0 else (width - 1, width)
            for face, flux in zip(faces, fluxes):
                for k in range(NV):
                    fp[k, pl.ds(face, 8, stride=span), :] = flux[k]

    def edge_radial(u, halo):
        for side in range(2):
            own = (0, 1, 2) if side == 0 else (rows - 3, rows - 2, rows - 1)
            inside = [[u[k, pl.ds(8 + r * width, width), :] for k in range(NV)] for r in own]
            outside = [
                [halo[side, k, pl.ds(width * i, width), :] for k in range(NV)] for i in range(2)
            ]
            cells = outside + inside if side == 0 else inside + outside
            fluxes = edge_pair(cells, 1)
            faces = (0, 1) if side == 0 else (rows - 1, rows)
            for face, flux in zip(faces, fluxes):
                for k in range(NV):
                    fr[k, pl.ds(face * width, width), :] = flux[k]

    def advanced_row(r):
        return row_sum(r, 1.0, width, acc, fp, fr, tab, ct)

    with jax.named_scope("pre1"):
        polar_and_azimuth(u0)
    with jax.named_scope("rad1"):
        inner_radial(u0)

    with jax.named_scope("wedge_wait"):
        wedge_all().wait_recv()
    shell_row = wedge_rows[0]
    for j in range(1, wedges):
        shell_row = shell_row + wedge_rows[j]
    below_above[2] = shell_row
    pl.when(place < last)(lambda: side_copy(0).start())
    pl.when(place > 0)(lambda: side_copy(1).start())

    @pl.when(sender)
    def _():
        many(wedges, chip_send, chip_recv).wait_recv()
        chip_row = shell_row
        for j in range(wedges):
            chip_row = chip_row + chip_rows[j]
        below_above[3] = chip_row
        send_across(0, jnp.minimum(level, near))
        pl.when(near_answers > 0)(lambda: pl.semaphore_wait(from_near, near_answers))
        send_across(jnp.minimum(level, near), near)

    with jax.named_scope("h1_phi_wait"):
        first_halos[2].wait_recv()
        first_halos[3].wait_recv()
    with jax.named_scope("edge_phi1"):
        edge_azimuth(u0, hp0)
    with jax.named_scope("h1_rad_wait"):
        wait_radial(first_halos)
    with jax.named_scope("edge_rad1"):
        edge_radial(u0, hr0)

    def section_one_row(r, carry):
        values = advanced_row(r)
        for k in range(NV):
            u1[k, pl.ds(pl.multiple_of(8 + r * width, 8), width), :] = values[k]
        return carry

    with jax.named_scope("final1"):
        two_at_a_time(0, rows, section_one_row)
    for k in range(NV):
        sr[0, k] = u1[k, pl.ds(8 + (rows - 2) * width, 2 * width), :]
        sr[1, k] = u1[k, pl.ds(8, 2 * width), :]
    pack(u1, pk1)
    wait_sent(first_halos)
    second_halos = halo_copies(1, sr.at[0], sr.at[1], pk1, hr1, hp1)
    start_halos(
        second_halos, hr1,
        lambda k: sr[1, k, pl.ds(0, width), :],
        lambda k: sr[0, k, pl.ds(width, width), :],
    )

    with jax.named_scope("asc_wait"):
        pl.when(far_answers > 0)(lambda: pl.semaphore_wait(from_far, far_answers))
    pl.when(sender)(send_along)

    def gather_across():
        for x in range(1, groups):

            @pl.when(group == x)
            def _(count=x):
                many(count * levels, shared_send, shared_recv).wait_recv()
                value = [shared[n] for n in range(count)]
                for z in range(1, levels):
                    value = [value[n] + shared[z * groups + n] for n in range(count)]
                inside_rows[0] = functools.reduce(jnp.add, value)
                for passer, z_start, z_stop in passers:

                    @pl.when(jnp.logical_and(sender, level == passer))
                    def _(z_start=z_start, z_stop=z_stop):
                        for z in range(z_start, z_stop):
                            for c in both:
                                pass_copy(z, c).start()

    def gather_along():
        for z in range(1, levels):

            @pl.when(level == z)
            def _(z=z):
                many(z, along_send, along_recv).wait_recv()
                inside_rows[2] = functools.reduce(jnp.add, [along[n] for n in range(z)])

    half_of = lambda index: jnp.where(lane < index, 1.0, jnp.where(lane == index, 0.5, 0.0))
    none = jnp.zeros((8, 128), jnp.float32)
    lower = jnp.where(row < 2, jnp.where(place == 0, half_of(0), none), 0.0)
    upper = jnp.where(row < 2, none, jnp.where(place == last, half_of(rows - 1), 1.0))
    minus = jnp.where(lane >= rows, 0.0, half_of(rows - 2 + row) - 1.0)
    minus = jnp.where(jnp.logical_and(row < 2, place > 0), minus, none)
    plus = jnp.where(jnp.logical_or(row < 2, place == last), none, half_of(row - 2))
    beyond = jnp.clip(first + jnp.where(row < 2, row - 2, rows - 2 + row), 0, slabs * rows - 1)
    weights[0] = half_of(row)
    weights[1] = lower + upper
    weights[2] = minus
    weights[3] = plus
    for i, target in enumerate((first + row, beyond)):
        inverse = 1.0 / radius_of(target)
        weights[4 + i] = (timestep * strength) * inverse * inverse
    fetch_mass.wait()

    with jax.named_scope("prepare"):
        prepare(u1)
    with jax.named_scope("m1_wait"):
        pl.when(is_near)(gather_across)
        gather_along()
        pl.when(jnp.logical_and(group > 0, jnp.logical_not(is_near)))(
            lambda: pass_copy(levels - 1, 1).wait_recv()
        )
        pl.when(place > 0)(lambda: side_copy(0).wait_recv())
        pl.when(place < last)(lambda: side_copy(1).wait_recv())
    below, above, own = below_above[0], below_above[1], below_above[2]
    smaller_x = jnp.where(is_near, inside_rows[0], inside_rows[1])
    inside = jnp.where(level > 0, inside_rows[2], 0.0)
    inside = inside + jnp.where(group > 0, smaller_x, 0.0) + jnp.where(core_index == 1, below, 0.0)
    table = (
        inside + weights[0] * own,
        inside + weights[1] * own + weights[2] * below + weights[3] * above,
    )
    for i in range(2):
        enclosed = jnp.sum(table[i], axis=1, keepdims=True) + core[0]
        grav[8 * i : 8 * i + 8, :] = weights[4 + i] * enclosed
        if i == 0:
            enclosed_ref[...] = jnp.sum(
                jnp.where(lane == row, enclosed, 0.0), axis=0, keepdims=True
            )[:, :rows]

    def gravity_row(r, carry):
        base = pl.ds(pl.multiple_of(8 + r * width, 8), width)
        pull = grav[pl.ds(r, 1), :]
        u1[1, base, :] = u1[1, base, :] - pull * jnp.maximum(u0[0, base, :], MINIMUM_DENSITY)
        u1[4, base, :] = u1[4, base, :] - pull * u0[1, base, :]
        return carry

    with jax.named_scope("grav"):
        two_at_a_time(0, rows, gravity_row)

    with jax.named_scope("pre2"):
        polar_and_azimuth(u1, prepared=True)
    with jax.named_scope("h2_phi_wait"):
        second_halos[2].wait_recv()
        second_halos[3].wait_recv()
    pull = grav[0:8, :]
    for side in range(2):
        for i in range(2):
            hp1[side, 1, i] = hp1[side, 1, i] - pull * jnp.maximum(
                hp0[side, 0, i], MINIMUM_DENSITY
            )
            hp1[side, 4, i] = hp1[side, 4, i] - pull * hp0[side, 1, i]
    with jax.named_scope("edge_phi2"):
        edge_azimuth(u1, hp1)
    with jax.named_scope("h2_rad_wait"):
        wait_radial(second_halos)
    for side in range(2):
        for i in range(2):
            which = pl.ds(width * i, width)
            pull = grav[8 + 2 * side + i : 9 + 2 * side + i, :]
            hr1[side, 1, which, :] = hr1[side, 1, which, :] - pull * jnp.maximum(
                hr0[side, 0, which, :], MINIMUM_DENSITY
            )
            hr1[side, 4, which, :] = hr1[side, 4, which, :] - pull * hr0[side, 1, which, :]
    with jax.named_scope("edge_rad2"):
        edge_radial(u1, hr1)

    with jax.named_scope("drain"):
        @pl.when(sender)
        def _():
            for x in range(groups - 1):

                @pl.when(group == x)
                def _(count=2 * near * (groups - 1 - x)):
                    many(count, shared_send, shared_recv).wait_send()

            for z in range(levels - 1):
                pl.when(level == z)(
                    lambda count=2 * (levels - 1 - z): many(
                        count, along_send, along_recv
                    ).wait_send()
                )
            for passer, z_start, z_stop in passers:
                pl.when(jnp.logical_and(group > 0, level == passer))(
                    lambda count=2 * (z_stop - z_start): many(
                        count, pass_send, pass_recv
                    ).wait_send()
                )

        pl.when(jnp.logical_not(sender))(lambda: many(wedges, chip_send, chip_recv).wait_send())
        wedge_all().wait_send()
        pl.when(place < last)(lambda: side_copy(0).wait_send())
        pl.when(place > 0)(lambda: side_copy(1).wait_send())
        wait_sent(second_halos)


def put_out(
    rows, width, acc, fp, fr, tab, ct, enclosed, advanced_hbm, enclosed_hbm, outv, sem
):
    copies = [pltpu.make_async_copy(enclosed, enclosed_hbm, sem.at[rows // 2])]
    copies[0].start()
    for pair in range(rows // 2):
        for r in (2 * pair, 2 * pair + 1):
            for k, value in enumerate(row_sum(r, 0.5, width, acc, fp, fr, tab, ct)):
                outv[k, r * width : (r + 1) * width, :] = value
        where = pl.ds(2 * pair * width, 2 * width)
        copies.append(
            pltpu.make_async_copy(
                outv.at[:, where, :], advanced_hbm.at[:, where, :], sem.at[pair]
            )
        )
        copies[-1].start()
    for copy in copies:
        copy.wait()


def body(groups, conserved, core_mass):
    _, rows, width, lanes = conserved.shape
    slabs, wedges = lax.axis_size("radial"), lax.axis_size("phi")
    inner = slabs // groups
    radial_step, theta_step, phi_step, timestep = step_sizes(rows * slabs, width * wedges, lanes)
    centers = (np.arange(lanes) + 0.5) * theta_step
    faces = (np.arange(lanes) + 1.0) * theta_step
    angles = np.zeros((8, lanes))
    angles[0] = np.sin(faces) * (0.5 / theta_step)
    angles[1] = 1.0 / np.sin(centers)
    angles[2] = np.cos(centers) / np.sin(centers)
    angles[3] = np.sin(centers)
    angles[4] = np.where(np.arange(lanes) == lanes - 1, 0.0, 0.5)
    angles[6] = angles[1] * (0.5 / phi_step)
    angles[5] = np.where(np.arange(lanes) == 0, 0.0, 0.5)
    angles = jnp.asarray(angles.astype(np.float32))
    sizes = (rows, width, slabs, wedges, groups, radial_step, theta_step, phi_step, timestep)
    f32 = jnp.float32
    vmem = lambda *shape: pltpu.VMEM(shape, f32)
    dma = lambda count: pltpu.SemaphoreType.DMA((count,))
    in_hbm = lambda value: pltpu.with_memory_space_constraint(value, pltpu.HBM)
    cells = rows * width
    *parts, enclosed = pl.pallas_call(
        functools.partial(kernel, sizes),
        out_shape=[
            jax.ShapeDtypeStruct(shape, f32)
            for shape in (
                (NV, cells, lanes),
                (NV, rows * (width + 8), lanes),
                (NV, cells + width, lanes),
                (3, 8, lanes),
                (8, lanes),
                (1, rows),
            )
        ],
        in_specs=[
            pl.BlockSpec(memory_space=pltpu.HBM),
            pl.BlockSpec(memory_space=pltpu.HBM),
            pl.BlockSpec(memory_space=pltpu.HBM),
        ],
        out_specs=[pl.BlockSpec(memory_space=pltpu.VMEM)] * 6,
        scratch_shapes=[
            vmem(NV, cells + 16, lanes), vmem(NV, cells + 16, lanes),
            vmem(2, NV, 2 * width, lanes), vmem(2, NV, 2 * width, lanes),
            vmem(2, NV, 2, 8, lanes), vmem(2, NV, 2, 8, lanes),
            vmem(2, NV, 2, 8, lanes), vmem(2, NV, 2, 8, lanes),
            vmem(2, NV, 2 * width, lanes),
            vmem(NV, cells, lanes),
            vmem(NV, cells, lanes), vmem(NV, cells, lanes), vmem(NV, cells, lanes),
            vmem(3, 2, len(STEADY) + 3, cells, lanes),
            vmem(slabs // 2, 1, lanes), vmem(inner // 2, 1, lanes), vmem(4, 1, lanes), vmem(wedges, 1, lanes),
            vmem(wedges, 1, lanes), vmem(3, 1, lanes), vmem(6, 8, lanes),
            vmem(16, lanes), pltpu.SMEM((1,), f32),
            dma(4), dma(4), dma(8), *[pltpu.SemaphoreType.DMA] * 4, dma(2), dma(2),
            pltpu.SemaphoreType.DMA, pltpu.SemaphoreType.DMA,
            pltpu.SemaphoreType.DMA, pltpu.SemaphoreType.DMA,
            pltpu.SemaphoreType.DMA, pltpu.SemaphoreType.DMA,
            pltpu.SemaphoreType.REGULAR, pltpu.SemaphoreType.REGULAR,
        ],
        compiler_params=pltpu.CompilerParams(
            collective_id=0, has_side_effects=True, vmem_limit_bytes=12 << 20
        ),
    )(in_hbm(conserved.reshape(NV, cells, lanes)), core_mass, in_hbm(angles))
    advanced, enclosed = pl.pallas_call(
        functools.partial(put_out, rows, width),
        out_shape=(
            jax.ShapeDtypeStruct((NV, cells, lanes), f32),
            jax.ShapeDtypeStruct((1, rows), f32),
        ),
        in_specs=[pl.BlockSpec(memory_space=pltpu.VMEM)] * 6,
        out_specs=[pl.BlockSpec(memory_space=pltpu.HBM)] * 2,
        scratch_shapes=[vmem(NV, cells, lanes), dma(rows // 2 + 1)],
        compiler_params=pltpu.CompilerParams(vmem_limit_bytes=8 << 20),
    )(*parts, enclosed)
    return advanced.reshape(conserved.shape), enclosed.reshape(rows)


def solution(mesh):
    in_specs = (P(None, "radial", "phi", None), P())
    out_specs = (P(None, "radial", "phi", None), P("radial"))
    return jax.shard_map(
        functools.partial(body, 4), mesh=mesh, in_specs=in_specs, out_specs=out_specs,
        check_vma=False,
    )
```

```python
import functools
import math

import jax
import jax.numpy as jnp
import numpy as np
from jax import lax
from jax.experimental import pallas as pl
from jax.experimental.pallas import tpu as pltpu
from jax.sharding import PartitionSpec as P

ADIABATIC = 4.0 / 3.0
INNER_RADIUS = 1.0
OUTER_RADIUS = 2.0
COURANT = 0.4
GRAVITY_KICK = 0.004
MINIMUM_DENSITY = 0.05
PRESSURE_FLOOR = 0.01

NV = 8
STEADY = (0, 2, 3, 5, 6, 7)
MOVED = (1, 4)
MESH = pl.DeviceIdType.MESH


def step_sizes(radial_total, phi_total, theta_total):
    theta_step = math.pi / theta_total
    phi_step = 2.0 * math.pi / phi_total
    polar_width = INNER_RADIUS * math.sin(0.5 * theta_step) * phi_step
    radial_step = min(2.0 * polar_width, (OUTER_RADIUS - INNER_RADIUS) / radial_total)
    timestep = COURANT * min(radial_step, polar_width)
    return (radial_step, theta_step, phi_step, timestep)


def half_slope(low, high):
    return jnp.maximum(jnp.minimum(low, high), jnp.minimum(jnp.maximum(low, high), 0.0))


def side_ready(state):
    density = jnp.maximum(state[0], MINIMUM_DENSITY)
    squares = state[2] * state[2] + state[3] * state[3]
    return 1.0 / density, squares, PRESSURE_FLOOR * density


def face_side(state, component, ready=None):
    if ready is None:
        ready = side_ready(state)
    inverse, squares, floor = ready
    squares = state[1] * state[1] + squares
    pressure = jnp.maximum((ADIABATIC - 1.0) * (state[4] - 0.5 * squares * inverse), floor)
    normal = state[component] * inverse
    square = ADIABATIC * pressure * inverse
    sound = square * lax.rsqrt(square)
    return pressure, normal, jnp.abs(normal) + sound


def twice_flux(left, right, component, ready=(None, None), factor=None):
    left_p, left_v, left_s = face_side(left, component, ready[0])
    right_p, right_v, right_s = face_side(right, component, ready[1])
    signal = jnp.maximum(left_s, right_s)
    left_w, right_w = left_v + signal, right_v - signal
    if factor is not None:
        left_w, right_w = left_w * factor, right_w * factor
        left_p, right_p = left_p * factor, right_p * factor
    flux = [left[k] * left_w + right[k] * right_w for k in range(NV)]
    flux[component] = flux[component] + (left_p + right_p)
    flux[4] = flux[4] + (left_p * left_v + right_p * right_v)
    return flux


def edge_pair(cells, component):
    lefts, rights = [], []
    for k in range(NV):
        halves = [0.5 * (cells[i + 1][k] - cells[i][k]) for i in range(4)]
        slopes = [half_slope(halves[i], halves[i + 1]) for i in range(3)]
        lefts.append((cells[1][k] + slopes[0], cells[2][k] + slopes[1]))
        rights.append((cells[2][k] - slopes[1], cells[3][k] - slopes[2]))
    return [
        twice_flux([a[i] for a in lefts], [b[i] for b in rights], component) for i in range(2)
    ]


def two_at_a_time(start, stop, one_row):
    def two_rows(i, carry):
        for n in range(2):
            one_row(start + 2 * i + n, carry)
        return carry

    lax.fori_loop(0, (stop - start) // 2, two_rows, 0)


def row_sum(r, part, width, acc, fp, fr, tab, ct):
    store = r * width if isinstance(r, int) else pl.multiple_of(r * width, 8)
    below = r * (width + 8) if isinstance(r, int) else pl.multiple_of(r * (width + 8), 8)
    following = store + width if isinstance(r, int) else pl.multiple_of(store + width, 8)
    low_area, high_area = part * tab[1, pl.ds(r, 1), :], part * tab[2, pl.ds(r, 1), :]
    across = part * tab[0, pl.ds(r, 1), :] * ct[6:7, :]
    return [
        acc[k, pl.ds(store, width), :]
        + across * (fp[k, pl.ds(below, width), :] - fp[k, pl.ds(below + 1, width), :])
        + low_area * fr[k, pl.ds(store, width), :]
        - high_area * fr[k, pl.ds(following, width), :]
        for k in range(NV)
    ]


def sources(cells, cotangent):
    density = jnp.maximum(cells[0], MINIMUM_DENSITY)
    inverse = 1.0 / density
    speed = [None] + [cells[m] * inverse for m in (1, 2, 3)]
    squares = cells[1] * speed[1] + cells[2] * speed[2] + cells[3] * speed[3]
    pressure = jnp.maximum(
        (ADIABATIC - 1.0) * (cells[4] - 0.5 * squares), PRESSURE_FLOOR * density
    )
    spin = cells[3] * speed[3]
    source = [None] * NV
    source[1] = 2.0 * pressure + (cells[2] * speed[2] + spin)
    source[2] = (pressure + spin) * cotangent - cells[1] * speed[2]
    source[3] = -speed[3] * (cells[1] + cells[2] * cotangent)
    return source, density


def kernel(
    sizes, state_hbm, mass_hbm, angles_hbm,
    acc, fp, fr, tab, ct, enclosed_ref,
    u0, u1, hr0, hr1, hp0, hp1, pk0, pk1, sr, sl, lt, rt, th, prep,
    shared, along, below_above, wedge_rows, chip_rows, inside_rows, weights, grav, core,
    in_sem, halo_send, halo_recv, shared_send, shared_recv, along_send, along_recv,
    side_send, side_recv, pass_send, pass_recv, wedge_send, wedge_recv, chip_send, chip_recv,
    from_near, from_far,
):
    rows, width, slabs, wedges, groups, radial_step, theta_step, phi_step, timestep = sizes
    strength = GRAVITY_KICK / timestep
    place = lax.axis_index("radial")
    wedge = lax.axis_index("phi")
    inner = slabs // groups
    levels = inner // 2
    group, member = place // inner, lax.rem(place, inner)
    level, core_index = member // 2, lax.rem(member, 2)
    span = width + 8
    last = slabs - 1

    def at(radial, phi):
        return {"radial": radial, "phi": phi}

    def signal(semaphore, radial, phi):
        pl.semaphore_signal(semaphore, inc=1, device_id=at(radial, phi), device_id_type=MESH)

    east, west = lax.rem(wedge + 1, wedges), lax.rem(wedge + wedges - 1, wedges)

    fetch_mass = pltpu.make_async_copy(mass_hbm, core, in_sem.at[3])
    fetch_density = pltpu.make_async_copy(
        state_hbm.at[pl.ds(0, 1)], u0.at[pl.ds(0, 1), pl.ds(8, rows * width), :], in_sem.at[0]
    )
    fetch = pltpu.make_async_copy(
        state_hbm.at[pl.ds(1, NV - 1)], u0.at[pl.ds(1, NV - 1), pl.ds(8, rows * width), :],
        in_sem.at[1],
    )
    fetch_angles = pltpu.make_async_copy(angles_hbm, ct, in_sem.at[2])
    for copy in (fetch_density, fetch_angles, fetch, fetch_mass):
        copy.start()

    for side in range(2):
        below_above[side] = jnp.zeros((1, 128), jnp.float32)

    barrier = pltpu.get_barrier_semaphore()
    for step in range(1, wedges):
        signal(barrier, place, lax.rem(wedge + step, wedges))
    pl.when(place < last)(lambda: signal(barrier, place + 1, wedge))
    pl.when(place > 0)(lambda: signal(barrier, place - 1, wedge))

    def greet(x_start, x_stop, z_start, z_stop, cores, semaphore):
        def one_level(back, carry):
            z = z_start + z_stop - 1 - back

            def one_group(x, inner_carry):
                for c in cores:
                    signal(semaphore, x * inner + z * 2 + c, wedge)
                return inner_carry

            return lax.fori_loop(x_start, x_stop, one_group, carry)

        lax.fori_loop(z_start, z_stop, one_level, 0)

    near = levels // 4
    is_near = level < near
    sender = core_index == 1
    both = (0, 1)

    pl.when(is_near)(lambda: greet(0, group, level + 1, levels, (1,), barrier))

    @pl.when(sender)
    def _():
        for step in range(1, wedges):
            signal(barrier, place - 1, lax.rem(wedge + step, wedges))
        greet(group, group + 1, level + 1, levels, both, barrier)
        pl.when(is_near)(lambda: greet(group + 1, groups, level, near, both, barrier))

    def answer():
        greet(group, group + 1, 0, level, (1,), from_far)
        pl.when(is_near)(lambda: greet(0, group, 0, level + 1, (1,), from_near))

    near_answers = jnp.where(
        jnp.logical_and(sender, is_near), 2 * (groups - 1 - group) * (near - level), 0
    )
    far_answers = jnp.where(sender, 2 * (levels - 1 - level), 0)
    greetings = (
        wedges - 1 + jnp.where(place > 0, 1, 0) + jnp.where(place < last, 1, 0) + level
        + jnp.where(is_near, group * (level + 1), 0)
        + jnp.where(sender, 2 * (groups - 1 - group) * jnp.minimum(level, near), wedges - 1)
    )

    row = lax.broadcasted_iota(jnp.int32, (8, 128), 0)
    lane = lax.broadcasted_iota(jnp.int32, (8, 128), 1)
    first = place * rows

    def radius_of(index):
        return INNER_RADIUS + (index.astype(jnp.float32) + 0.5) * radial_step

    radius = radius_of(first + row)
    inverse_radius = 1.0 / radius
    low_face, high_face = radius - 0.5 * radial_step, radius + 0.5 * radial_step
    area = inverse_radius * inverse_radius * (0.5 * timestep / radial_step)
    tab[0] = timestep * inverse_radius
    tab[1] = low_face * low_face * area
    tab[2] = high_face * high_face * area

    with jax.named_scope("fetch_wait"):
        fetch_angles.wait()
        fetch_density.wait()
    total = u0[0, pl.ds(8, 8, stride=width), :]
    for f in range(1, width):
        total = total + u0[0, pl.ds(8 + f, 8, stride=width), :]
    shells = jnp.sum(total * ct[3:4, :], axis=1, keepdims=True) * (
        radius * radius * (radial_step * theta_step * phi_step)
    )
    wedge_rows[0] = jnp.sum(jnp.where(lane == row, shells, 0.0), axis=0, keepdims=True)

    def pack(source, packed):
        for side, zones in enumerate(((width - 2, width - 1), (0, 1))):
            for k in range(NV):
                for i, zone in enumerate(zones):
                    packed[side, k, i] = source[k, pl.ds(8 + zone, 8, stride=width), :]

    with jax.named_scope("barrier_wait"):
        pl.semaphore_wait(barrier, greetings)

    def copy_of(source, target, send, recv, radial, phi):
        return pltpu.make_async_remote_copy(
            src_ref=source, dst_ref=target, send_sem=send, recv_sem=recv,
            device_id=at(radial, phi), device_id_type=MESH,
        )

    def send_across(z_start, z_stop):
        def one_group(x, carry):
            def one_level(z, inner_carry):
                for c in both:
                    copy_of(
                        below_above.at[3], shared.at[level * groups + group], shared_send,
                        shared_recv, x * inner + z * 2 + c, wedge,
                    ).start()
                return inner_carry

            return lax.fori_loop(z_start, z_stop, one_level, carry)

        lax.fori_loop(group + 1, groups, one_group, 0)

    def send_along():
        def one_level(z, carry):
            for c in both:
                copy_of(
                    below_above.at[3], along.at[level], along_send, along_recv,
                    group * inner + z * 2 + c, wedge,
                ).start()
            return carry

        lax.fori_loop(level + 1, levels, one_level, 0)

    def many(count, send, recv):
        rows_of = shared.at[pl.ds(0, count)]
        return copy_of(rows_of, rows_of, send, recv, place, wedge)

    passers = (
        (near - 1, near, near + (levels - near + 1) // 2),
        (0, near + (levels - near + 1) // 2, levels),
    )

    def pass_copy(z, c):
        return copy_of(
            inside_rows.at[0], inside_rows.at[1], pass_send, pass_recv,
            group * inner + z * 2 + c, wedge,
        )

    def chip_copy(step):
        return copy_of(
            wedge_rows.at[0], chip_rows.at[step], chip_send, chip_recv,
            jnp.minimum(place + 1, last), lax.rem(wedge + step, wedges),
        )

    def wedge_copy(step):
        return copy_of(
            wedge_rows.at[0], wedge_rows.at[step], wedge_send, wedge_recv, place,
            lax.rem(wedge + step, wedges),
        )

    def wedge_all():
        others = wedge_rows.at[pl.ds(1, wedges - 1)]
        return copy_of(others, others, wedge_send, wedge_recv, place, east)

    def side_copy(side):
        target = jnp.minimum(place + 1, last) if side == 0 else jnp.maximum(place - 1, 0)
        return copy_of(
            below_above.at[2], below_above.at[side], side_send.at[side], side_recv.at[side],
            target, wedge,
        )

    @pl.when(jnp.logical_not(sender))
    def _():
        for step in range(wedges):
            chip_copy(step).start()

    for step in range(1, wedges):
        wedge_copy(step).start()

    fetch.wait()
    pack(u0, pk0)

    def halo_copies(number, high_rows, low_rows, packed, radial_halo, phi_halo):
        def copy(which, source, target, peer):
            return pltpu.make_async_remote_copy(
                src_ref=source, dst_ref=target, send_sem=halo_send.at[which],
                recv_sem=halo_recv.at[4 * number + which], device_id=peer, device_id_type=MESH,
            )

        return (
            copy(0, high_rows, radial_halo.at[0], at(jnp.minimum(place + 1, last), wedge)),
            copy(1, low_rows, radial_halo.at[1], at(jnp.maximum(place - 1, 0), wedge)),
            copy(2, packed.at[0], phi_halo.at[0], at(place, east)),
            copy(3, packed.at[1], phi_halo.at[1], at(place, west)),
        )

    def start_halos(copies, radial_halo, low_row, high_row):
        pl.when(place < last)(lambda: copies[0].start())
        pl.when(place > 0)(lambda: copies[1].start())
        copies[2].start()
        copies[3].start()

        @pl.when(place == 0)
        def _():
            for k in range(NV):
                for i in range(2):
                    radial_halo[0, k, pl.ds(width * i, width), :] = low_row(k)

        @pl.when(place == last)
        def _():
            for k in range(NV):
                for i in range(2):
                    radial_halo[1, k, pl.ds(width * i, width), :] = high_row(k)

    def wait_radial(copies):
        pl.when(place > 0)(lambda: copies[0].wait_recv())
        pl.when(place < last)(lambda: copies[1].wait_recv())

    def wait_sent(copies):
        pl.when(place < last)(lambda: copies[0].wait_send())
        pl.when(place > 0)(lambda: copies[1].wait_send())
        copies[2].wait_send()
        copies[3].wait_send()

    first_halos = halo_copies(
        0, u0.at[:, pl.ds(8 + (rows - 2) * width, 2 * width), :], u0.at[:, pl.ds(8, 2 * width), :],
        pk0, hr0, hp0,
    )
    start_halos(
        first_halos, hr0,
        lambda k: u0[k, pl.ds(8, width), :],
        lambda k: u0[k, pl.ds(8 + (rows - 1) * width, width), :],
    )

    answer()

    wide_lane = lax.broadcasted_iota(jnp.int32, (width, 128), 1)

    def keep(direction, side, where, state):
        for n, k in enumerate(STEADY):
            prep[direction, side, n, where, :] = state[k]
        for n, value in enumerate(side_ready(state)):
            prep[direction, side, len(STEADY) + n, where, :] = value

    def kept(direction, where, left, right):
        ready = []
        for side, state in enumerate((left, right)):
            for n, k in enumerate(STEADY):
                state[k] = prep[direction, side, n, where, :]
            ready.append(tuple(prep[direction, side, len(STEADY) + n, where, :] for n in range(3)))
        return ready

    def prepare(u):
        def one_row(r, carry):
            base = pl.multiple_of(8 + r * width, 8)
            where = pl.ds(pl.multiple_of(r * width, 8), width)
            left, right = {}, {}
            for k in STEADY:
                cell = u[k, pl.ds(base, width), :]
                high = (pltpu.roll(cell, 127, 1) - cell) * ct[4:5, :]
                low = (cell - pltpu.roll(cell, 1, 1)) * ct[5:6, :]
                slope = half_slope(low, high)
                left[k] = cell + slope
                right[k] = jnp.where(wide_lane == 127, cell, pltpu.roll(cell - slope, 127, 1))
            keep(0, 0, where, left)
            keep(0, 1, where, right)
            for k in STEADY:
                cell = u[k, pl.ds(base, width), :]
                low = 0.5 * (cell - u[k, pl.ds(base - 1, width), :])
                high = 0.5 * (u[k, pl.ds(base + 1, width), :] - cell)
                slope = half_slope(low, high)
                left[k] = pltpu.roll(cell + slope, 1, 0)
                right[k] = cell - slope
            keep(1, 0, where, left)
            keep(1, 1, where, right)
            return carry

        lax.fori_loop(0, rows, one_row, 0)

        def one_inner_row(r, carry):
            base = pl.multiple_of(8 + r * width, 8)
            where = pl.multiple_of(r * width, 8)
            left, right = {}, {}
            for k in STEADY:
                cell = u[k, pl.ds(base, width), :]
                low = 0.5 * (cell - u[k, pl.ds(base - width, width), :])
                high = 0.5 * (u[k, pl.ds(base + width, width), :] - cell)
                slope = half_slope(low, high)
                left[k], right[k] = cell + slope, cell - slope
            keep(2, 0, pl.ds(pl.multiple_of(where + width, 8), width), left)
            keep(2, 1, pl.ds(where, width), right)
            return carry

        lax.fori_loop(1, rows - 1, one_inner_row, 0)

    def inner_radial_row(u, prepared=False):
        moving = MOVED if prepared else range(NV)

        def one_row(r, carry=0):
            base = pl.multiple_of(8 + r * width, 8)
            store = pl.multiple_of(r * width, 8)
            left, right = {}, {}
            for k in moving:
                cell = u[k, pl.ds(base, width), :]
                low = 0.5 * (cell - u[k, pl.ds(base - width, width), :])
                high = 0.5 * (u[k, pl.ds(base + width, width), :] - cell)
                slope = half_slope(low, high)
                right[k] = cell - slope
                left[k] = sl[k, pl.ds(store - width, width), :]
                sl[k, pl.ds(store, width), :] = cell + slope
            ready = kept(2, pl.ds(store, width), left, right) if prepared else (None, None)
            flux = twice_flux(left, right, 1, ready)
            for k in range(NV):
                fr[k, pl.ds(store, width), :] = flux[k]
            return carry

        return one_row

    def inner_radial(u):
        two_at_a_time(1, rows - 1, inner_radial_row(u))

    def polar_and_azimuth(u, prepared=None):
        moving = MOVED if prepared else range(NV)
        radial_row = inner_radial_row(u, prepared)

        together = 2 if prepared else 1
        sine, inverse_sine, cotangent, mask = ct[0:1, :], ct[1:2, :], ct[2:3, :], ct[4:5, :]

        def third(i, n):
            r = jnp.maximum((i - 2) * together, 0) + n
            store = pl.ds(pl.multiple_of(r * width, 8), width)
            scale = tab[0, pl.ds(r, 1), :]
            cells = [u[k, pl.ds(pl.multiple_of(8 + r * width, 8), width), :] for k in range(NV)]
            source, density = sources(cells, cotangent)
            pull = grav[pl.ds(r, 1), :]
            across = scale * inverse_sine
            for k in range(NV):
                through = th[k, store, :]
                value = cells[k] + across * (pltpu.roll(through, 1, 1) - through)
                if source[k] is not None:
                    value = value + scale * source[k]
                if prepared:
                    if k == 1:
                        value = value - pull * density
                    elif k == 4:
                        value = value - pull * cells[1]
                    before = u0[k, pl.ds(pl.multiple_of(8 + r * width, 8), width), :]
                    value = 0.5 * (before + value)
                acc[k, store, :] = value

        def second(i, n):
            r = jnp.clip((i - 1) * together, 0, rows - together) + n
            store = pl.ds(pl.multiple_of(r * width, 8), width)
            left = {k: lt[k, store, :] for k in moving}
            right = {}
            for k in moving:
                value = rt[k, store, :]
                cell = u[k, pl.ds(pl.multiple_of(8 + r * width, 8), width), :]
                right[k] = jnp.where(wide_lane == 127, cell, pltpu.roll(value, 127, 1))
            ready = kept(0, store, left, right) if prepared else (None, None)
            flux = twice_flux(left, right, 2, ready, sine)
            for k in range(NV):
                th[k, store, :] = flux[k]

        def first(i, n):
            r = jnp.minimum(i * together, rows - together) + n
            base = pl.multiple_of(8 + r * width, 8)
            store = pl.ds(pl.multiple_of(r * width, 8), width)
            cells = {k: u[k, pl.ds(base, width), :] for k in moving}
            for k in moving:
                high = (pltpu.roll(cells[k], 127, 1) - cells[k]) * mask
                low = (cells[k] - pltpu.roll(cells[k], 1, 1)) * ct[5:6, :]
                slope = half_slope(low, high)
                lt[k, store, :] = cells[k] + slope
                rt[k, store, :] = cells[k] - slope
            left, right = {}, {}
            for k in moving:
                low = 0.5 * (cells[k] - u[k, pl.ds(base - 1, width), :])
                high = 0.5 * (u[k, pl.ds(base + 1, width), :] - cells[k])
                slope = half_slope(low, high)
                left[k] = pltpu.roll(cells[k] + slope, 1, 0)
                right[k] = cells[k] - slope
            ready = kept(1, store, left, right) if prepared else (None, None)
            flux = twice_flux(left, right, 3, ready)
            for k in range(NV):
                fp[k, pl.ds(pl.multiple_of(r * span, 8), width), :] = flux[k]

        def run(i, stages):
            for stage in stages:
                for n in range(together):
                    stage(i, n)

        def one_step(i, carry):
            run(i, (third, second, first))
            return carry

        steps = rows // together
        if prepared:
            third_part = (rows - 2) // 3
            run(0, (first,))
            for r in range(1, 1 + third_part):
                radial_row(jnp.int32(r))
            run(1, (second, first))
            lax.fori_loop(2, steps, one_step, 0)
            run(steps, (third, second))
            for r in range(1 + third_part, 1 + 2 * third_part):
                radial_row(jnp.int32(r))
            for r in range(1 + 2 * third_part, rows - 1):
                radial_row(jnp.int32(r))
            prepared()
            run(steps + 1, (third,))
            edge_azimuth(u1, hp1)
            edge_radial(u1, hr1)
        else:
            lax.fori_loop(0, steps + 2, one_step, 0)

    def edge_azimuth(u, halo):
        for side in range(2):
            own = (0, 1, 2) if side == 0 else (width - 3, width - 2, width - 1)
            inside = [
                [u[k, pl.ds(8 + f, 8, stride=width), :] for k in range(NV)] for f in own
            ]
            outside = [[halo[side, k, i] for k in range(NV)] for i in range(2)]
            cells = outside + inside if side == 0 else inside + outside
            fluxes = edge_pair(cells, 3)
            faces = (0, 1) if side == 0 else (width - 1, width)
            for face, flux in zip(faces, fluxes):
                for k in range(NV):
                    fp[k, pl.ds(face, 8, stride=span), :] = flux[k]

    def edge_radial(u, halo):
        for side in range(2):
            own = (0, 1, 2) if side == 0 else (rows - 3, rows - 2, rows - 1)
            inside = [[u[k, pl.ds(8 + r * width, width), :] for k in range(NV)] for r in own]
            outside = [
                [halo[side, k, pl.ds(width * i, width), :] for k in range(NV)] for i in range(2)
            ]
            cells = outside + inside if side == 0 else inside + outside
            fluxes = edge_pair(cells, 1)
            faces = (0, 1) if side == 0 else (rows - 1, rows)
            for face, flux in zip(faces, fluxes):
                for k in range(NV):
                    fr[k, pl.ds(face * width, width), :] = flux[k]

    def advanced_row(r):
        return row_sum(r, 1.0, width, acc, fp, fr, tab, ct)

    with jax.named_scope("pre1"):
        polar_and_azimuth(u0)
    with jax.named_scope("rad1"):
        inner_radial(u0)

    with jax.named_scope("wedge_wait"):
        wedge_all().wait_recv()
    shell_row = wedge_rows[0]
    for j in range(1, wedges):
        shell_row = shell_row + wedge_rows[j]
    below_above[2] = shell_row
    pl.when(place < last)(lambda: side_copy(0).start())
    pl.when(place > 0)(lambda: side_copy(1).start())

    @pl.when(sender)
    def _():
        many(wedges, chip_send, chip_recv).wait_recv()
        chip_row = shell_row
        for j in range(wedges):
            chip_row = chip_row + chip_rows[j]
        below_above[3] = chip_row
        send_across(0, jnp.minimum(level, near))
        pl.when(near_answers > 0)(lambda: pl.semaphore_wait(from_near, near_answers))
        send_across(jnp.minimum(level, near), near)

    with jax.named_scope("h1_phi_wait"):
        first_halos[2].wait_recv()
        first_halos[3].wait_recv()
    with jax.named_scope("edge_phi1"):
        edge_azimuth(u0, hp0)
    with jax.named_scope("h1_rad_wait"):
        wait_radial(first_halos)
    with jax.named_scope("edge_rad1"):
        edge_radial(u0, hr0)

    def section_one_row(r, carry):
        values = advanced_row(r)
        for k in range(NV):
            u1[k, pl.ds(pl.multiple_of(8 + r * width, 8), width), :] = values[k]
        return carry

    with jax.named_scope("final1"):
        two_at_a_time(0, rows, section_one_row)
    for k in range(NV):
        sr[0, k] = u1[k, pl.ds(8 + (rows - 2) * width, 2 * width), :]
        sr[1, k] = u1[k, pl.ds(8, 2 * width), :]
    pack(u1, pk1)
    wait_sent(first_halos)
    second_halos = halo_copies(1, sr.at[0], sr.at[1], pk1, hr1, hp1)
    start_halos(
        second_halos, hr1,
        lambda k: sr[1, k, pl.ds(0, width), :],
        lambda k: sr[0, k, pl.ds(width, width), :],
    )

    with jax.named_scope("asc_wait"):
        pl.when(far_answers > 0)(lambda: pl.semaphore_wait(from_far, far_answers))
    pl.when(sender)(send_along)

    def gather_across():
        for x in range(1, groups):

            @pl.when(group == x)
            def _(count=x):
                many(count * levels, shared_send, shared_recv).wait_recv()
                value = [shared[n] for n in range(count)]
                for z in range(1, levels):
                    value = [value[n] + shared[z * groups + n] for n in range(count)]
                inside_rows[0] = functools.reduce(jnp.add, value)
                for passer, z_start, z_stop in passers:

                    @pl.when(jnp.logical_and(sender, level == passer))
                    def _(z_start=z_start, z_stop=z_stop):
                        for z in range(z_start, z_stop):
                            for c in both:
                                pass_copy(z, c).start()

    def gather_along():
        for z in range(1, levels):

            @pl.when(level == z)
            def _(z=z):
                many(z, along_send, along_recv).wait_recv()
                inside_rows[2] = functools.reduce(jnp.add, [along[n] for n in range(z)])

    half_of = lambda index: jnp.where(lane < index, 1.0, jnp.where(lane == index, 0.5, 0.0))
    none = jnp.zeros((8, 128), jnp.float32)
    lower = jnp.where(row < 2, jnp.where(place == 0, half_of(0), none), 0.0)
    upper = jnp.where(row < 2, none, jnp.where(place == last, half_of(rows - 1), 1.0))
    minus = jnp.where(lane >= rows, 0.0, half_of(rows - 2 + row) - 1.0)
    minus = jnp.where(jnp.logical_and(row < 2, place > 0), minus, none)
    plus = jnp.where(jnp.logical_or(row < 2, place == last), none, half_of(row - 2))
    beyond = jnp.clip(first + jnp.where(row < 2, row - 2, rows - 2 + row), 0, slabs * rows - 1)
    weights[0] = half_of(row)
    weights[1] = lower + upper
    weights[2] = minus
    weights[3] = plus
    for i, target in enumerate((first + row, beyond)):
        inverse = 1.0 / radius_of(target)
        weights[4 + i] = (timestep * strength) * inverse * inverse
    fetch_mass.wait()

    with jax.named_scope("prepare"):
        prepare(u1)
    with jax.named_scope("m1_wait"):
        pl.when(is_near)(gather_across)
        gather_along()
        pl.when(jnp.logical_and(group > 0, jnp.logical_not(is_near)))(
            lambda: pass_copy(levels - 1, 1).wait_recv()
        )
        pl.when(place > 0)(lambda: side_copy(0).wait_recv())
        pl.when(place < last)(lambda: side_copy(1).wait_recv())
    below, above, own = below_above[0], below_above[1], below_above[2]
    smaller_x = jnp.where(is_near, inside_rows[0], inside_rows[1])
    inside = jnp.where(level > 0, inside_rows[2], 0.0)
    inside = inside + jnp.where(group > 0, smaller_x, 0.0) + jnp.where(core_index == 1, below, 0.0)
    table = (
        inside + weights[0] * own,
        inside + weights[1] * own + weights[2] * below + weights[3] * above,
    )
    for i in range(2):
        enclosed = jnp.sum(table[i], axis=1, keepdims=True) + core[0]
        grav[8 * i : 8 * i + 8, :] = weights[4 + i] * enclosed
        if i == 0:
            enclosed_ref[...] = jnp.sum(
                jnp.where(lane == row, enclosed, 0.0), axis=0, keepdims=True
            )[:, :rows]

    def gravity_row(r, carry):
        base = pl.ds(pl.multiple_of(8 + r * width, 8), width)
        pull = grav[pl.ds(r, 1), :]
        u1[1, base, :] = u1[1, base, :] - pull * jnp.maximum(u0[0, base, :], MINIMUM_DENSITY)
        u1[4, base, :] = u1[4, base, :] - pull * u0[1, base, :]
        return carry

    with jax.named_scope("grav"):
        two_at_a_time(0, rows, gravity_row)

    def outer_faces():
        second_halos[2].wait_recv()
        second_halos[3].wait_recv()
        wait_radial(second_halos)
        pull = grav[0:8, :]
        for side in range(2):
            for i in range(2):
                hp1[side, 1, i] = hp1[side, 1, i] - pull * jnp.maximum(
                    hp0[side, 0, i], MINIMUM_DENSITY
                )
                hp1[side, 4, i] = hp1[side, 4, i] - pull * hp0[side, 1, i]
        for side in range(2):
            for i in range(2):
                which = pl.ds(width * i, width)
                pull = grav[8 + 2 * side + i : 9 + 2 * side + i, :]
                hr1[side, 1, which, :] = hr1[side, 1, which, :] - pull * jnp.maximum(
                    hr0[side, 0, which, :], MINIMUM_DENSITY
                )
                hr1[side, 4, which, :] = hr1[side, 4, which, :] - pull * hr0[side, 1, which, :]

    with jax.named_scope("pre2"):
        polar_and_azimuth(u1, outer_faces)
    with jax.named_scope("drain"):
        @pl.when(sender)
        def _():
            for x in range(groups - 1):

                @pl.when(group == x)
                def _(count=2 * near * (groups - 1 - x)):
                    many(count, shared_send, shared_recv).wait_send()

            for z in range(levels - 1):
                pl.when(level == z)(
                    lambda count=2 * (levels - 1 - z): many(
                        count, along_send, along_recv
                    ).wait_send()
                )
            for passer, z_start, z_stop in passers:
                pl.when(jnp.logical_and(group > 0, level == passer))(
                    lambda count=2 * (z_stop - z_start): many(
                        count, pass_send, pass_recv
                    ).wait_send()
                )

        pl.when(jnp.logical_not(sender))(lambda: many(wedges, chip_send, chip_recv).wait_send())
        wedge_all().wait_send()
        pl.when(place < last)(lambda: side_copy(0).wait_send())
        pl.when(place > 0)(lambda: side_copy(1).wait_send())
        wait_sent(second_halos)


def put_out(
    rows, width, acc, fp, fr, tab, ct, enclosed, advanced_hbm, enclosed_hbm, outv, sem
):
    copies = [pltpu.make_async_copy(enclosed, enclosed_hbm, sem.at[rows // 2])]
    copies[0].start()
    for pair in range(rows // 2):
        for r in (2 * pair, 2 * pair + 1):
            for k, value in enumerate(row_sum(r, 0.5, width, acc, fp, fr, tab, ct)):
                outv[k, r * width : (r + 1) * width, :] = value
        where = pl.ds(2 * pair * width, 2 * width)
        copies.append(
            pltpu.make_async_copy(
                outv.at[:, where, :], advanced_hbm.at[:, where, :], sem.at[pair]
            )
        )
        copies[-1].start()
    for copy in copies:
        copy.wait()


def body(groups, conserved, core_mass):
    _, rows, width, lanes = conserved.shape
    slabs, wedges = lax.axis_size("radial"), lax.axis_size("phi")
    inner = slabs // groups
    radial_step, theta_step, phi_step, timestep = step_sizes(rows * slabs, width * wedges, lanes)
    centers = (np.arange(lanes) + 0.5) * theta_step
    faces = (np.arange(lanes) + 1.0) * theta_step
    angles = np.zeros((8, lanes))
    angles[0] = np.sin(faces) * (0.5 / theta_step)
    angles[1] = 1.0 / np.sin(centers)
    angles[2] = np.cos(centers) / np.sin(centers)
    angles[3] = np.sin(centers)
    angles[4] = np.where(np.arange(lanes) == lanes - 1, 0.0, 0.5)
    angles[6] = angles[1] * (0.5 / phi_step)
    angles[5] = np.where(np.arange(lanes) == 0, 0.0, 0.5)
    angles = jnp.asarray(angles.astype(np.float32))
    sizes = (rows, width, slabs, wedges, groups, radial_step, theta_step, phi_step, timestep)
    f32 = jnp.float32
    vmem = lambda *shape: pltpu.VMEM(shape, f32)
    dma = lambda count: pltpu.SemaphoreType.DMA((count,))
    in_hbm = lambda value: pltpu.with_memory_space_constraint(value, pltpu.HBM)
    cells = rows * width
    *parts, enclosed = pl.pallas_call(
        functools.partial(kernel, sizes),
        out_shape=[
            jax.ShapeDtypeStruct(shape, f32)
            for shape in (
                (NV, cells, lanes),
                (NV, rows * (width + 8), lanes),
                (NV, cells + width, lanes),
                (3, 8, lanes),
                (8, lanes),
                (1, rows),
            )
        ],
        in_specs=[
            pl.BlockSpec(memory_space=pltpu.HBM),
            pl.BlockSpec(memory_space=pltpu.HBM),
            pl.BlockSpec(memory_space=pltpu.HBM),
        ],
        out_specs=[pl.BlockSpec(memory_space=pltpu.VMEM)] * 6,
        scratch_shapes=[
            vmem(NV, cells + 16, lanes), vmem(NV, cells + 16, lanes),
            vmem(2, NV, 2 * width, lanes), vmem(2, NV, 2 * width, lanes),
            vmem(2, NV, 2, 8, lanes), vmem(2, NV, 2, 8, lanes),
            vmem(2, NV, 2, 8, lanes), vmem(2, NV, 2, 8, lanes),
            vmem(2, NV, 2 * width, lanes),
            vmem(NV, cells, lanes),
            vmem(NV, cells, lanes), vmem(NV, cells, lanes), vmem(NV, cells, lanes),
            vmem(3, 2, len(STEADY) + 3, cells, lanes),
            vmem(slabs // 2, 1, lanes), vmem(inner // 2, 1, lanes), vmem(4, 1, lanes), vmem(wedges, 1, lanes),
            vmem(wedges, 1, lanes), vmem(3, 1, lanes), vmem(6, 8, lanes),
            vmem(16, lanes), pltpu.SMEM((1,), f32),
            dma(4), dma(4), dma(8), *[pltpu.SemaphoreType.DMA] * 4, dma(2), dma(2),
            pltpu.SemaphoreType.DMA, pltpu.SemaphoreType.DMA,
            pltpu.SemaphoreType.DMA, pltpu.SemaphoreType.DMA,
            pltpu.SemaphoreType.DMA, pltpu.SemaphoreType.DMA,
            pltpu.SemaphoreType.REGULAR, pltpu.SemaphoreType.REGULAR,
        ],
        compiler_params=pltpu.CompilerParams(
            collective_id=0, has_side_effects=True, vmem_limit_bytes=12 << 20
        ),
    )(in_hbm(conserved.reshape(NV, cells, lanes)), core_mass, in_hbm(angles))
    advanced, enclosed = pl.pallas_call(
        functools.partial(put_out, rows, width),
        out_shape=(
            jax.ShapeDtypeStruct((NV, cells, lanes), f32),
            jax.ShapeDtypeStruct((1, rows), f32),
        ),
        in_specs=[pl.BlockSpec(memory_space=pltpu.VMEM)] * 6,
        out_specs=[pl.BlockSpec(memory_space=pltpu.HBM)] * 2,
        scratch_shapes=[vmem(NV, cells, lanes), dma(rows // 2 + 1)],
        compiler_params=pltpu.CompilerParams(vmem_limit_bytes=8 << 20),
    )(*parts, enclosed)
    return advanced.reshape(conserved.shape), enclosed.reshape(rows)


def solution(mesh):
    in_specs = (P(None, "radial", "phi", None), P())
    out_specs = (P(None, "radial", "phi", None), P("radial"))
    return jax.shard_map(
        functools.partial(body, 4), mesh=mesh, in_specs=in_specs, out_specs=out_specs,
        check_vma=False,
    )
```
